256 devices in a mesh: bvec: 4 (over x), row: 16 (over z, core), col: 4 (over y).
Axes of the slice: x: 4, y: 4, z: 8, core: 2. Of those that a mesh axis runs over, the one named last changes fastest.
Arguments:
- m_matrices: float32 [4, 2, 2048, 2048], P('bvec', None, 'row', 'col'), may hold values from -2 to 2, as said below
- bvec_index: int32 [4], replicated, may hold values from 0 to 5
- weight_table: float32 [6], replicated, may hold values from 0.25 to 2
- grad_prev: float32 [2048, 2048], P('row', 'col'), may hold values from -4 to 4, as said below
- dir_prev: float32 [2048, 2048], P('row', 'col'), may hold values from -4 to 4, as said below
Outputs:
- spread: float32 [], replicated
- trial_spread: float32 [], replicated
- gradient: float32 [2048, 2048], P('row', 'col')
- direction: float32 [2048, 2048], P('row', 'col')
- trial_diag: float32 [4, 2, 2048], replicated
The draws below stay inside these ranges and needn't reach their ends.
Inputs may be any that keep to these rules, and one draw needn't show every extreme that they name: Each matrix m_matrices[b, p] is symmetric. grad_prev is antisymmetric. dir_prev is antisymmetric.
All inputs are finite; a program needn't handle non-finite values.
Results may differ from the reference program's by a relative error of at most 0.0003.
Values sent between devices are 32-bit elements; how exact they have to be, the bound alone decides.
A program may use at most 64 MiB of HBM per device.

```python
import math
import jax
import jax.numpy as jnp
from jax import lax

N = 2048
NTAB = 6
TAYLOR = 8
NB = 4


def draw_m_matrices(key, part):
    subkeys = jax.random.split(jax.random.fold_in(key, 101), 4)
    gaussian = jax.random.normal(subkeys[0], (NB, 2, N, N), jnp.float32)
    noise_scale = 0.25
    radius = jax.random.uniform(subkeys[1], (NB, N), jnp.float32, 0.3, 0.95)
    angles = jax.random.uniform(subkeys[2], (NB, N), jnp.float32, -math.pi, math.pi)
    symmetric = (gaussian + jnp.swapaxes(gaussian, 2, 3)) * (noise_scale / math.sqrt(2.0))
    identity = jnp.eye(N, dtype=jnp.float32)
    diag_parts = jnp.stack([radius * jnp.cos(angles), radius * jnp.sin(angles)], axis=1)
    matrix = symmetric * (1.0 - identity) + diag_parts[:, :, :, None] * identity
    return jnp.clip(matrix, -2.0, 2.0)


def antisymmetric(key, noise_scale):
    gaussian = jax.random.normal(key, (N, N), jnp.float32)
    factor = noise_scale
    return jnp.clip((gaussian - gaussian.T) * (factor / math.sqrt(2.0)), -4.0, 4.0)


def draw_grad_prev(key, part):
    return antisymmetric(jax.random.fold_in(key, 7), 0.6)


def draw_dir_prev(key, part):
    return antisymmetric(jax.random.fold_in(key, 13), 0.6)


def plant(array, rng, smallest, top_value):
    spot = [jax.random.randint(jax.random.fold_in(rng, axis), (), 0, length) for axis, length in enumerate(array.shape)]
    longest = array.shape.index(max(array.shape))
    neighbour = spot[:longest] + [(spot[longest] + 1) % array.shape[longest]] + spot[longest + 1:]
    return array.at[tuple(spot)].set(smallest).at[tuple(neighbour)].set(top_value)


def setup_inputs(seed: int = 0) -> dict:
    seeds = jax.random.split(jax.random.key(seed), 6)
    return {
        "m_matrices": draw_m_matrices(jax.random.fold_in(seeds[5], 71), 0),
        "bvec_index": plant(jax.random.randint(seeds[1], (NB,), 0, NTAB), jax.random.fold_in(seeds[1], 1), 0, NTAB - 1).astype(jnp.int32),
        "weight_table": jnp.clip(jnp.exp(jax.random.uniform(seeds[2], (NTAB,), jnp.float32, math.log(0.25), math.log(2.0))), 0.25, 2.0),
        "grad_prev": draw_grad_prev(jax.random.fold_in(seeds[5], 71), 0),
        "dir_prev": draw_dir_prev(jax.random.fold_in(seeds[5], 71), 0),
    }


def product(left, right):
    return jnp.dot(left, right, precision=lax.Precision.HIGHEST, preferred_element_type=jnp.float32)

def reference(m_matrices, bvec_index, weight_table, grad_prev, dir_prev):
    table_slots = jnp.arange(weight_table.shape[0], dtype=jnp.int32)
    weight = lax.optimization_barrier(jnp.sum(jnp.where(table_slots[None, :] == bvec_index[:, None], weight_table[None, :], 0.0), axis=1))
    re_diag = jnp.diagonal(m_matrices[:, 0], axis1=1, axis2=2)
    im_diag = jnp.diagonal(m_matrices[:, 1], axis1=1, axis2=2)
    spread = jnp.sum(weight[:, None] * (1.0 - re_diag ** 2 - im_diag ** 2)) / N
    gradient = jnp.zeros((N, N), jnp.float32)
    for bvec in range(NB):
        real_term = m_matrices[bvec, 0] * (re_diag[bvec][:, None] - re_diag[bvec][None, :])
        imag_term = m_matrices[bvec, 1] * (im_diag[bvec][:, None] - im_diag[bvec][None, :])
        gradient = gradient + 2.0 * weight[bvec] * (real_term + imag_term)
    beta_factor = jnp.sum(gradient * gradient) / (1.0 + jnp.sum(grad_prev * grad_prev))
    direction = beta_factor * dir_prev - gradient
    trial_generator = 1.75 * direction / jnp.sqrt(1.0 + jnp.sum(direction * direction) / N)
    identity = jnp.eye(N, dtype=jnp.float32)
    horner = identity + trial_generator / TAYLOR
    for degree in range(TAYLOR - 1, 0, -1):
        horner = identity + product(horner, trial_generator) / degree
    expmap = horner
    entries = []
    for bvec in range(NB):
        parts = []
        for index in range(2):
            rotated = product(m_matrices[bvec, index], expmap)
            parts.append(lax.optimization_barrier(jnp.sum(expmap * rotated, axis=0)))
        entries.append(jnp.stack(parts, axis=0))
    trial_diag = jnp.stack(entries, axis=0)
    trial_spread = jnp.sum(weight[:, None] * (1.0 - trial_diag[:, 0] ** 2 - trial_diag[:, 1] ** 2)) / N
    return (spread, trial_spread, gradient, direction, trial_diag)
```

```python
import functools
import math

import jax
import jax.numpy as jnp
from jax import lax
from jax.experimental import pallas as pl
from jax.experimental.pallas import tpu as pltpu
from jax.sharding import Mesh
from jax.sharding import PartitionSpec as P

ROW = ("zed", "core")
STEP_SCALE = 1.75
BLK = 128
MESH = pl.DeviceIdType.MESH

R177 = math.sqrt(177.0)
X3 = 2.0 / 3.0
X1 = X3 * (1.0 + R177) / 88.0
X2 = X3 * (1.0 + R177) / 352.0
X4 = (-271.0 + 29.0 * R177) / (315.0 * X3)
X5 = 11.0 * (-1.0 + R177) / (1260.0 * X3)
X6 = 11.0 * (-9.0 + R177) / (5040.0 * X3)
X7 = (89.0 - R177) / (5040.0 * X3 * X3)
Y2 = (857.0 - 58.0 * R177) / 630.0


def split(value):
    high = value.astype(jnp.bfloat16)
    low = (value - high.astype(jnp.float32)).astype(jnp.bfloat16)
    return high, low


def dot(left, right):
    return jnp.dot(left, right, preferred_element_type=jnp.float32)


def dot_split(left, right):
    (lh, ll), (rh, rl) = left, right
    return dot(lh, rh) + (dot(lh, rl) + dot(ll, rh))


def kernel(
    dims, idx_ref, tab_ref, m_ref, gp_ref, dp_ref,
    grad_ref, dir_ref, trial_ref, stat_ref,
    mall, dcm, drt, dsrc, gblk, blk2, blk4, eblk, etr, stile, sx, sz,
    drow, dcol, grow, gcol, acol, row2, col2, row4, col4, erow, ej, part, pz, px, qtile, ttile, tfin,
    a2a_s, a2a_r, dia_s, dia_r, dpr_s, dpr_r, row_s, row_r, col_s, col_r, fwd_s, fwd_r, one_s, one_r, sml_s, sml_r,
):
    nx, ny, nz, nk = dims
    count = nx * ny
    order = count * BLK
    wide = nx * BLK
    x, y = lax.axis_index("bvec"), lax.axis_index("col")
    z, k = lax.axis_index("zed"), lax.axis_index("core")
    r = nk * z + k
    c = nx * y + x

    def dev(xx, yy, zz, kk):
        return {"bvec": xx, "zed": zz, "core": kk, "col": yy}

    def off(value, step, size):
        return lax.rem(value + step, size) if step else value

    def lanes(index, size=BLK):
        return pl.ds(pl.multiple_of(index * size, size), size)

    plane = [(ox, oy) for ox in range(nx) for oy in range(ny) if (ox, oy) != (0, 0)]
    line = [(oz, ok) for oz in range(nz) for ok in range(nk)]
    others = line[1:]

    def at_plane(ox, oy):
        return dev(off(x, ox, nx), off(y, oy, ny), z, k)

    def at_line(oz, ok):
        return dev(x, y, off(z, oz, nz), off(k, ok, nk))

    px_t, py_t = lax.rem(r, nx), lax.div(r, nx)
    pz_t, pk_t = lax.div(c, nk), lax.rem(c, nk)
    off_diag = r != c
    holds = y == py_t

    barrier = pltpu.get_barrier_semaphore()
    for ox, oy in plane:
        pl.semaphore_signal(barrier, inc=1, device_id=at_plane(ox, oy), device_id_type=MESH)
    for oz, ok in others:
        pl.semaphore_signal(barrier, inc=1, device_id=at_line(oz, ok), device_id_type=MESH)

    @pl.when(off_diag)
    def _():
        pl.semaphore_signal(barrier, inc=1, device_id=dev(px_t, py_t, pz_t, pk_t), device_id_type=MESH)

    for b in range(nx):
        @pl.when((x != b) | off_diag)
        def _(b=b):
            pl.semaphore_signal(barrier, inc=1, device_id=dev(b, y, pz_t, pk_t), device_id_type=MESH)

    mall[pl.ds(x, 1)] = m_ref[:, :, lanes(x)][None]
    own_d = dp_ref[:, lanes(x)]
    eye_r = lax.broadcasted_iota(jnp.int32, (BLK, BLK), 0)
    eye_c = lax.broadcasted_iota(jnp.int32, (BLK, BLK), 1)
    eye = eye_r == eye_c
    dsrc[...] = jnp.zeros((8, BLK), jnp.float32)
    for p in range(2):
        dsrc[p:p + 1, :] = jnp.sum(jnp.where(eye, m_ref[p, :, lanes(px_t)], 0.0), axis=0, keepdims=True)
    if nx * 8 < BLK:
        dcm[nx * 8:, :] = jnp.zeros((BLK - nx * 8, BLK), jnp.float32)
    drow[:, lanes(y, wide)] = dp_ref[...]
    dcol[lanes(r), :] = own_d

    expected = len(plane) + len(others) + off_diag.astype(jnp.int32)
    asked = len(line) - (x == px_t).astype(jnp.int32)
    pl.semaphore_wait(barrier, expected + holds.astype(jnp.int32) * asked)

    def remote(src, dst, send, recv, device):
        return pltpu.make_async_remote_copy(
            src_ref=src, dst_ref=dst, send_sem=send, recv_sem=recv, device_id=device, device_id_type=MESH
        )

    dia_row = [
        remote(dsrc, dcm.at[pl.ds(pl.multiple_of(8 * x, 8), 8), :], dia_s.at[i], dia_r.at[x], at_plane(ox, oy))
        for i, (ox, oy) in enumerate(plane)
    ]
    dia_col = [
        remote(dsrc, drt.at[x], dia_s.at[len(plane) + i], dia_r.at[nx + x],
               dev(px_t, y, off(z, oz, nz), off(k, ok, nk)))
        for i, (oz, ok) in enumerate(line)
    ]

    @pl.when(holds)
    def _():
        for copy in dia_row:
            copy.start()
        for copy in dia_col[1:]:
            copy.start()
        dcm[pl.ds(pl.multiple_of(8 * x, 8), 8), :] = dsrc[...]

    @pl.when(holds & (x != px_t))
    def _():
        dia_col[0].start()

    @pl.when(jnp.logical_not(off_diag))
    def _():
        drt[pl.ds(x, 1)] = dsrc[...][None]

    a2a = []
    for ox in range(1, nx):
        xp = off(x, ox, nx)
        copy = remote(m_ref.at[:, :, lanes(xp)], mall.at[x], a2a_s.at[ox - 1], a2a_r.at[ox - 1], dev(xp, y, z, k))
        copy.start()
        a2a.append(copy)

    dprow = []
    for oy in range(1, ny):
        copy = remote(dp_ref, drow.at[:, lanes(y, wide)], dpr_s.at[oy - 1], dpr_r.at[oy - 1], at_plane(0, oy))
        copy.start()
        dprow.append(copy)

    def row_gather(stage, src, dst):
        copies = []
        for i, (ox, oy) in enumerate(plane):
            copy = remote(src, dst.at[:, lanes(c)], row_s.at[i], row_r.at[stage, i], at_plane(ox, oy))
            copy.start()
            copies.append(copy)
        return copies

    near = sorted(range(1, nz), key=lambda oz: (min(oz, nz - oz), oz))

    def line_gather(stage, src, slot):
        sends = {}
        for oz in near:
            sends[oz] = remote(src, slot(r), col_s.at[oz - 1], col_r.at[stage, oz - 1], at_line(oz, 0))
            sends[oz].start()
        forwards = [remote(src, slot(r), fwd_s.at[0], fwd_r.at[stage, 0], at_line(0, 1))]
        forwards[0].start()
        return sends, forwards, stage, slot

    def line_wait(state):
        sends, forwards, stage, slot = state
        for oz in near:
            sends[oz].wait_recv()
            held = slot(nk * off(z, nz - oz, nz) + k)
            copy = remote(held, held, fwd_s.at[oz], fwd_r.at[stage, oz], at_line(0, 1))
            copy.start()
            forwards.append(copy)
        for copy in forwards:
            copy.wait()
        for oz in near:
            sends[oz].wait_send()

    def column_slots(ref):
        return lambda index: ref.at[lanes(index), :]

    def row_slots(ref):
        return lambda index: ref.at[:, lanes(index)]

    dcol_state = line_gather(0, dp_ref.at[:, lanes(x)], column_slots(dcol))

    for b in range(nx):
        @pl.when(jnp.logical_not(holds & (x == b)))
        def _(b=b):
            slot = dcm.at[8 * b:8 * b + 8, :]
            remote(slot, slot, dia_s.at[0], dia_r.at[b], dev(x, y, z, k)).wait_recv()

        @pl.when(off_diag | (x != b))
        def _(b=b):
            slot = drt.at[b]
            remote(slot, slot, dia_s.at[0], dia_r.at[nx + b], dev(x, y, z, k)).wait_recv()

    weights = []
    for b in range(nx):
        value = jnp.float32(0.0)
        for t in range(tab_ref.shape[0]):
            value = value + jnp.where(idx_ref[b] == t, tab_ref[t], jnp.float32(0.0))
        weights.append(value)

    columns = jnp.transpose(dcm[...])
    for copy in a2a:
        copy.wait()
    total = jnp.zeros((BLK, BLK), jnp.float32)
    spread_row = jnp.zeros((1, BLK), jnp.float32)
    for b in range(nx):
        term = jnp.zeros((BLK, BLK), jnp.float32)
        for p in range(2):
            at_row = columns[:, 8 * b + p:8 * b + p + 1]
            at_col = drt[b, p:p + 1, :]
            term = term + mall[b, p] * (at_row - at_col)
        total = total + (2.0 * weights[b]) * term
        re_d, im_d = drt[b, 0:1, :], drt[b, 1:2, :]
        spread_row = spread_row + weights[b] * (1.0 - re_d * re_d - im_d * im_d)
    gblk[...] = total
    own_p = gp_ref[:, lanes(x)]
    first_line = (r == 0).astype(jnp.float32)
    stile[...] = jnp.zeros((8, BLK), jnp.float32)
    stile[0:1, :] = jnp.sum(total * total, axis=0, keepdims=True)
    stile[1:2, :] = jnp.sum(total * own_d, axis=0, keepdims=True)
    stile[2:3, :] = jnp.sum(own_d * own_d, axis=0, keepdims=True)
    stile[3:4, :] = jnp.sum(own_p * own_p, axis=0, keepdims=True)
    stile[4:5, :] = spread_row * first_line

    def small_plane(stage, src, dst):
        dst[pl.ds(c, 1)] = src[...][None]
        copies = []
        for i, (ox, oy) in enumerate(plane):
            copy = remote(src, dst.at[c], sml_s.at[i], sml_r.at[stage, i], at_plane(ox, oy))
            copy.start()
            copies.append(copy)
        return copies

    def small_line(stage, src, dst):
        dst[pl.ds(r, 1)] = src(r)[...][None]
        copies = []
        for i, (oz, ok) in enumerate(others):
            rp = nk * off(z, oz, nz) + off(k, ok, nk)
            copy = remote(src(rp), dst.at[r], sml_s.at[i], sml_r.at[stage, i], at_line(oz, ok))
            copy.start()
            copies.append(copy)
        return copies

    def wait_all(copies):
        for copy in copies:
            copy.wait()

    def summed(ref):
        value = ref[0]
        for i in range(1, count):
            value = value + ref[i]
        return value

    copies = small_plane(0, stile, sx)
    grow[:, lanes(c)] = total
    gcol[lanes(r), :] = total
    g_row = row_gather(0, gblk, grow)
    line_wait(dcol_state)
    g_col = line_gather(1, gblk, column_slots(gcol))
    wait_all(copies)
    stile[...] = summed(sx)
    copies = small_line(1, lambda index: stile, sz)
    wait_all(dprow)
    wait_all(copies)
    sums = jnp.broadcast_to(jnp.sum(summed(sz), axis=1, keepdims=True), (8, BLK))
    gg, gd, dd, pp = (sums[i:i + 1, :] for i in range(4))
    spread = sums[4:5, :] / order
    beta = gg / (1.0 + pp)
    norm = jnp.maximum(gg - 2.0 * beta * gd + beta * beta * dd, 0.0)
    scale = STEP_SCALE / jnp.sqrt(1.0 + norm / order)

    wait_all(g_row)
    line_wait(g_col)
    for j in range(nx):
        at = pl.ds(pl.multiple_of(y * wide + j * BLK, BLK), BLK)
        piece = grow[:, at]
        grad_ref[:, j * BLK:(j + 1) * BLK] = piece
        dir_ref[:, j * BLK:(j + 1) * BLK] = beta * drow[:, at] - piece

    chunk = 4 * BLK if order % (4 * BLK) == 0 else BLK
    beta_w = jnp.concatenate([beta] * (chunk // BLK), axis=1)
    scale_w = jnp.concatenate([scale] * (chunk // BLK), axis=1)

    acc = jnp.zeros((BLK, BLK), jnp.float32)
    for at in range(0, order, chunk):
        left = scale_w * (beta_w * drow[:, at:at + chunk] - grow[:, at:at + chunk])
        right = scale * (beta * dcol[at:at + chunk, :] - gcol[at:at + chunk, :])
        acol[at:at + chunk, :] = right
        acc = acc + dot_split(split(left), split(right))
    blk2[...] = acc
    row2[:, lanes(c)] = acc
    col2[lanes(r), :] = acc
    rows = row_gather(1, blk2, row2)
    cols = line_gather(2, blk2, column_slots(col2))
    wait_all(rows)
    line_wait(cols)

    acc = jnp.zeros((BLK, BLK), jnp.float32)
    for at in range(0, order, chunk):
        right = X1 * acol[at:at + chunk, :] + X2 * col2[at:at + chunk, :]
        acc = acc + dot_split(split(row2[:, at:at + chunk]), split(right))
    blk4[...] = acc
    row4[:, lanes(c)] = acc
    col4[lanes(r), :] = acc
    rows = row_gather(2, blk4, row4)
    cols = line_gather(3, blk4, column_slots(col4))
    wait_all(rows)
    line_wait(cols)

    acc = jnp.zeros((BLK, BLK), jnp.float32)
    for at in range(0, order, chunk):
        left = X3 * row2[:, at:at + chunk] + row4[:, at:at + chunk]
        right = X5 * acol[at:at + chunk, :] + X6 * col2[at:at + chunk, :] + X7 * col4[at:at + chunk, :]
        acc = acc + dot_split(split(left), split(right))
    acc = acc + X4 * (X3 * blk2[...] + blk4[...]) + Y2 * blk2[...] + acol[lanes(r), :]
    acc = acc + jnp.where(eye & jnp.logical_not(off_diag), 1.0, 0.0)
    eblk[...] = acc

    turn = remote(eblk, etr, one_s.at[0], one_r.at[0], dev(px_t, py_t, pz_t, pk_t))

    @pl.when(off_diag)
    def _():
        turn.start()

    erow[:, lanes(c)] = acc
    rows = row_gather(3, eblk, erow)

    @pl.when(off_diag)
    def _():
        turn.wait()

    @pl.when(jnp.logical_not(off_diag))
    def _():
        etr[...] = eblk[...]

    cols = line_gather(4, etr, row_slots(ej))
    ej[:, lanes(r)] = etr[...]
    pairs = [[split(mall[b, p]) for p in range(2)] for b in range(nx)]
    wait_all(rows)
    line_wait(cols)

    part[...] = jnp.zeros((8, order), jnp.float32)
    for at in range(0, order, chunk):
        right = split(ej[:, at:at + chunk])
        left = erow[:, at:at + chunk]
        for b in range(nx):
            for p in range(2):
                turned = dot_split(pairs[b][p], right)
                part[2 * b + p:2 * b + p + 1, at:at + chunk] = jnp.sum(left * turned, axis=0, keepdims=True)

    wait_all(small_line(2, lambda index: part.at[:, lanes(index)], pz))
    qtile[...] = summed(pz)
    wait_all(small_plane(3, qtile, px))
    sumt = summed(px)
    ttile[...] = sumt
    tfin[:, lanes(r)] = sumt
    copies = []
    for i, (oz, ok) in enumerate(others):
        copy = remote(ttile, tfin.at[:, lanes(r)], sml_s.at[i], sml_r.at[4, i], at_line(oz, ok))
        copy.start()
        copies.append(copy)

    @pl.when(holds)
    def _():
        for copy in dia_row:
            copy.wait_send()
        for copy in dia_col[1:]:
            copy.wait_send()

    @pl.when(holds & (x != px_t))
    def _():
        dia_col[0].wait_send()

    wait_all(copies)
    trial_ref[...] = tfin[...]
    trial = jnp.zeros((1, order), jnp.float32)
    for b in range(nx):
        re_t, im_t = tfin[2 * b:2 * b + 1, :], tfin[2 * b + 1:2 * b + 2, :]
        trial = trial + weights[b] * (1.0 - re_t * re_t - im_t * im_t)
    stat_ref[...] = jnp.zeros((8, BLK), jnp.float32)
    stat_ref[0:1, :] = spread
    stat_ref[1:2, :] = jnp.broadcast_to(jnp.sum(trial, axis=1, keepdims=True) / order, (1, BLK))


def shards(dims, m_matrices, bvec_index, weight_table, grad_prev, dir_prev):
    nx, ny, nz, nk = dims
    count = nx * ny
    order = count * BLK
    f32 = jnp.float32
    rows, cols = grad_prev.shape
    vmem = pl.BlockSpec(memory_space=pltpu.VMEM)
    smem = pl.BlockSpec(memory_space=pltpu.SMEM)
    wide = pltpu.VMEM((BLK, order), f32)
    tall = pltpu.VMEM((order, BLK), f32)
    block = pltpu.VMEM((BLK, BLK), f32)
    tile = pltpu.VMEM((8, BLK), f32)
    tiles = pltpu.VMEM((count, 8, BLK), f32)
    dma = pltpu.SemaphoreType.DMA
    n_plane, n_line = count - 1, nz * nk
    grad, direction, trial, stat = pl.pallas_call(
        functools.partial(kernel, dims),
        out_shape=(
            jax.ShapeDtypeStruct((rows, cols), f32),
            jax.ShapeDtypeStruct((rows, cols), f32),
            jax.ShapeDtypeStruct((8, order), f32),
            jax.ShapeDtypeStruct((8, BLK), f32),
        ),
        in_specs=[smem, smem, vmem, vmem, vmem],
        out_specs=(vmem, vmem, vmem, vmem),
        scratch_shapes=[
            pltpu.VMEM((nx, 2, BLK, BLK), f32), block, pltpu.VMEM((nx, 8, BLK), f32), tile,
            block, block, block, block, block, tile, tiles, tiles,
            wide, tall, wide, tall, tall, wide, tall, wide, tall, wide, wide,
            pltpu.VMEM((8, order), f32), tiles, tiles, tile, tile, pltpu.VMEM((8, order), f32),
            dma((nx - 1,)), dma((nx - 1,)),
            dma((n_plane + n_line,)), dma((2 * nx,)),
            dma((ny - 1,)), dma((ny - 1,)),
            dma((n_plane,)), dma((4, n_plane)),
            dma((nz - 1,)), dma((5, nz - 1)),
            dma((nz,)), dma((5, nz)),
            dma((1,)), dma((1,)),
            dma((n_plane,)), dma((5, n_plane)),
        ],
        compiler_params=pltpu.CompilerParams(
            collective_id=0, has_side_effects=True, vmem_limit_bytes=56 * 1024 * 1024
        ),
    )(bvec_index, weight_table, m_matrices.reshape(m_matrices.shape[1:]), grad_prev, dir_prev)
    return stat[0, 0], stat[1, 0], grad, direction, trial[: 2 * nx].reshape(nx, 2, order)


def solution(mesh):
    nx, ny, nk = mesh.shape["bvec"], mesh.shape["col"], 2
    nz = mesh.shape["row"] // nk
    torus = Mesh(mesh.devices.reshape(nx, nz, nk, ny), ("bvec", "zed", "core", "col"))
    return jax.shard_map(
        functools.partial(shards, (nx, ny, nz, nk)),
        mesh=torus,
        in_specs=(P("bvec", None, ROW, "col"), P(), P(), P(ROW, "col"), P(ROW, "col")),
        out_specs=(P(), P(), P(ROW, "col"), P(ROW, "col"), P()),
        check_vma=False,
    )
```

```python
import functools
import math

import jax
import jax.numpy as jnp
from jax import lax
from jax.experimental import pallas as pl
from jax.experimental.pallas import tpu as pltpu
from jax.sharding import Mesh
from jax.sharding import PartitionSpec as P

ROW = ("zed", "core")
STEP_SCALE = 1.75
BLK = 128
MESH = pl.DeviceIdType.MESH

R177 = math.sqrt(177.0)
X3 = 2.0 / 3.0
X1 = X3 * (1.0 + R177) / 88.0
X2 = X3 * (1.0 + R177) / 352.0
X4 = (-271.0 + 29.0 * R177) / (315.0 * X3)
X5 = 11.0 * (-1.0 + R177) / (1260.0 * X3)
X6 = 11.0 * (-9.0 + R177) / (5040.0 * X3)
X7 = (89.0 - R177) / (5040.0 * X3 * X3)
Y2 = (857.0 - 58.0 * R177) / 630.0


def split(value):
    high = value.astype(jnp.bfloat16)
    low = (value - high.astype(jnp.float32)).astype(jnp.bfloat16)
    return high, low


def dot(left, right):
    return jnp.dot(left, right, preferred_element_type=jnp.float32)


def dot_split(left, right):
    (lh, ll), (rh, rl) = left, right
    return dot(lh, rh) + (dot(lh, rl) + dot(ll, rh))


def kernel(
    dims, idx_ref, tab_ref, m_ref, gp_ref, dp_ref,
    grad_ref, dir_ref, trial_ref, stat_ref,
    mall, dcm, drt, dsrc, gblk, blk2, blk4, eblk, etr, stile, sx, sz,
    drow, dcol, grow, gcol, acol, row2, col2, row4, col4, erow, ej, part, pz, px, qtile, ttile, tfin,
    a2a_s, a2a_r, dia_s, dia_r, dpr_s, dpr_r, row_s, row_r, col_s, col_r, fwd_s, fwd_r, one_s, one_r, sml_s, sml_r,
):
    nx, ny, nz, nk = dims
    count = nx * ny
    order = count * BLK
    wide = nx * BLK
    x, y = lax.axis_index("bvec"), lax.axis_index("col")
    z, k = lax.axis_index("zed"), lax.axis_index("core")
    r = nk * z + k
    c = nx * y + x

    def dev(xx, yy, zz, kk):
        return {"bvec": xx, "zed": zz, "core": kk, "col": yy}

    def off(value, step, size):
        return lax.rem(value + step, size) if step else value

    def lanes(index, size=BLK):
        return pl.ds(pl.multiple_of(index * size, size), size)

    plane = [(ox, oy) for ox in range(nx) for oy in range(ny) if (ox, oy) != (0, 0)]
    line = [(oz, ok) for oz in range(nz) for ok in range(nk)]
    others = line[1:]

    def at_plane(ox, oy):
        return dev(off(x, ox, nx), off(y, oy, ny), z, k)

    def at_line(oz, ok):
        return dev(x, y, off(z, oz, nz), off(k, ok, nk))

    px_t, py_t = lax.rem(r, nx), lax.div(r, nx)
    pz_t, pk_t = lax.div(c, nk), lax.rem(c, nk)
    off_diag = r != c
    holds = y == py_t

    barrier = pltpu.get_barrier_semaphore()
    for ox, oy in plane:
        pl.semaphore_signal(barrier, inc=1, device_id=at_plane(ox, oy), device_id_type=MESH)
    for oz, ok in others:
        pl.semaphore_signal(barrier, inc=1, device_id=at_line(oz, ok), device_id_type=MESH)

    @pl.when(off_diag)
    def _():
        pl.semaphore_signal(barrier, inc=1, device_id=dev(px_t, py_t, pz_t, pk_t), device_id_type=MESH)

    for b in range(nx):
        @pl.when((x != b) | off_diag)
        def _(b=b):
            pl.semaphore_signal(barrier, inc=1, device_id=dev(b, y, pz_t, pk_t), device_id_type=MESH)

    mall[pl.ds(x, 1)] = m_ref[:, :, lanes(x)][None]
    own_d = dp_ref[:, lanes(x)]
    eye_r = lax.broadcasted_iota(jnp.int32, (BLK, BLK), 0)
    eye_c = lax.broadcasted_iota(jnp.int32, (BLK, BLK), 1)
    eye = eye_r == eye_c
    dsrc[...] = jnp.zeros((8, BLK), jnp.float32)
    for p in range(2):
        dsrc[p:p + 1, :] = jnp.sum(jnp.where(eye, m_ref[p, :, lanes(px_t)], 0.0), axis=0, keepdims=True)
    if nx * 8 < BLK:
        dcm[nx * 8:, :] = jnp.zeros((BLK - nx * 8, BLK), jnp.float32)
    drow[:, lanes(y, wide)] = dp_ref[...]
    dcol[lanes(r), :] = own_d

    expected = len(plane) + len(others) + off_diag.astype(jnp.int32)
    asked = len(line) - (x == px_t).astype(jnp.int32)
    with jax.named_scope("barrier"):
        pl.semaphore_wait(barrier, expected + holds.astype(jnp.int32) * asked)

    def remote(src, dst, send, recv, device):
        return pltpu.make_async_remote_copy(
            src_ref=src, dst_ref=dst, send_sem=send, recv_sem=recv, device_id=device, device_id_type=MESH
        )

    dia_row = [
        remote(dsrc, dcm.at[pl.ds(pl.multiple_of(8 * x, 8), 8), :], dia_s.at[i], dia_r.at[x], at_plane(ox, oy))
        for i, (ox, oy) in enumerate(plane)
    ]
    dia_col = [
        remote(dsrc, drt.at[x], dia_s.at[len(plane) + i], dia_r.at[nx + x],
               dev(px_t, y, off(z, oz, nz), off(k, ok, nk)))
        for i, (oz, ok) in enumerate(line)
    ]

    @pl.when(holds)
    def _():
        for copy in dia_row:
            copy.start()
        for copy in dia_col[1:]:
            copy.start()
        dcm[pl.ds(pl.multiple_of(8 * x, 8), 8), :] = dsrc[...]

    @pl.when(holds & (x != px_t))
    def _():
        dia_col[0].start()

    @pl.when(jnp.logical_not(off_diag))
    def _():
        drt[pl.ds(x, 1)] = dsrc[...][None]

    a2a = []
    for ox in range(1, nx):
        xp = off(x, ox, nx)
        copy = remote(m_ref.at[:, :, lanes(xp)], mall.at[x], a2a_s.at[ox - 1], a2a_r.at[ox - 1], dev(xp, y, z, k))
        copy.start()
        a2a.append(copy)

    def wait_all(copies, name="wait"):
        with jax.named_scope(name):
            for copy in copies:
                copy.wait()

    half = BLK // 2
    top, low = slice(0, half), slice(half, BLK)

    def far_block(step, part, index):
        held = drow.at[part, lanes(off(y, ny - step, ny), wide)]
        return remote(held, held, dpr_s.at[index], dpr_r.at[index], at_plane(0, step))

    dprow = []
    for i, oy in enumerate((1, ny - 1)):
        copy = remote(dp_ref, drow.at[:, lanes(y, wide)], dpr_s.at[i], dpr_r.at[i], at_plane(0, oy))
        copy.start()
        dprow.append(copy)

    ring_x = [1, nx - 1, 2]
    ring_y = [1, ny - 1, 2]

    def plane_start(stage, src, dst):
        first = []
        for i, ox in enumerate(ring_x):
            first.append(remote(src, dst.at[:, lanes(c)], row_s.at[i], row_r.at[stage, i], at_plane(ox, 0)))
            first.append(remote(src, dst.at[:, lanes(c)], row_s.at[3 + i], row_r.at[stage, 3 + i], at_plane(0, ring_y[i])))
        for copy in first:
            copy.start()
        return stage, dst, first, []

    def plane_forward(state):
        stage, dst, first, second = state
        with jax.named_scope(f"row{stage}a"):
            for i in range(3):
                first[2 * i].wait_recv()
                held = dst.at[top, lanes(nx * y + off(x, nx - ring_x[i], nx))]
                for j in range(3):
                    at = 6 + 3 * i + j
                    second.append(remote(held, held, row_s.at[at], row_r.at[stage, at], at_plane(0, ring_y[j])))
                    second[-1].start()
                first[2 * i + 1].wait_recv()
                held = dst.at[low, lanes(nx * off(y, ny - ring_y[i], ny) + x)]
                for j in range(3):
                    at = 15 + 3 * i + j
                    second.append(remote(held, held, row_s.at[at], row_r.at[stage, at], at_plane(ring_x[j], 0)))
                    second[-1].start()

    def plane_finish(state):
        stage, _, first, second = state
        with jax.named_scope(f"row{stage}b"):
            for copy in second:
                copy.wait()
            for copy in first:
                copy.wait_send()

    def line_start(stage, src, slot):
        bank = 1 if stage == 0 else 0
        first = {}
        for i, oz in enumerate((1, nz - 1, 2, nz - 2)):
            first[oz] = remote(src, slot(r), col_s.at[bank, i], col_r.at[stage, i], at_line(oz, 0))
            first[oz].start()
        over = [remote(src, slot(r), fwd_s.at[bank, 0], fwd_r.at[stage, 0], at_line(0, 1))]
        over[0].start()
        return stage, bank, slot, first, {}, over

    def line_across(state, oz):
        stage, bank, slot, first, second, over = state
        held = slot(nk * off(z, nz - oz, nz) + k)
        over.append(remote(held, held, fwd_s.at[bank, oz], fwd_r.at[stage, oz], at_line(0, 1)))
        over[-1].start()

    def line_forward(state):
        stage, bank, slot, first, second, over = state
        with jax.named_scope(f"line{stage}a"):
            for i, (oz, step, part) in enumerate(((2, 1, top), (nz - 2, nz - 1, low))):
                first[oz].wait_recv()
                held = slot(nk * off(z, nz - oz, nz) + k)
                second[i] = remote(held, held, col_s.at[bank, 4 + i], col_r.at[stage, 4 + i], at_line(step, 0))
                second[i].start()
                held = slot(nk * off(z, nz - oz, nz) + k, part)
                second[2 + i] = remote(held, held, col_s.at[bank, 6 + i], col_r.at[stage, 6 + i], at_line(oz, 0))
                second[2 + i].start()
            for oz in (1, nz - 1, 2, nz - 2):
                if oz in (1, nz - 1):
                    first[oz].wait_recv()
                line_across(state, oz)

    def line_finish(state):
        stage, bank, slot, first, second, over = state
        with jax.named_scope(f"line{stage}b"):
            second[0].wait_recv()
            line_across(state, 3)
            second[1].wait_recv()
            line_across(state, nz - 3)
            second[2].wait_recv()
            second[3].wait_recv()
            line_across(state, 4)
            for copy in over:
                copy.wait()
            for copy in list(first.values()) + list(second.values()):
                copy.wait_send()

    def column_slots(ref):
        def slot(index, part=slice(0, BLK)):
            return ref.at[pl.ds(pl.multiple_of(index * BLK + part.start, half), part.stop - part.start), :]
        return slot

    def row_slots(ref):
        return lambda index, part=slice(0, BLK): ref.at[part, lanes(index)]

    d_col = line_start(0, dp_ref.at[:, lanes(x)], column_slots(dcol))

    for b in range(nx):
        @pl.when(jnp.logical_not(holds & (x == b)))
        @jax.named_scope("diag_r")
        def _(b=b):
            slot = dcm.at[8 * b:8 * b + 8, :]
            remote(slot, slot, dia_s.at[0], dia_r.at[b], dev(x, y, z, k)).wait_recv()

        @pl.when(off_diag | (x != b))
        def _(b=b):
            slot = drt.at[b]
            remote(slot, slot, dia_s.at[0], dia_r.at[nx + b], dev(x, y, z, k)).wait_recv()

    weights = []
    for b in range(nx):
        value = jnp.float32(0.0)
        for t in range(tab_ref.shape[0]):
            value = value + jnp.where(idx_ref[b] == t, tab_ref[t], jnp.float32(0.0))
        weights.append(value)

    columns = jnp.transpose(dcm[...])
    line_forward(d_col)
    far = []
    for i, (step, piece) in enumerate(((1, top), (ny - 1, low))):
        dprow[i].wait_recv()
        far.append(far_block(step, piece, 2 + i))
        far[-1].start()
    wait_all(a2a, "a2a")
    total = jnp.zeros((BLK, BLK), jnp.float32)
    spread_row = jnp.zeros((1, BLK), jnp.float32)
    for b in range(nx):
        term = jnp.zeros((BLK, BLK), jnp.float32)
        for p in range(2):
            at_row = columns[:, 8 * b + p:8 * b + p + 1]
            at_col = drt[b, p:p + 1, :]
            term = term + mall[b, p] * (at_row - at_col)
        total = total + (2.0 * weights[b]) * term
        re_d, im_d = drt[b, 0:1, :], drt[b, 1:2, :]
        spread_row = spread_row + weights[b] * (1.0 - re_d * re_d - im_d * im_d)
    gblk[...] = total
    own_p = gp_ref[:, lanes(x)]
    first_line = (r == 0).astype(jnp.float32)
    stile[...] = jnp.zeros((8, BLK), jnp.float32)
    stile[0:1, :] = jnp.sum(total * total, axis=0, keepdims=True)
    stile[1:2, :] = jnp.sum(total * own_d, axis=0, keepdims=True)
    stile[2:3, :] = jnp.sum(own_d * own_d, axis=0, keepdims=True)
    stile[3:4, :] = jnp.sum(own_p * own_p, axis=0, keepdims=True)
    stile[4:5, :] = spread_row * first_line

    def small_plane(stage, src, dst):
        dst[pl.ds(c, 1)] = src[...][None]
        copies = []
        for i, (ox, oy) in enumerate(plane):
            copy = remote(src, dst.at[c], sml_s.at[i], sml_r.at[stage, i], at_plane(ox, oy))
            copy.start()
            copies.append(copy)
        return copies

    def small_line(stage, src, dst):
        dst[pl.ds(r, 1)] = src(r)[...][None]
        copies = []
        for i, (oz, ok) in enumerate(others):
            rp = nk * off(z, oz, nz) + off(k, ok, nk)
            copy = remote(src(rp), dst.at[r], sml_s.at[i], sml_r.at[stage, i], at_line(oz, ok))
            copy.start()
            copies.append(copy)
        return copies

    def summed(ref):
        value = ref[0]
        for i in range(1, count):
            value = value + ref[i]
        return value

    copies = small_line(0, lambda index: stile, sx)
    grow[:, lanes(c)] = total
    gcol[lanes(r), :] = total
    rows = plane_start(0, gblk, grow)
    cols = line_start(1, gblk, column_slots(gcol))
    line_finish(d_col)
    plane_forward(rows)
    line_forward(cols)
    wait_all(copies, "small0")
    stile[...] = summed(sx)
    copies = small_plane(1, stile, sz)
    wait_all(far, "far")
    for copy in dprow:
        copy.wait_send()
    line_finish(cols)
    plane_finish(rows)
    wait_all(copies, "small1")
    sums = jnp.broadcast_to(jnp.sum(summed(sz), axis=1, keepdims=True), (8, BLK))
    gg, gd, dd, pp = (sums[i:i + 1, :] for i in range(4))
    spread = sums[4:5, :] / order
    beta = gg / (1.0 + pp)
    norm = jnp.maximum(gg - 2.0 * beta * gd + beta * beta * dd, 0.0)
    scale = STEP_SCALE / jnp.sqrt(1.0 + norm / order)

    for j in range(nx):
        at = pl.ds(pl.multiple_of(y * wide + j * BLK, BLK), BLK)
        piece = grow[:, at]
        grad_ref[:, j * BLK:(j + 1) * BLK] = piece
        dir_ref[:, j * BLK:(j + 1) * BLK] = beta * drow[:, at] - piece

    chunk = 4 * BLK if order % (4 * BLK) == 0 else BLK
    beta_w = jnp.concatenate([beta] * (chunk // BLK), axis=1)
    scale_w = jnp.concatenate([scale] * (chunk // BLK), axis=1)

    acc = jnp.zeros((BLK, BLK), jnp.float32)
    for at in range(0, order, chunk):
        left = scale_w * (beta_w * drow[:, at:at + chunk] - grow[:, at:at + chunk])
        right = scale * (beta * dcol[at:at + chunk, :] - gcol[at:at + chunk, :])
        acol[at:at + chunk, :] = right
        acc = acc + dot_split(split(left), split(right))
    blk2[...] = acc
    row2[:, lanes(c)] = acc
    col2[lanes(r), :] = acc
    rows = plane_start(1, blk2, row2)
    cols = line_start(2, blk2, column_slots(col2))
    line_forward(cols)
    plane_forward(rows)
    line_finish(cols)
    plane_finish(rows)

    acc = jnp.zeros((BLK, BLK), jnp.float32)
    for at in range(0, order, chunk):
        right = X1 * acol[at:at + chunk, :] + X2 * col2[at:at + chunk, :]
        acc = acc + dot_split(split(row2[:, at:at + chunk]), split(right))
    blk4[...] = acc
    row4[:, lanes(c)] = acc
    col4[lanes(r), :] = acc
    rows = plane_start(2, blk4, row4)
    cols = line_start(3, blk4, column_slots(col4))
    line_forward(cols)
    plane_forward(rows)
    line_finish(cols)
    plane_finish(rows)

    acc = jnp.zeros((BLK, BLK), jnp.float32)
    for at in range(0, order, chunk):
        left = X3 * row2[:, at:at + chunk] + row4[:, at:at + chunk]
        right = X5 * acol[at:at + chunk, :] + X6 * col2[at:at + chunk, :] + X7 * col4[at:at + chunk, :]
        acc = acc + dot_split(split(left), split(right))
    acc = acc + X4 * (X3 * blk2[...] + blk4[...]) + Y2 * blk2[...] + acol[lanes(r), :]
    acc = acc + jnp.where(eye & jnp.logical_not(off_diag), 1.0, 0.0)
    eblk[...] = acc

    turn = remote(eblk, etr, one_s.at[0], one_r.at[0], dev(px_t, py_t, pz_t, pk_t))

    @pl.when(off_diag)
    def _():
        turn.start()

    erow[:, lanes(c)] = acc
    rows = plane_start(3, eblk, erow)

    @pl.when(off_diag)
    def _():
        with jax.named_scope("turn"):
            turn.wait()

    @pl.when(jnp.logical_not(off_diag))
    def _():
        etr[...] = eblk[...]

    cols = line_start(4, etr, row_slots(ej))
    ej[:, lanes(r)] = etr[...]
    pairs = [[split(mall[b, p]) for p in range(2)] for b in range(nx)]
    plane_forward(rows)
    line_forward(cols)
    line_finish(cols)
    plane_finish(rows)

    part[...] = jnp.zeros((8, order), jnp.float32)
    for at in range(0, order, chunk):
        right = split(ej[:, at:at + chunk])
        left = erow[:, at:at + chunk]
        for b in range(nx):
            for p in range(2):
                turned = dot_split(pairs[b][p], right)
                part[2 * b + p:2 * b + p + 1, at:at + chunk] = jnp.sum(left * turned, axis=0, keepdims=True)

    wait_all(small_line(2, lambda index: part.at[:, lanes(index)], pz), "small2")
    qtile[...] = summed(pz)
    wait_all(small_plane(3, qtile, px), "small3")
    sumt = summed(px)
    ttile[...] = sumt
    tfin[:, lanes(r)] = sumt
    copies = []
    for i, (oz, ok) in enumerate(others):
        copy = remote(ttile, tfin.at[:, lanes(r)], sml_s.at[i], sml_r.at[4, i], at_line(oz, ok))
        copy.start()
        copies.append(copy)

    @pl.when(holds)
    def _():
        for copy in dia_row:
            copy.wait_send()
        for copy in dia_col[1:]:
            copy.wait_send()

    @pl.when(holds & (x != px_t))
    def _():
        dia_col[0].wait_send()

    wait_all(copies, "small4")
    trial_ref[...] = tfin[...]
    trial = jnp.zeros((1, order), jnp.float32)
    for b in range(nx):
        re_t, im_t = tfin[2 * b:2 * b + 1, :], tfin[2 * b + 1:2 * b + 2, :]
        trial = trial + weights[b] * (1.0 - re_t * re_t - im_t * im_t)
    stat_ref[...] = jnp.zeros((8, BLK), jnp.float32)
    stat_ref[0:1, :] = spread
    stat_ref[1:2, :] = jnp.broadcast_to(jnp.sum(trial, axis=1, keepdims=True) / order, (1, BLK))


def shards(dims, m_matrices, bvec_index, weight_table, grad_prev, dir_prev):
    nx, ny, nz, nk = dims
    count = nx * ny
    order = count * BLK
    f32 = jnp.float32
    rows, cols = grad_prev.shape
    vmem = pl.BlockSpec(memory_space=pltpu.VMEM)
    smem = pl.BlockSpec(memory_space=pltpu.SMEM)
    wide = pltpu.VMEM((BLK, order), f32)
    tall = pltpu.VMEM((order, BLK), f32)
    block = pltpu.VMEM((BLK, BLK), f32)
    tile = pltpu.VMEM((8, BLK), f32)
    tiles = pltpu.VMEM((count, 8, BLK), f32)
    dma = pltpu.SemaphoreType.DMA
    n_plane, n_line = count - 1, nz * nk
    grad, direction, trial, stat = pl.pallas_call(
        functools.partial(kernel, dims),
        out_shape=(
            jax.ShapeDtypeStruct((rows, cols), f32),
            jax.ShapeDtypeStruct((rows, cols), f32),
            jax.ShapeDtypeStruct((8, order), f32),
            jax.ShapeDtypeStruct((8, BLK), f32),
        ),
        in_specs=[smem, smem, vmem, vmem, vmem],
        out_specs=(vmem, vmem, vmem, vmem),
        scratch_shapes=[
            pltpu.VMEM((nx, 2, BLK, BLK), f32), block, pltpu.VMEM((nx, 8, BLK), f32), tile,
            block, block, block, block, block, tile, tiles, tiles,
            wide, tall, wide, tall, tall, wide, tall, wide, tall, wide, wide,
            pltpu.VMEM((8, order), f32), tiles, tiles, tile, tile, pltpu.VMEM((8, order), f32),
            dma((nx - 1,)), dma((nx - 1,)),
            dma((n_plane + n_line,)), dma((2 * nx,)),
            dma((4,)), dma((4,)),
            dma((24,)), dma((4, 24)),
            dma((2, 8)), dma((5, 8)),
            dma((2, nz)), dma((5, nz)),
            dma((1,)), dma((1,)),
            dma((n_plane,)), dma((5, n_plane)),
        ],
        compiler_params=pltpu.CompilerParams(
            collective_id=0, has_side_effects=True, vmem_limit_bytes=56 * 1024 * 1024
        ),
    )(bvec_index, weight_table, m_matrices.reshape(m_matrices.shape[1:]), grad_prev, dir_prev)
    return stat[0, 0], stat[1, 0], grad, direction, trial[: 2 * nx].reshape(nx, 2, order)


def solution(mesh):
    nx, ny, nk = mesh.shape["bvec"], mesh.shape["col"], 2
    nz = mesh.shape["row"] // nk
    torus = Mesh(mesh.devices.reshape(nx, nz, nk, ny), ("bvec", "zed", "core", "col"))
    return jax.shard_map(
        functools.partial(shards, (nx, ny, nz, nk)),
        mesh=torus,
        in_specs=(P("bvec", None, ROW, "col"), P(), P(), P(ROW, "col"), P(ROW, "col")),
        out_specs=(P(), P(), P(ROW, "col"), P(ROW, "col"), P()),
        check_vma=False,
    )
```

```python
import functools
import math

import jax
import jax.numpy as jnp
from jax import lax
from jax.experimental import pallas as pl
from jax.experimental.pallas import tpu as pltpu
from jax.sharding import Mesh
from jax.sharding import PartitionSpec as P

ROW = ("zed", "core")
STEP_SCALE = 1.75
BLK = 128
MESH = pl.DeviceIdType.MESH

R177 = math.sqrt(177.0)
X3 = 2.0 / 3.0
X1 = X3 * (1.0 + R177) / 88.0
X2 = X3 * (1.0 + R177) / 352.0
X4 = (-271.0 + 29.0 * R177) / (315.0 * X3)
X5 = 11.0 * (-1.0 + R177) / (1260.0 * X3)
X6 = 11.0 * (-9.0 + R177) / (5040.0 * X3)
X7 = (89.0 - R177) / (5040.0 * X3 * X3)
Y2 = (857.0 - 58.0 * R177) / 630.0


def split(value):
    high = value.astype(jnp.bfloat16)
    low = (value - high.astype(jnp.float32)).astype(jnp.bfloat16)
    return high, low


def dot(left, right):
    return jnp.dot(left, right, preferred_element_type=jnp.float32)


def dot_split(left, right):
    (lh, ll), (rh, rl) = left, right
    size = rh.shape[1]
    both = dot(lh, jnp.concatenate([rh, rl], axis=1))
    return both[:, :size] + (both[:, size:] + dot(ll, rh))


def kernel(
    dims, m_in, dp_in, gp_in, idx_in, tab_in,
    grad_ref, dir_ref, tfin, stat_ref,
    idx_ref, tab_ref, m_ref, gp_ref, dp_ref, in_s,
    mall, dcm, drt, dsrc, gblk, blk2, blk4, eblk, etr, stile, sx, sz,
    drow, dcol, grow, gcol, acol, row2, col2, row4, col4, erow, ej, mt, turned, part, pz, px, qtile, ttile,
    a2a_s, a2a_r, dia_s, dia_r, dpr_s, dpr_r, row_s, row_r, col_s, col_r, fwd_s, fwd_r, one_s, one_r, sml_s, sml_r, pz_s, pz_r,
):
    nx, ny, nz, nk = dims
    count = nx * ny
    order = count * BLK
    wide = nx * BLK
    x, y = lax.axis_index("bvec"), lax.axis_index("col")
    z, k = lax.axis_index("zed"), lax.axis_index("core")
    r = nk * z + k
    c = nx * y + x

    def dev(xx, yy, zz, kk):
        return {"bvec": xx, "zed": zz, "core": kk, "col": yy}

    def off(value, step, size):
        return lax.rem(value + step, size) if step else value

    def lanes(index, size=BLK):
        return pl.ds(pl.multiple_of(index * size, size), size)

    plane = [(ox, oy) for ox in range(nx) for oy in range(ny) if (ox, oy) != (0, 0)]
    line = [(oz, ok) for oz in range(nz) for ok in range(nk)]
    others = line[1:]

    def at_plane(ox, oy):
        return dev(off(x, ox, nx), off(y, oy, ny), z, k)

    def at_line(oz, ok):
        return dev(x, y, off(z, oz, nz), off(k, ok, nk))

    px_t, py_t = lax.rem(r, nx), lax.div(r, nx)
    pz_t, pk_t = lax.div(c, nk), lax.rem(c, nk)
    off_diag = r != c
    holds = y == py_t

    loads = [
        pltpu.make_async_copy(src, dst, in_s.at[i])
        for i, (src, dst) in enumerate(
            ((m_in, m_ref), (dp_in, dp_ref), (gp_in, gp_ref), (idx_in, idx_ref), (tab_in, tab_ref))
        )
    ]
    for copy in loads:
        copy.start()

    barrier = pltpu.get_barrier_semaphore()
    for ox, oy in plane:
        pl.semaphore_signal(barrier, inc=1, device_id=at_plane(ox, oy), device_id_type=MESH)
    for oz, ok in others:
        pl.semaphore_signal(barrier, inc=1, device_id=at_line(oz, ok), device_id_type=MESH)

    for b in range(nx):
        @pl.when((x != b) | off_diag)
        def _(b=b):
            pl.semaphore_signal(barrier, inc=1, device_id=dev(b, y, pz_t, pk_t), device_id_type=MESH)

    for copy in loads:
        copy.wait()

    mall[pl.ds(x, 1)] = m_ref[:, :, lanes(x)][None]
    own_d = dp_ref[:, lanes(x)]
    eye_r = lax.broadcasted_iota(jnp.int32, (BLK, BLK), 0)
    eye_c = lax.broadcasted_iota(jnp.int32, (BLK, BLK), 1)
    eye = eye_r == eye_c
    dsrc[...] = jnp.zeros((8, BLK), jnp.float32)
    for p in range(2):
        dsrc[p:p + 1, :] = jnp.sum(jnp.where(eye, m_ref[p, :, lanes(px_t)], 0.0), axis=0, keepdims=True)
    if nx * 8 < BLK:
        dcm[nx * 8:, :] = jnp.zeros((BLK - nx * 8, BLK), jnp.float32)
    drow[:, lanes(y, wide)] = dp_ref[...]
    dcol[lanes(r), :] = own_d

    expected = len(plane) + len(others)
    asked = len(line) - (x == px_t).astype(jnp.int32)
    with jax.named_scope("barrier"):
        pl.semaphore_wait(barrier, expected + holds.astype(jnp.int32) * asked)

    def remote(src, dst, send, recv, device):
        return pltpu.make_async_remote_copy(
            src_ref=src, dst_ref=dst, send_sem=send, recv_sem=recv, device_id=device, device_id_type=MESH
        )

    dia_row = [
        remote(dsrc, dcm.at[pl.ds(pl.multiple_of(8 * x, 8), 8), :], dia_s.at[i], dia_r.at[x], at_plane(ox, oy))
        for i, (ox, oy) in enumerate(plane)
    ]
    dia_col = [
        remote(dsrc, drt.at[x], dia_s.at[len(plane) + i], dia_r.at[nx + x],
               dev(px_t, y, off(z, oz, nz), off(k, ok, nk)))
        for i, (oz, ok) in enumerate(line)
    ]

    @pl.when(holds)
    def _():
        for copy in dia_row:
            copy.start()
        for copy in dia_col[1:]:
            copy.start()
        dcm[pl.ds(pl.multiple_of(8 * x, 8), 8), :] = dsrc[...]

    @pl.when(holds & (x != px_t))
    def _():
        dia_col[0].start()

    @pl.when(jnp.logical_not(off_diag))
    def _():
        drt[pl.ds(x, 1)] = dsrc[...][None]

    a2a = []
    for ox in range(1, nx):
        xp = off(x, ox, nx)
        copy = remote(m_ref.at[:, :, lanes(xp)], mall.at[x], a2a_s.at[ox - 1], a2a_r.at[ox - 1], dev(xp, y, z, k))
        copy.start()
        a2a.append(copy)

    def wait_all(copies, name="wait"):
        with jax.named_scope(name):
            for copy in copies:
                copy.wait()

    half = BLK // 2
    top, low = slice(0, half), slice(half, BLK)

    def far_block(step, part, index):
        held = drow.at[part, lanes(off(y, ny - step, ny), wide)]
        return remote(held, held, dpr_s.at[index], dpr_r.at[index], at_plane(0, step))

    dprow = []
    for i, oy in enumerate((1, ny - 1)):
        copy = remote(dp_ref, drow.at[:, lanes(y, wide)], dpr_s.at[i], dpr_r.at[i], at_plane(0, oy))
        copy.start()
        dprow.append(copy)

    ring_x = [1, nx - 1, 2]
    ring_y = [1, ny - 1, 2]

    def plane_start(stage, src, dst):
        first = []
        for i, ox in enumerate(ring_x):
            first.append(remote(src, dst.at[:, lanes(c)], row_s.at[i], row_r.at[stage, i], at_plane(ox, 0)))
            first.append(remote(src, dst.at[:, lanes(c)], row_s.at[3 + i], row_r.at[stage, 3 + i], at_plane(0, ring_y[i])))
        for copy in first:
            copy.start()
        return stage, dst, first, []

    def plane_forward(state):
        stage, dst, first, second = state
        with jax.named_scope(f"row{stage}a"):
            for i in range(3):
                first[2 * i].wait_recv()
                held = dst.at[top, lanes(nx * y + off(x, nx - ring_x[i], nx))]
                for j in range(3):
                    at = 6 + 3 * i + j
                    second.append(remote(held, held, row_s.at[at], row_r.at[stage, at], at_plane(0, ring_y[j])))
                    second[-1].start()
                first[2 * i + 1].wait_recv()
                held = dst.at[low, lanes(nx * off(y, ny - ring_y[i], ny) + x)]
                for j in range(3):
                    at = 15 + 3 * i + j
                    second.append(remote(held, held, row_s.at[at], row_r.at[stage, at], at_plane(ring_x[j], 0)))
                    second[-1].start()

    def plane_finish(state):
        stage, _, first, second = state
        with jax.named_scope(f"row{stage}b"):
            for copy in second:
                copy.wait()
            for copy in first:
                copy.wait_send()

    def line_start(stage, src, slot):
        bank = 1 if stage == 0 else 0
        first = {}
        for i, oz in enumerate((2, nz - 2, 1, nz - 1)):
            first[oz] = remote(src, slot(r), col_s.at[bank, i], col_r.at[stage, i], at_line(oz, 0))
            first[oz].start()
        over = [remote(src, slot(r), fwd_s.at[bank, 0], fwd_r.at[stage, 0], at_line(0, 1))]
        over[0].start()
        return stage, bank, slot, first, {}, over

    def line_across(state, oz):
        stage, bank, slot, first, second, over = state
        held = slot(nk * off(z, nz - oz, nz) + k)
        over.append(remote(held, held, fwd_s.at[bank, oz], fwd_r.at[stage, oz], at_line(0, 1)))
        over[-1].start()

    def line_forward(state):
        stage, bank, slot, first, second, over = state
        with jax.named_scope(f"line{stage}a"):
            for i, (oz, step, part) in enumerate(((2, 1, top), (nz - 2, nz - 1, low))):
                first[oz].wait_recv()
                held = slot(nk * off(z, nz - oz, nz) + k)
                second[i] = remote(held, held, col_s.at[bank, 4 + i], col_r.at[stage, 4 + i], at_line(step, 0))
                second[i].start()
                held = slot(nk * off(z, nz - oz, nz) + k, part)
                second[2 + i] = remote(held, held, col_s.at[bank, 6 + i], col_r.at[stage, 6 + i], at_line(oz, 0))
                second[2 + i].start()

    def line_near(state):
        stage, bank, slot, first, second, over = state
        with jax.named_scope(f"line{stage}n"):
            for oz in (2, nz - 2, 1, nz - 1):
                if oz in (1, nz - 1):
                    first[oz].wait_recv()
                line_across(state, oz)

    def line_finish(state):
        stage, bank, slot, first, second, over = state
        with jax.named_scope(f"line{stage}b"):
            second[0].wait_recv()
            line_across(state, 3)
            second[1].wait_recv()
            line_across(state, nz - 3)
            second[2].wait_recv()
            second[3].wait_recv()
            line_across(state, 4)
            for copy in over:
                copy.wait()
            for copy in list(first.values()) + list(second.values()):
                copy.wait_send()

    def column_slots(ref):
        def slot(index, part=slice(0, BLK)):
            return ref.at[pl.ds(pl.multiple_of(index * BLK + part.start, half), part.stop - part.start), :]
        return slot

    def row_slots(ref):
        return lambda index, part=slice(0, BLK): ref.at[part, lanes(index)]

    d_col = line_start(0, dp_ref.at[:, lanes(x)], column_slots(dcol))

    for b in range(nx):
        @pl.when(jnp.logical_not(holds & (x == b)))
        @jax.named_scope("diag_r")
        def _(b=b):
            slot = dcm.at[8 * b:8 * b + 8, :]
            remote(slot, slot, dia_s.at[0], dia_r.at[b], dev(x, y, z, k)).wait_recv()

        @pl.when(off_diag | (x != b))
        def _(b=b):
            slot = drt.at[b]
            remote(slot, slot, dia_s.at[0], dia_r.at[nx + b], dev(x, y, z, k)).wait_recv()

    weights = []
    for b in range(nx):
        value = jnp.float32(0.0)
        for t in range(tab_ref.shape[0]):
            value = value + jnp.where(idx_ref[b] == t, tab_ref[t], jnp.float32(0.0))
        weights.append(value)

    columns = jnp.transpose(dcm[...])
    line_forward(d_col)
    line_near(d_col)
    far = []
    for i, (step, piece) in enumerate(((1, top), (ny - 1, low))):
        dprow[i].wait_recv()
        far.append(far_block(step, piece, 2 + i))
        far[-1].start()
    wait_all(a2a, "a2a")
    total = jnp.zeros((BLK, BLK), jnp.float32)
    spread_row = jnp.zeros((1, BLK), jnp.float32)
    for b in range(nx):
        term = jnp.zeros((BLK, BLK), jnp.float32)
        for p in range(2):
            at_row = columns[:, 8 * b + p:8 * b + p + 1]
            at_col = drt[b, p:p + 1, :]
            term = term + mall[b, p] * (at_row - at_col)
        total = total + (2.0 * weights[b]) * term
        re_d, im_d = drt[b, 0:1, :], drt[b, 1:2, :]
        spread_row = spread_row + weights[b] * (1.0 - re_d * re_d - im_d * im_d)
    gblk[...] = total
    own_p = gp_ref[:, lanes(x)]
    first_line = (r == 0).astype(jnp.float32)
    stile[...] = jnp.zeros((8, BLK), jnp.float32)
    stile[0:1, :] = jnp.sum(total * total, axis=0, keepdims=True)
    stile[1:2, :] = jnp.sum(total * own_d, axis=0, keepdims=True)
    stile[2:3, :] = jnp.sum(own_d * own_d, axis=0, keepdims=True)
    stile[3:4, :] = jnp.sum(own_p * own_p, axis=0, keepdims=True)
    stile[4:5, :] = spread_row * first_line

    def small_plane(stage, src, dst):
        dst[pl.ds(c, 1)] = src[...][None]
        copies = []
        for i, (ox, oy) in enumerate(plane):
            copy = remote(src, dst.at[c], sml_s.at[i], sml_r.at[stage, i], at_plane(ox, oy))
            copy.start()
            copies.append(copy)
        return copies

    def small_line(stage, src, dst):
        dst[pl.ds(r, 1)] = src(r)[...][None]
        copies = []
        for i, (oz, ok) in enumerate(others):
            rp = nk * off(z, oz, nz) + off(k, ok, nk)
            copy = remote(src(rp), dst.at[r], sml_s.at[i], sml_r.at[stage, i], at_line(oz, ok))
            copy.start()
            copies.append(copy)
        return copies

    def summed(ref):
        value = ref[0]
        for i in range(1, count):
            value = value + ref[i]
        return value

    copies = small_line(0, lambda index: stile, sx)
    grow[:, lanes(c)] = total
    gcol[lanes(r), :] = total
    rows = plane_start(0, gblk, grow)
    cols = line_start(1, gblk, column_slots(gcol))
    line_forward(cols)
    plane_forward(rows)
    line_near(cols)
    line_finish(d_col)
    wait_all(copies, "small0")
    stile[...] = summed(sx)
    copies = small_plane(1, stile, sz)
    wait_all(far, "far")
    for copy in dprow:
        copy.wait_send()
    line_finish(cols)
    plane_finish(rows)
    wait_all(copies, "small1")
    sums = jnp.broadcast_to(jnp.sum(summed(sz), axis=1, keepdims=True), (8, BLK))
    gg, gd, dd, pp = (sums[i:i + 1, :] for i in range(4))
    spread = sums[4:5, :] / order
    beta = gg / (1.0 + pp)
    norm = jnp.maximum(gg - 2.0 * beta * gd + beta * beta * dd, 0.0)
    scale = STEP_SCALE / jnp.sqrt(1.0 + norm / order)

    for j in range(nx):
        at = pl.ds(pl.multiple_of(y * wide + j * BLK, BLK), BLK)
        piece = grow[:, at]
        grad_ref[:, j * BLK:(j + 1) * BLK] = piece
        dir_ref[:, j * BLK:(j + 1) * BLK] = beta * drow[:, at] - piece

    chunk = 4 * BLK if order % (4 * BLK) == 0 else BLK
    beta_w = jnp.concatenate([beta] * (chunk // BLK), axis=1)
    scale_w = jnp.concatenate([scale] * (chunk // BLK), axis=1)

    acc = jnp.zeros((BLK, BLK), jnp.float32)
    for at in range(0, order, chunk):
        left = scale_w * (beta_w * drow[:, at:at + chunk] - grow[:, at:at + chunk])
        right = scale * (beta * dcol[at:at + chunk, :] - gcol[at:at + chunk, :])
        acol[at:at + chunk, :] = right
        acc = acc + dot_split(split(left), split(right))
    blk2[...] = acc
    row2[:, lanes(c)] = acc
    col2[lanes(r), :] = acc
    rows = plane_start(1, blk2, row2)
    cols = line_start(2, blk2, column_slots(col2))
    for b in range(nx):
        for p in range(2):
            i = 2 * b + p
            high, tail = split(jnp.transpose(mall[b, p]))
            mt[i * BLK:(i + 1) * BLK, :] = jnp.concatenate([high, tail], axis=1)
    line_forward(cols)
    plane_forward(rows)
    line_near(cols)
    line_finish(cols)
    plane_finish(rows)

    acc = jnp.zeros((BLK, BLK), jnp.float32)
    for at in range(0, order, chunk):
        right = X1 * acol[at:at + chunk, :] + X2 * col2[at:at + chunk, :]
        acc = acc + dot_split(split(row2[:, at:at + chunk]), split(right))
    blk4[...] = acc
    row4[:, lanes(c)] = acc
    col4[lanes(r), :] = acc
    rows = plane_start(2, blk4, row4)
    cols = line_start(3, blk4, column_slots(col4))
    for at in range(0, order, chunk):
        grow[:, at:at + chunk] = X3 * row2[:, at:at + chunk]
        gcol[at:at + chunk, :] = X5 * acol[at:at + chunk, :] + X6 * col2[at:at + chunk, :]
    line_forward(cols)
    plane_forward(rows)
    line_near(cols)
    line_finish(cols)
    plane_finish(rows)

    acc = jnp.zeros((BLK, BLK), jnp.float32)
    for at in range(0, order, chunk):
        left = grow[:, at:at + chunk] + row4[:, at:at + chunk]
        right = gcol[at:at + chunk, :] + X7 * col4[at:at + chunk, :]
        acc = acc + dot_split(split(left), split(right))
    acc = acc + X4 * (X3 * blk2[...] + blk4[...]) + Y2 * blk2[...] + acol[lanes(r), :]
    acc = acc + jnp.where(eye & jnp.logical_not(off_diag), 1.0, 0.0)
    eblk[...] = acc

    turn = remote(eblk, etr, one_s.at[0], one_r.at[0], dev(px_t, py_t, pz_t, pk_t))

    @pl.when(off_diag)
    def _():
        turn.start()

    erow[:, lanes(c)] = acc
    rows = plane_start(3, eblk, erow)

    @pl.when(off_diag)
    def _():
        with jax.named_scope("turn"):
            turn.wait()

    @pl.when(jnp.logical_not(off_diag))
    def _():
        etr[...] = eblk[...]

    cols = line_start(4, etr, row_slots(ej))
    ej[:, lanes(r)] = etr[...]
    plane_forward(rows)
    line_forward(cols)
    line_near(cols)
    plane_finish(rows)
    for at in range(0, order, chunk):
        high, tail = split(erow[:, at:at + chunk])
        turned[:, at:at + chunk] = dot(mt[...], jnp.concatenate([high, high], axis=0)) + dot(mt[:, :BLK], tail)
    line_finish(cols)

    def to_owner(j):
        return remote(part.at[:, j * BLK:(j + 1) * BLK], pz.at[r], pz_s.at[j], pz_r.at[r], dev(x, y, j // nk, j % nk))

    for at in range(0, order, chunk):
        left = ej[:, at:at + chunk]
        for i in range(2 * nx):
            part[i:i + 1, at:at + chunk] = jnp.sum(
                left * turned[i * BLK:(i + 1) * BLK, at:at + chunk], axis=0, keepdims=True
            )
        for j in range(at // BLK, (at + chunk) // BLK):
            @pl.when(r != j)
            def _(j=j):
                to_owner(j).start()

    pz[pl.ds(r, 1)] = part[:, lanes(r)][None]
    with jax.named_scope("small2"):
        for oz, ok in others:
            rp = nk * off(z, oz, nz) + off(k, ok, nk)
            remote(pz.at[rp], pz.at[rp], pz_s.at[0], pz_r.at[rp], at_line(oz, ok)).wait_recv()
    qtile[...] = summed(pz)
    wait_all(small_plane(3, qtile, px), "small3")
    sumt = summed(px)
    ttile[...] = sumt
    tfin[:, lanes(r)] = sumt
    copies = []
    for i, (oz, ok) in enumerate(others):
        copy = remote(ttile, tfin.at[:, lanes(r)], sml_s.at[i], sml_r.at[4, i], at_line(oz, ok))
        copy.start()
        copies.append(copy)

    @pl.when(holds)
    def _():
        for copy in dia_row:
            copy.wait_send()
        for copy in dia_col[1:]:
            copy.wait_send()

    @pl.when(holds & (x != px_t))
    def _():
        dia_col[0].wait_send()

    for j in range(count):
        @pl.when(r != j)
        def _(j=j):
            to_owner(j).wait_send()

    wait_all(copies, "small4")
    trial = jnp.zeros((1, order), jnp.float32)
    for b in range(nx):
        re_t, im_t = tfin[2 * b:2 * b + 1, :], tfin[2 * b + 1:2 * b + 2, :]
        trial = trial + weights[b] * (1.0 - re_t * re_t - im_t * im_t)
    stat_ref[...] = jnp.zeros((8, BLK), jnp.float32)
    stat_ref[0:1, :] = spread
    stat_ref[1:2, :] = jnp.broadcast_to(jnp.sum(trial, axis=1, keepdims=True) / order, (1, BLK))


def hand_out(grad_ref, dir_ref, trial_ref, stat_ref, spread_out, trial_spread_out, grad_out, dir_out, trial_out):
    spread_out[0, 0] = jnp.sum(stat_ref[0:1, 0:1])
    trial_spread_out[0, 0] = jnp.sum(stat_ref[1:2, 0:1])
    grad_out[...] = grad_ref[...]
    dir_out[...] = dir_ref[...]
    for b in range(trial_out.shape[0]):
        trial_out[b] = trial_ref[2 * b:2 * b + 2, :]


def shards(dims, m_matrices, bvec_index, weight_table, grad_prev, dir_prev):
    nx, ny, nz, nk = dims
    count = nx * ny
    order = count * BLK
    f32 = jnp.float32
    rows, cols = grad_prev.shape
    vmem = pl.BlockSpec(memory_space=pltpu.VMEM)
    smem = pl.BlockSpec(memory_space=pltpu.SMEM)
    wide = pltpu.VMEM((BLK, order), f32)
    tall = pltpu.VMEM((order, BLK), f32)
    block = pltpu.VMEM((BLK, BLK), f32)
    tile = pltpu.VMEM((8, BLK), f32)
    tiles = pltpu.VMEM((count, 8, BLK), f32)
    dma = pltpu.SemaphoreType.DMA
    n_plane, n_line = count - 1, nz * nk
    grad, direction, trial, stat = pl.pallas_call(
        functools.partial(kernel, dims),
        out_shape=(
            jax.ShapeDtypeStruct((rows, cols), f32),
            jax.ShapeDtypeStruct((rows, cols), f32),
            jax.ShapeDtypeStruct((8, order), f32),
            jax.ShapeDtypeStruct((8, BLK), f32),
        ),
        in_specs=[pl.BlockSpec(memory_space=pltpu.HBM)] * 5,
        out_specs=(vmem, vmem, vmem, vmem),
        scratch_shapes=[
            pltpu.SMEM(bvec_index.shape, jnp.int32), pltpu.SMEM(weight_table.shape, f32),
            pltpu.VMEM(m_matrices.shape[1:], f32), pltpu.VMEM((rows, cols), f32), pltpu.VMEM((rows, cols), f32), dma((5,)),
            pltpu.VMEM((nx, 2, BLK, BLK), f32), block, pltpu.VMEM((nx, 8, BLK), f32), tile,
            block, block, block, block, block, tile, tiles, tiles,
            wide, tall, wide, tall, tall, wide, tall, wide, tall, wide, wide,
            pltpu.VMEM((2 * nx * BLK, 2 * BLK), jnp.bfloat16), pltpu.VMEM((2 * nx * BLK, order), f32),
            pltpu.VMEM((8, order), f32), tiles, tiles, tile, tile,
            dma((nx - 1,)), dma((nx - 1,)),
            dma((n_plane + n_line,)), dma((2 * nx,)),
            dma((4,)), dma((4,)),
            dma((24,)), dma((4, 24)),
            dma((2, 8)), dma((5, 8)),
            dma((2, nz)), dma((5, nz)),
            dma((1,)), dma((1,)),
            dma((n_plane,)), dma((5, n_plane)), dma((count,)), dma((count,)),
        ],
        compiler_params=pltpu.CompilerParams(
            collective_id=0, has_side_effects=True, vmem_limit_bytes=40 * 1024 * 1024
        ),
    )(*(
        pltpu.with_memory_space_constraint(array, pltpu.HBM)
        for array in (m_matrices.reshape(m_matrices.shape[1:]), dir_prev, grad_prev, bvec_index, weight_table)
    ))
    one = jax.ShapeDtypeStruct((1, 1), f32)
    block_out = jax.ShapeDtypeStruct((rows, cols), f32)
    spread, trial_spread, grad, direction, trial = pl.pallas_call(
        hand_out,
        out_shape=(one, one, block_out, block_out, jax.ShapeDtypeStruct((nx, 2, order), f32)),
        in_specs=[vmem] * 4,
        out_specs=(smem, smem, vmem, vmem, vmem),
        compiler_params=pltpu.CompilerParams(vmem_limit_bytes=8 * 1024 * 1024),
    )(grad, direction, trial, stat)
    return spread.reshape(()), trial_spread.reshape(()), grad, direction, trial


def solution(mesh):
    nx, ny, nk = mesh.shape["bvec"], mesh.shape["col"], 2
    nz = mesh.shape["row"] // nk
    torus = Mesh(mesh.devices.reshape(nx, nz, nk, ny), ("bvec", "zed", "core", "col"))
    return jax.shard_map(
        functools.partial(shards, (nx, ny, nz, nk)),
        mesh=torus,
        in_specs=(P("bvec", None, ROW, "col"), P(), P(), P(ROW, "col"), P(ROW, "col")),
        out_specs=(P(), P(), P(ROW, "col"), P(ROW, "col"), P()),
        check_vma=False,
    )
```

```python
import functools

import jax
import jax.numpy as jnp
from jax import lax
from jax.experimental import pallas as pl
from jax.experimental.pallas import tpu as pltpu
from jax.sharding import Mesh
from jax.sharding import PartitionSpec as P

ROW = ("zed", "core")
STEP_SCALE = 1.75
BLK = 128
MESH = pl.DeviceIdType.MESH


def split(value):
    high = value.astype(jnp.bfloat16)
    low = (value - high.astype(jnp.float32)).astype(jnp.bfloat16)
    return high, low


def dot(left, right):
    return jnp.dot(left, right, preferred_element_type=jnp.float32)


def dot_split(left, right):
    (lh, ll), (rh, rl) = left, right
    size = rh.shape[1]
    both = dot(lh, jnp.concatenate([rh, rl], axis=1))
    return both[:, :size] + (both[:, size:] + dot(ll, rh))


def kernel(
    dims, m_in, dp_in, gp_in, idx_in, tab_in,
    grad_ref, dir_ref, tfin, stat_ref,
    idx_ref, tab_ref, m_ref, gp_ref, dp_ref, in_s,
    mall, dcm, drt, dsrc, gblk, blk1, blk2, blk3, blk4, eblk, etr, stile, sx, sz,
    drow, dcol, grow, gcol, acol, row2, col2, row3, row4, col4, erow, ej, mt, turned, part, pz, px, qtile, ttile,
    a2a_s, a2a_r, dia_s, dia_r, dpr_s, dpr_r, row_s, row_r, col_s, col_r, fwd_s, fwd_r, sml_s, sml_r, pz_s, pz_r,
):
    nx, ny, nz, nk = dims
    count = nx * ny
    order = count * BLK
    wide = nx * BLK
    x, y = lax.axis_index("bvec"), lax.axis_index("col")
    z, k = lax.axis_index("zed"), lax.axis_index("core")
    r = nk * z + k
    c = nx * y + x

    def dev(xx, yy, zz, kk):
        return {"bvec": xx, "zed": zz, "core": kk, "col": yy}

    def off(value, step, size):
        return lax.rem(value + step, size) if step else value

    def lanes(index, size=BLK):
        return pl.ds(pl.multiple_of(index * size, size), size)

    plane = [(ox, oy) for ox in range(nx) for oy in range(ny) if (ox, oy) != (0, 0)]
    line = [(oz, ok) for oz in range(nz) for ok in range(nk)]
    others = line[1:]

    def at_plane(ox, oy):
        return dev(off(x, ox, nx), off(y, oy, ny), z, k)

    def at_line(oz, ok):
        return dev(x, y, off(z, oz, nz), off(k, ok, nk))

    px_t, py_t = lax.rem(r, nx), lax.div(r, nx)
    pz_t, pk_t = lax.div(c, nk), lax.rem(c, nk)
    off_diag = r != c
    holds = y == py_t

    loads = [
        pltpu.make_async_copy(src, dst, in_s.at[i])
        for i, (src, dst) in enumerate(
            ((m_in, m_ref), (dp_in, dp_ref), (gp_in, gp_ref), (idx_in, idx_ref), (tab_in, tab_ref))
        )
    ]
    for copy in loads:
        copy.start()

    barrier = pltpu.get_barrier_semaphore()
    for ox, oy in plane:
        pl.semaphore_signal(barrier, inc=1, device_id=at_plane(ox, oy), device_id_type=MESH)
    for oz, ok in others:
        pl.semaphore_signal(barrier, inc=1, device_id=at_line(oz, ok), device_id_type=MESH)

    for b in range(nx):
        @pl.when((x != b) | off_diag)
        def _(b=b):
            pl.semaphore_signal(barrier, inc=1, device_id=dev(b, y, pz_t, pk_t), device_id_type=MESH)

    for copy in loads:
        copy.wait()

    own_d = dp_ref[:, lanes(x)]
    eye_r = lax.broadcasted_iota(jnp.int32, (BLK, BLK), 0)
    eye_c = lax.broadcasted_iota(jnp.int32, (BLK, BLK), 1)
    eye = eye_r == eye_c
    dsrc[...] = jnp.zeros((8, BLK), jnp.float32)
    for p in range(2):
        dsrc[p:p + 1, :] = jnp.sum(jnp.where(eye, m_ref[p, :, lanes(px_t)], 0.0), axis=0, keepdims=True)
    if nx * 8 < BLK:
        dcm[nx * 8:, :] = jnp.zeros((BLK - nx * 8, BLK), jnp.float32)

    expected = len(plane) + len(others)
    asked = len(line) - (x == px_t).astype(jnp.int32)
    with jax.named_scope("barrier"):
        pl.semaphore_wait(barrier, expected + holds.astype(jnp.int32) * asked)

    def remote(src, dst, send, recv, device):
        return pltpu.make_async_remote_copy(
            src_ref=src, dst_ref=dst, send_sem=send, recv_sem=recv, device_id=device, device_id_type=MESH
        )

    dia_row = [
        remote(dsrc, dcm.at[pl.ds(pl.multiple_of(8 * x, 8), 8), :], dia_s.at[i], dia_r.at[x], at_plane(ox, oy))
        for i, (ox, oy) in enumerate(plane)
    ]
    dia_col = [
        remote(dsrc, drt.at[x], dia_s.at[len(plane) + i], dia_r.at[nx + x],
               dev(px_t, y, off(z, oz, nz), off(k, ok, nk)))
        for i, (oz, ok) in enumerate(line)
    ]

    @pl.when(holds)
    def _():
        for copy in dia_row:
            copy.start()
        for copy in dia_col[1:]:
            copy.start()
        dcm[pl.ds(pl.multiple_of(8 * x, 8), 8), :] = dsrc[...]

    @pl.when(holds & (x != px_t))
    def _():
        dia_col[0].start()

    @pl.when(jnp.logical_not(off_diag))
    def _():
        drt[pl.ds(x, 1)] = dsrc[...][None]

    a2a = []
    for ox in range(1, nx):
        xp = off(x, ox, nx)
        copy = remote(m_ref.at[:, :, lanes(xp)], mall.at[x], a2a_s.at[ox - 1], a2a_r.at[ox - 1], dev(xp, y, z, k))
        copy.start()
        a2a.append(copy)

    def wait_all(copies, name="wait"):
        with jax.named_scope(name):
            for copy in copies:
                copy.wait()

    half = BLK // 2
    top, low = slice(0, half), slice(half, BLK)

    def far_block(step, part, index):
        held = drow.at[part, lanes(off(y, ny - step, ny), wide)]
        return remote(held, held, dpr_s.at[index], dpr_r.at[index], at_plane(0, step))

    dprow = []
    for i, oy in enumerate((1, ny - 1)):
        copy = remote(dp_ref, drow.at[:, lanes(y, wide)], dpr_s.at[i], dpr_r.at[i], at_plane(0, oy))
        copy.start()
        dprow.append(copy)

    ring_x = [1, nx - 1, 2]
    ring_y = [1, ny - 1, 2]

    def plane_start(stage, src, dst):
        bank = 1 if stage == 4 else 0
        first = []
        for i, ox in enumerate(ring_x):
            for at, device in ((i, at_plane(ox, 0)), (3 + i, at_plane(0, ring_y[i]))):
                first.append(remote(src, dst.at[:, lanes(c)], row_s.at[bank, at], row_r.at[stage, at], device))
                first[-1].start()
        return stage, bank, dst, first, []

    def plane_forward(state):
        stage, bank, dst, first, second = state
        with jax.named_scope(f"row{stage}a"):
            for i in range(3):
                first[2 * i].wait_recv()
                held = dst.at[top, lanes(nx * y + off(x, nx - ring_x[i], nx))]
                for j in range(3):
                    at = 6 + 3 * i + j
                    second.append(remote(held, held, row_s.at[bank, at], row_r.at[stage, at], at_plane(0, ring_y[j])))
                    second[-1].start()
                first[2 * i + 1].wait_recv()
                held = dst.at[low, lanes(nx * off(y, ny - ring_y[i], ny) + x)]
                for j in range(3):
                    at = 15 + 3 * i + j
                    second.append(remote(held, held, row_s.at[bank, at], row_r.at[stage, at], at_plane(ring_x[j], 0)))
                    second[-1].start()

    arrivals = [(0, 0), (1, 0), (0, 1), (nx - 1, 0), (0, ny - 1), (2, 0), (0, 2)]
    arrivals += [(ox, oy) for ox in (1, nx - 1) for oy in (1, ny - 1)]
    arrivals += [(ox, oy) for ox, oy in plane if ox and oy and 2 in (ox, oy) and ox != oy] + [(2, 2)]
    groups = [arrivals[i:i + 4] for i in range(0, len(arrivals), 4)]

    def plane_pieces(state, pieces):
        stage, _, _, first, second = state
        with jax.named_scope(f"row{stage}w"):
            for ox, oy in pieces:
                if ox and oy:
                    i, j = ring_x.index(ox), ring_y.index(oy)
                    second[6 * i + j].wait_recv()
                    second[6 * j + 3 + i].wait_recv()
        return [lanes(nx * off(y, ny - oy if oy else 0, ny) + off(x, nx - ox if ox else 0, nx)) for ox, oy in pieces]

    def plane_sum(state, left, right, acc, before_last=lambda: None):
        for pieces in groups:
            if pieces is groups[-1]:
                before_last()
            places = plane_pieces(state, pieces)
            rows_l = jnp.concatenate([left[:, at] for at in places], axis=1)
            cols_r = jnp.concatenate([right(at) for at in places], axis=0)
            acc = acc + dot_split(split(rows_l), split(cols_r))
        plane_done(state)
        return acc

    def plane_done(state):
        _, _, _, first, second = state
        for copy in first + second:
            copy.wait_send()

    def plane_finish(state):
        for pieces in groups:
            plane_pieces(state, pieces)
        plane_done(state)

    def line_start(stage, src, slot):
        bank = 1 if stage == 0 else 0
        first = {}
        for i, oz in enumerate((2, nz - 2, 1, nz - 1)):
            first[oz] = remote(src, slot(r), col_s.at[bank, i], col_r.at[stage, i], at_line(oz, 0))
            first[oz].start()
        over = [remote(src, slot(r), fwd_s.at[bank, 0], fwd_r.at[stage, 0], at_line(0, 1))]
        over[0].start()
        return stage, bank, slot, first, {}, over

    def line_across(state, oz):
        stage, bank, slot, first, second, over = state
        held = slot(nk * off(z, nz - oz, nz) + k)
        over.append(remote(held, held, fwd_s.at[bank, oz], fwd_r.at[stage, oz], at_line(0, 1)))
        over[-1].start()

    def line_forward(state):
        stage, bank, slot, first, second, over = state
        with jax.named_scope(f"line{stage}a"):
            for i, (oz, step, part) in enumerate(((2, 1, top), (nz - 2, nz - 1, low))):
                first[oz].wait_recv()
                held = slot(nk * off(z, nz - oz, nz) + k)
                second[i] = remote(held, held, col_s.at[bank, 4 + i], col_r.at[stage, 4 + i], at_line(step, 0))
                second[i].start()
                held = slot(nk * off(z, nz - oz, nz) + k, part)
                second[2 + i] = remote(held, held, col_s.at[bank, 6 + i], col_r.at[stage, 6 + i], at_line(oz, 0))
                second[2 + i].start()

    def line_near(state):
        stage, bank, slot, first, second, over = state
        with jax.named_scope(f"line{stage}n"):
            for oz in (2, nz - 2, 1, nz - 1):
                if oz in (1, nz - 1):
                    first[oz].wait_recv()
                line_across(state, oz)

    close = (0, 2, nz - 2, 1, nz - 1)
    distant = (3, nz - 3, 4)

    def line_far(state):
        stage, bank, slot, first, second, over = state
        with jax.named_scope(f"line{stage}f"):
            second[0].wait_recv()
            line_across(state, 3)
            second[1].wait_recv()
            line_across(state, nz - 3)
            second[2].wait_recv()
            second[3].wait_recv()
            line_across(state, 4)

    def line_mid(state):
        with jax.named_scope(f"line{state[0]}m"):
            for copy in state[5][:5]:
                copy.wait_recv()

    def line_done(state):
        stage, bank, slot, first, second, over = state
        with jax.named_scope(f"line{stage}d"):
            for copy in over[5:]:
                copy.wait_recv()
            for copy in over + list(first.values()) + list(second.values()):
                copy.wait_send()

    def line_finish(state):
        line_far(state)
        line_mid(state)
        line_done(state)

    def part_of_sum(steps):
        size = nk * BLK
        return [pl.ds(pl.multiple_of(off(z, step, nz) * size, size), size) for step in steps]

    def column_slots(ref):
        def slot(index, part=slice(0, BLK)):
            return ref.at[pl.ds(pl.multiple_of(index * BLK + part.start, half), part.stop - part.start), :]
        return slot

    def row_slots(ref):
        return lambda index, part=slice(0, BLK): ref.at[part, lanes(index)]

    d_col = line_start(0, dp_ref.at[:, lanes(x)], column_slots(dcol))

    mall[pl.ds(x, 1)] = m_ref[:, :, lanes(x)][None]
    drow[:, lanes(y, wide)] = dp_ref[...]
    dcol[lanes(r), :] = own_d
    line_forward(d_col)

    for b in range(nx):
        @pl.when(jnp.logical_not(holds & (x == b)))
        @jax.named_scope("diag_r")
        def _(b=b):
            slot = dcm.at[8 * b:8 * b + 8, :]
            remote(slot, slot, dia_s.at[0], dia_r.at[b], dev(x, y, z, k)).wait_recv()

        @pl.when(off_diag | (x != b))
        def _(b=b):
            slot = drt.at[b]
            remote(slot, slot, dia_s.at[0], dia_r.at[nx + b], dev(x, y, z, k)).wait_recv()

    weights = []
    for b in range(nx):
        value = jnp.float32(0.0)
        for t in range(tab_ref.shape[0]):
            value = value + jnp.where(idx_ref[b] == t, tab_ref[t], jnp.float32(0.0))
        weights.append(value)

    row_index = lax.broadcasted_iota(jnp.int32, (nx, BLK), 0)
    row_weights = []
    for h in range(nk):
        value = jnp.zeros((nx, BLK), jnp.float32)
        for b in range(nx // nk):
            value = jnp.where((row_index >= 2 * b) & (row_index < 2 * b + 2), weights[h * (nx // nk) + b], value)
        row_weights.append(value)
    columns = jnp.transpose(dcm[...])
    line_near(d_col)
    far = []
    for i, (step, piece) in enumerate(((1, top), (ny - 1, low))):
        dprow[i].wait_recv()
        far.append(far_block(step, piece, 2 + i))
        far[-1].start()
    wait_all(a2a, "a2a")
    total = jnp.zeros((BLK, BLK), jnp.float32)
    spread_row = jnp.zeros((1, BLK), jnp.float32)
    for b in range(nx):
        term = jnp.zeros((BLK, BLK), jnp.float32)
        for p in range(2):
            at_row = columns[:, 8 * b + p:8 * b + p + 1]
            at_col = drt[b, p:p + 1, :]
            term = term + mall[b, p] * (at_row - at_col)
        total = total + (2.0 * weights[b]) * term
        re_d, im_d = drt[b, 0:1, :], drt[b, 1:2, :]
        spread_row = spread_row + weights[b] * (1.0 - re_d * re_d - im_d * im_d)
    gblk[...] = total
    own_p = gp_ref[:, lanes(x)]
    first_line = (r == 0).astype(jnp.float32)
    sums = [total * total, total * own_d, own_d * own_d, own_p * own_p]
    row_sums = [jnp.sum(value, axis=0, keepdims=True) for value in sums] + [spread_row * first_line]
    row_sums.append(jnp.zeros((8 - len(row_sums), BLK), jnp.float32))
    row_sums = jnp.sum(jnp.concatenate(row_sums, axis=0), axis=1, keepdims=True)
    pick = lax.broadcasted_iota(jnp.int32, (8, BLK), 0) == lax.broadcasted_iota(jnp.int32, (8, BLK), 1)
    stile[...] = jnp.sum(jnp.where(pick, row_sums, 0.0), axis=0, keepdims=True)

    def small_plane(stage, src, dst):
        dst[pl.ds(c, 1)] = src[...][None]
        copies = []
        for i, (ox, oy) in enumerate(plane):
            copy = remote(src, dst.at[c], sml_s.at[i], sml_r.at[stage, i], at_plane(ox, oy))
            copy.start()
            copies.append(copy)
        return copies

    def small_line(stage, src, dst):
        dst[pl.ds(r, 1)] = src(r)[...][None]
        copies = []
        for i, (oz, ok) in enumerate(others):
            rp = nk * off(z, oz, nz) + off(k, ok, nk)
            copy = remote(src(rp), dst.at[r], sml_s.at[i], sml_r.at[stage, i], at_line(oz, ok))
            copy.start()
            copies.append(copy)
        return copies

    def summed(ref):
        value = ref[0]
        for i in range(1, count):
            value = value + ref[i]
        return value

    copies = small_line(0, lambda index: stile, sx)
    grow[:, lanes(c)] = total
    gcol[lanes(r), :] = total
    rows = plane_start(0, gblk, grow)
    cols = line_start(1, gblk, column_slots(gcol))
    wait_all(copies, "small0")
    stile[...] = summed(sx)
    copies = small_plane(1, stile, sz)
    line_forward(cols)
    plane_forward(rows)
    line_near(cols)
    line_finish(d_col)
    wait_all(far, "far")
    for copy in dprow:
        copy.wait_send()
    line_far(cols)
    plane_finish(rows)
    line_mid(cols)
    wait_all(copies, "small1")
    sums = jnp.sum(jnp.where(pick, summed(sz), 0.0), axis=1, keepdims=True)
    gg, gd, dd, pp, spread = (jnp.broadcast_to(sums[i:i + 1, :], (1, BLK)) for i in range(5))
    spread = spread / order
    beta = gg / (1.0 + pp)
    norm = jnp.maximum(gg - 2.0 * beta * gd + beta * beta * dd, 0.0)
    scale = STEP_SCALE / jnp.sqrt(1.0 + norm / order)

    chunk = 4 * BLK if order % (4 * BLK) == 0 else BLK
    beta_w = jnp.concatenate([beta] * nk, axis=1)
    scale_w = jnp.concatenate([scale] * nk, axis=1)

    def square(acc, steps):
        for at in part_of_sum(steps):
            left = scale_w * (beta_w * drow[:, at] - grow[:, at])
            right = scale * (beta * dcol[at, :] - gcol[at, :])
            acol[at, :] = right
            acc = acc + dot_split(split(left), split(right))
        return acc

    acc = square(jnp.zeros((BLK, BLK), jnp.float32), close)
    line_done(cols)
    acc = square(acc, distant)
    blk1[...] = acol[lanes(r), :]
    blk2[...] = acc
    row2[:, lanes(c)] = acc
    col2[lanes(r), :] = acc
    rows = plane_start(1, blk2, row2)
    cols = line_start(2, blk2, column_slots(col2))
    for j in range(nx):
        at = pl.ds(pl.multiple_of(y * wide + j * BLK, BLK), BLK)
        piece = grow[:, at]
        grad_ref[:, j * BLK:(j + 1) * BLK] = piece
        dir_ref[:, j * BLK:(j + 1) * BLK] = beta * drow[:, at] - piece

    for b in range(nx):
        for p in range(2):
            i = 2 * b + p
            high, tail = split(jnp.transpose(mall[b, p]))
            mt[i * BLK:(i + 1) * BLK, :] = jnp.concatenate([high, tail, high], axis=1)
    line_forward(cols)
    plane_forward(rows)
    line_near(cols)
    acc3 = plane_sum(
        rows, row2, lambda at: acol[at, :], jnp.zeros((BLK, BLK), jnp.float32), lambda: line_far(cols)
    )
    blk3[...] = acc3
    row3[:, lanes(c)] = acc3
    more = plane_start(4, blk3, row3)
    line_mid(cols)

    def fourth(acc, steps):
        for at in part_of_sum(steps):
            acc = acc + dot_split(split(row2[:, at]), split(col2[at, :]))
        return acc

    acc4 = fourth(jnp.zeros((BLK, BLK), jnp.float32), close)
    line_done(cols)
    acc4 = fourth(acc4, distant)
    blk4[...] = acc4
    row4[:, lanes(c)] = acc4
    col4[lanes(r), :] = acc4
    cols = line_start(3, blk4, column_slots(col4))
    rows = plane_start(2, blk4, row4)
    plane_forward(more)
    for at in range(0, order, chunk):
        acol[at:at + chunk, :] = col2[at:at + chunk, :] * (1.0 / 720.0)
        gcol[at:at + chunk, :] = col2[at:at + chunk, :] * (1.0 / 120.0)
    line_forward(cols)
    line_near(cols)
    plane_forward(rows)
    line_finish(cols)
    plane_finish(more)

    odd = jnp.zeros((BLK, BLK), jnp.float32)
    for at in range(0, order, chunk):
        right = gcol[at:at + chunk, :] + col4[at:at + chunk, :] * (1.0 / 5040.0)
        odd = odd + dot_split(split(row3[:, at:at + chunk]), split(right))
    odd = odd + blk1[...] + blk3[...] * (1.0 / 6.0)
    def even_columns(at):
        return acol[at, :] + col4[at, :] * (1.0 / 40320.0)

    even = plane_sum(rows, row4, even_columns, jnp.zeros((BLK, BLK), jnp.float32))
    even = even + blk2[...] * 0.5 + blk4[...] * (1.0 / 24.0)
    even = even + jnp.where(eye & jnp.logical_not(off_diag), 1.0, 0.0)

    eblk[...] = even + odd
    etr[...] = jnp.transpose(even - odd)
    cols = line_start(4, etr, row_slots(ej))
    rows = plane_start(3, eblk, erow)
    erow[:, lanes(c)] = eblk[...]
    ej[:, lanes(r)] = etr[...]
    plane_forward(rows)
    line_forward(cols)
    line_near(cols)

    def turn(g):
        slots = plane_pieces(rows, groups[g])
        high, tail = split(jnp.concatenate([erow[:, at] for at in slots], axis=1))
        turned[g] = dot(mt[...], jnp.concatenate([high, high, tail], axis=0))

    for g in range(len(groups) - 1):
        turn(g)
    line_far(cols)
    turn(len(groups) - 1)
    plane_done(rows)

    hall = [(ox, oy, ok) for ox in range(nx) for oy in range(ny) for ok in range(nk)]

    def at_hall(ox, oy, ok):
        return dev(off(x, ox, nx), off(y, oy, ny), z, off(k, ok, nk))

    line_mid(cols)
    line_done(cols)
    own = nk * c + k
    copies = []
    for g, pieces in enumerate(groups):
        for i, (ox, oy) in enumerate(pieces):
            back = (nx - ox) % nx, (ny - oy) % ny
            place = nx * off(y, back[1], ny) + off(x, back[0], nx)
            left = ej[:, lanes(place)]
            sums = jnp.concatenate(
                [
                    jnp.sum(left * turned[g, j * BLK:(j + 1) * BLK, i * BLK:(i + 1) * BLK], axis=0, keepdims=True)
                    for j in range(2 * nx)
                ],
                axis=0,
            )
            for h in range(nk):
                part[nk * (4 * g + i) + h] = sums[h * nx:(h + 1) * nx]
        for i, (ox, oy) in enumerate(pieces):
            back = (nx - ox) % nx, (ny - oy) % ny
            for ok in range(nk):
                src = part.at[nk * (4 * g + i) + off(k, ok, nk)]
                if (ox, oy, ok) == (0, 0, 0):
                    pz[pl.ds(own, 1)] = part[pl.ds(nk * (4 * g + i) + k, 1)]
                else:
                    at = hall.index((*back, ok))
                    copies.append(remote(src, pz.at[own], pz_s.at[at], pz_r.at[0, at], at_hall(*back, ok)))
                    copies[-1].start()
    wait_all(copies, "small2")
    value = pz[0]
    for i in range(1, nk * count):
        value = value + pz[i]
    ttile[...] = value
    px[pl.ds(z, 1)] = value[None]
    copies = []
    for oz in range(1, nz):
        copies.append(remote(ttile, px.at[z], pz_s.at[oz], pz_r.at[1, oz], at_line(oz, 0)))
        copies[-1].start()
    wait_all(copies, "small3")
    value = px[0]
    for i in range(1, nz):
        value = value + px[i]
    qtile[...] = value
    tfin[pl.ds(own, 1)] = value[None]
    copies = []
    for i, (ox, oy, ok) in enumerate(hall[1:]):
        copies.append(remote(qtile, tfin.at[own], pz_s.at[i], pz_r.at[2, i], at_hall(ox, oy, ok)))
        copies[-1].start()

    @pl.when(holds)
    def _():
        for copy in dia_row:
            copy.wait_send()
        for copy in dia_col[1:]:
            copy.wait_send()

    @pl.when(holds & (x != px_t))
    def _():
        dia_col[0].wait_send()

    wait_all(copies, "small4")
    trial = jnp.zeros((nx, BLK), jnp.float32)
    for h in range(nk):
        value = jnp.zeros((nx, BLK), jnp.float32)
        for i in range(count):
            value = value + (0.5 - tfin[nk * i + h] * tfin[nk * i + h])
        trial = trial + value * row_weights[h]
    trial = jnp.sum(trial, axis=0, keepdims=True)
    stat_ref[...] = jnp.zeros((8, BLK), jnp.float32)
    stat_ref[0:1, :] = spread
    stat_ref[1:2, :] = jnp.broadcast_to(jnp.sum(trial, axis=1, keepdims=True) / order, (1, BLK))


def hand_out(grad_ref, dir_ref, trial_ref, stat_ref, spread_out, trial_spread_out, grad_out, dir_out, trial_out):
    spread_out[0, 0] = jnp.sum(stat_ref[0:1, 0:1])
    trial_spread_out[0, 0] = jnp.sum(stat_ref[1:2, 0:1])
    grad_out[...] = grad_ref[...]
    dir_out[...] = dir_ref[...]
    halves = trial_out.shape[0] // 2
    for i in range(trial_ref.shape[0] // 2):
        for b in range(trial_out.shape[0]):
            at = 2 * (b % halves)
            trial_out[b, :, i * BLK:(i + 1) * BLK] = trial_ref[2 * i + b // halves, at:at + 2, :]


def shards(dims, m_matrices, bvec_index, weight_table, grad_prev, dir_prev):
    nx, ny, nz, nk = dims
    count = nx * ny
    order = count * BLK
    f32 = jnp.float32
    rows, cols = grad_prev.shape
    vmem = pl.BlockSpec(memory_space=pltpu.VMEM)
    smem = pl.BlockSpec(memory_space=pltpu.SMEM)
    wide = pltpu.VMEM((BLK, order), f32)
    tall = pltpu.VMEM((order, BLK), f32)
    block = pltpu.VMEM((BLK, BLK), f32)
    tile = pltpu.VMEM((8, BLK), f32)
    half_tile = pltpu.VMEM((nx, BLK), f32)
    line = pltpu.VMEM((1, BLK), f32)
    lines = pltpu.VMEM((count, 1, BLK), f32)
    dma = pltpu.SemaphoreType.DMA
    n_plane, n_line = count - 1, nz * nk
    grad, direction, trial, stat = pl.pallas_call(
        functools.partial(kernel, dims),
        out_shape=(
            jax.ShapeDtypeStruct((rows, cols), f32),
            jax.ShapeDtypeStruct((rows, cols), f32),
            jax.ShapeDtypeStruct((nk * count, nx, BLK), f32),
            jax.ShapeDtypeStruct((8, BLK), f32),
        ),
        in_specs=[pl.BlockSpec(memory_space=pltpu.HBM)] * 5,
        out_specs=(vmem, vmem, vmem, vmem),
        scratch_shapes=[
            pltpu.SMEM(bvec_index.shape, jnp.int32), pltpu.SMEM(weight_table.shape, f32),
            pltpu.VMEM(m_matrices.shape[1:], f32), pltpu.VMEM((rows, cols), f32), pltpu.VMEM((rows, cols), f32), dma((5,)),
            pltpu.VMEM((nx, 2, BLK, BLK), f32), block, pltpu.VMEM((nx, 8, BLK), f32), tile,
            block, block, block, block, block, block, block, line, lines, lines,
            wide, tall, wide, tall, tall, wide, tall, wide, wide, tall, wide, wide,
            pltpu.VMEM((2 * nx * BLK, 3 * BLK), jnp.bfloat16), pltpu.VMEM((count // 4, 2 * nx * BLK, 4 * BLK), f32),
            pltpu.VMEM((nk * count, nx, BLK), f32), pltpu.VMEM((nk * count, nx, BLK), f32), pltpu.VMEM((nz, nx, BLK), f32),
            half_tile, half_tile,
            dma((nx - 1,)), dma((nx - 1,)),
            dma((n_plane + n_line,)), dma((2 * nx,)),
            dma((4,)), dma((4,)),
            dma((2, 24)), dma((5, 24)),
            dma((2, 8)), dma((5, 8)),
            dma((2, nz)), dma((5, nz)),
            dma((n_plane,)), dma((2, n_plane)), dma((nk * count,)), dma((3, nk * count)),
        ],
        compiler_params=pltpu.CompilerParams(
            collective_id=0, has_side_effects=True, vmem_limit_bytes=40 * 1024 * 1024
        ),
    )(*(
        pltpu.with_memory_space_constraint(array, pltpu.HBM)
        for array in (m_matrices.reshape(m_matrices.shape[1:]), dir_prev, grad_prev, bvec_index, weight_table)
    ))
    one = jax.ShapeDtypeStruct((1, 1), f32)
    block_out = jax.ShapeDtypeStruct((rows, cols), f32)
    spread, trial_spread, grad, direction, trial = pl.pallas_call(
        hand_out,
        out_shape=(one, one, block_out, block_out, jax.ShapeDtypeStruct((nx, 2, order), f32)),
        in_specs=[vmem] * 4,
        out_specs=(smem, smem, vmem, vmem, vmem),
        compiler_params=pltpu.CompilerParams(vmem_limit_bytes=8 * 1024 * 1024),
    )(grad, direction, trial, stat)
    return spread.reshape(()), trial_spread.reshape(()), grad, direction, trial


def solution(mesh):
    nx, ny, nk = mesh.shape["bvec"], mesh.shape["col"], 2
    nz = mesh.shape["row"] // nk
    torus = Mesh(mesh.devices.reshape(nx, nz, nk, ny), ("bvec", "zed", "core", "col"))
    return jax.shard_map(
        functools.partial(shards, (nx, ny, nz, nk)),
        mesh=torus,
        in_specs=(P("bvec", None, ROW, "col"), P(), P(), P(ROW, "col"), P(ROW, "col")),
        out_specs=(P(), P(), P(ROW, "col"), P(ROW, "col"), P()),
        check_vma=False,
    )
```

```python
import functools

import jax
import jax.numpy as jnp
from jax import lax
from jax.experimental import pallas as pl
from jax.experimental.pallas import tpu as pltpu
from jax.sharding import Mesh
from jax.sharding import PartitionSpec as P

ROW = ("zed", "core")
STEP_SCALE = 1.75
BLK = 128
MESH = pl.DeviceIdType.MESH


def split(value):
    high = value.astype(jnp.bfloat16)
    low = (value - high.astype(jnp.float32)).astype(jnp.bfloat16)
    return high, low


def dot(left, right):
    return jnp.dot(left, right, preferred_element_type=jnp.float32)


def dot_split(left, right):
    (lh, ll), (rh, rl) = left, right
    size = rh.shape[1]
    both = dot(lh, jnp.concatenate([rh, rl], axis=1))
    return both[:, :size] + (both[:, size:] + dot(ll, rh))


def kernel(
    dims, m_in, dp_in, gp_in, idx_in, tab_in,
    grad_ref, dir_ref, tfin, stat_ref,
    idx_ref, tab_ref, m_ref, gp_ref, dp_ref, in_s,
    mall, dcm, drt, dsrc, gblk, blk1, blk2, blk3, blk4, eblk, etr, own_block, stile, sx, sz,
    drow, dcol, grow, gcol, acol, row2, col2, row3, row4, col4, erow, ej, mt, turned, part, pz, px, qtile, ttile,
    a2a_s, a2a_r, dia_s, dia_r, dpr_s, dpr_r, row_s, row_r, col_s, col_r, fwd_s, fwd_r, sml_s, sml_r,
):
    nx, ny, nz, nk = dims
    count = nx * ny
    order = count * BLK
    wide = nx * BLK
    x, y = lax.axis_index("bvec"), lax.axis_index("col")
    z, k = lax.axis_index("zed"), lax.axis_index("core")
    r = nk * z + k
    c = nx * y + x

    def dev(xx, yy, zz, kk):
        return {"bvec": xx, "zed": zz, "core": kk, "col": yy}

    def off(value, step, size):
        return lax.rem(value + step, size) if step else value

    def lanes(index, size=BLK):
        return pl.ds(pl.multiple_of(index * size, size), size)

    plane = [(ox, oy) for ox in range(nx) for oy in range(ny) if (ox, oy) != (0, 0)]
    line = [(oz, ok) for oz in range(nz) for ok in range(nk)]
    others = line[1:]

    def at_plane(ox, oy):
        return dev(off(x, ox, nx), off(y, oy, ny), z, k)

    def at_line(oz, ok):
        return dev(x, y, off(z, oz, nz), off(k, ok, nk))

    px_t, py_t = lax.rem(r, nx), lax.div(r, nx)
    pz_t, pk_t = lax.div(c, nk), lax.rem(c, nk)
    off_diag = r != c
    holds = y == py_t

    loads = [
        pltpu.make_async_copy(src, dst, in_s.at[i])
        for i, (src, dst) in enumerate(
            ((m_in, m_ref), (dp_in, dp_ref), (gp_in, gp_ref), (idx_in, idx_ref), (tab_in, tab_ref))
        )
    ]
    for copy in loads:
        copy.start()

    barrier = pltpu.get_barrier_semaphore()
    for ox, oy in plane:
        pl.semaphore_signal(barrier, inc=1, device_id=at_plane(ox, oy), device_id_type=MESH)
    for oz, ok in others:
        pl.semaphore_signal(barrier, inc=1, device_id=at_line(oz, ok), device_id_type=MESH)

    for b in range(nx):
        @pl.when((x != b) | off_diag)
        def _(b=b):
            pl.semaphore_signal(barrier, inc=1, device_id=dev(b, y, pz_t, pk_t), device_id_type=MESH)

    for copy in loads:
        copy.wait()

    own_d = dp_ref[:, lanes(x)]
    eye_r = lax.broadcasted_iota(jnp.int32, (BLK, BLK), 0)
    eye_c = lax.broadcasted_iota(jnp.int32, (BLK, BLK), 1)
    eye = eye_r == eye_c
    dsrc[...] = jnp.zeros((8, BLK), jnp.float32)
    for p in range(2):
        dsrc[p:p + 1, :] = jnp.sum(jnp.where(eye, m_ref[p, :, lanes(px_t)], 0.0), axis=0, keepdims=True)
    if nx * 8 < BLK:
        dcm[nx * 8:, :] = jnp.zeros((BLK - nx * 8, BLK), jnp.float32)

    expected = len(plane) + len(others)
    asked = len(line) - (x == px_t).astype(jnp.int32)
    with jax.named_scope("barrier"):
        pl.semaphore_wait(barrier, expected + holds.astype(jnp.int32) * asked)

    def remote(src, dst, send, recv, device):
        return pltpu.make_async_remote_copy(
            src_ref=src, dst_ref=dst, send_sem=send, recv_sem=recv, device_id=device, device_id_type=MESH
        )

    def all_sent(sem, ref):
        remote(ref, ref, sem, sem, dev(x, y, z, k)).wait_send()

    def all_here(sem, ref):
        remote(ref, ref, sem, sem, dev(x, y, z, k)).wait_recv()

    def pieces_of(count_blocks):
        return gcol.at[0:int(count_blocks * BLK), :]

    dia_row = [
        remote(dsrc, dcm.at[pl.ds(pl.multiple_of(8 * x, 8), 8), :], dia_s.at[0], dia_r.at[x], at_plane(ox, oy))
        for i, (ox, oy) in enumerate(plane)
    ]
    dia_col = [
        remote(dsrc, drt.at[x], dia_s.at[0], dia_r.at[nx + x],
               dev(px_t, y, off(z, oz, nz), off(k, ok, nk)))
        for i, (oz, ok) in enumerate(line)
    ]

    @pl.when(holds)
    def _():
        for copy in dia_row:
            copy.start()
        for copy in dia_col[1:]:
            copy.start()
        dcm[pl.ds(pl.multiple_of(8 * x, 8), 8), :] = dsrc[...]

    @pl.when(holds & (x != px_t))
    def _():
        dia_col[0].start()

    @pl.when(jnp.logical_not(off_diag))
    def _():
        drt[pl.ds(x, 1)] = dsrc[...][None]

    a2a = []
    for ox in range(1, nx):
        xp = off(x, ox, nx)
        copy = remote(m_ref.at[:, :, lanes(xp)], mall.at[x], a2a_s.at[0], a2a_r.at[0], dev(xp, y, z, k))
        copy.start()
        a2a.append(copy)

    def wait_all(copies, name="wait"):
        with jax.named_scope(name):
            for copy in copies:
                copy.wait()

    half = BLK // 2
    top, low = slice(0, half), slice(half, BLK)

    def far_block(step, part, index):
        held = drow.at[part, lanes(off(y, ny - step, ny), wide)]
        return remote(held, held, dpr_s.at[0], dpr_r.at[index], at_plane(0, step))

    dprow = []
    for i, oy in enumerate((1, ny - 1)):
        copy = remote(dp_ref, drow.at[:, lanes(y, wide)], dpr_s.at[0], dpr_r.at[i], at_plane(0, oy))
        copy.start()
        dprow.append(copy)

    ring_x = [1, nx - 1, 2]
    ring_y = [1, ny - 1, 2]

    arrivals = [(0, 0), (1, 0), (0, 1), (nx - 1, 0), (0, ny - 1), (2, 0), (0, 2)]
    arrivals += [(ox, oy) for ox in (1, nx - 1) for oy in (1, ny - 1)]
    arrivals += [(ox, oy) for ox, oy in plane if ox and oy and 2 in (ox, oy) and ox != oy] + [(2, 2)]
    groups = [arrivals[i:i + 4] for i in range(0, len(arrivals), 4)]

    def group_sem(bank, ox, oy):
        return row_r.at[bank, 6 + [g for g, pieces in enumerate(groups) if (ox, oy) in pieces][0]]

    def plane_start(stage, src, dst):
        bank = 2 if stage == 4 else stage % 2
        first = []
        for n, (over_x, over_y) in enumerate(((top, low), (low, top))):
            for i in range(3):
                for m, part_of, device in ((0, over_x, at_plane(ring_x[i], 0)), (1, over_y, at_plane(0, ring_y[i]))):
                    step = (0, ring_y[i]) if m else (ring_x[i], 0)
                    sem = group_sem(bank, *step) if n else row_r.at[bank, 2 * i + m]
                    first.append(remote(src.at[part_of, :], dst.at[part_of, lanes(c)], row_s.at[bank], sem, device))
                    first[-1].start()
        return stage, bank, dst, first, []

    def plane_forward(state):
        stage, bank, dst, first, second = state
        with jax.named_scope(f"row{stage}a"):
            for i in range(3):
                first[2 * i].wait_recv()
                held = dst.at[top, lanes(nx * y + off(x, nx - ring_x[i], nx))]
                for j in range(3):
                    sem = group_sem(bank, ring_x[i], ring_y[j])
                    second.append(remote(held, held, row_s.at[bank], sem, at_plane(0, ring_y[j])))
                    second[-1].start()
                first[2 * i + 1].wait_recv()
                held = dst.at[low, lanes(nx * off(y, ny - ring_y[i], ny) + x)]
                for j in range(3):
                    sem = group_sem(bank, ring_x[j], ring_y[i])
                    second.append(remote(held, held, row_s.at[bank], sem, at_plane(ring_x[j], 0)))
                    second[-1].start()

    def plane_pieces(state, pieces):
        stage, bank, _, _, _ = state
        halves = sum(2 if ox and oy else 1 for ox, oy in pieces if (ox, oy) != (0, 0))
        with jax.named_scope(f"row{stage}w"):
            all_here(row_r.at[bank, 6 + groups.index(pieces)], pieces_of(halves / 2))
        return [lanes(nx * off(y, ny - oy if oy else 0, ny) + off(x, nx - ox if ox else 0, nx)) for ox, oy in pieces]

    def plane_sum(state, left, right, acc, before_last=lambda: None):
        for pieces in groups:
            if pieces is groups[-1]:
                before_last()
            places = plane_pieces(state, pieces)
            rows_l = jnp.concatenate([left[:, at] for at in places], axis=1)
            cols_r = jnp.concatenate([right(at) for at in places], axis=0)
            acc = acc + dot_split(split(rows_l), split(cols_r))
        plane_done(state)
        return acc

    def plane_done(state):
        all_sent(row_s.at[state[1]], pieces_of(count - 1))

    def plane_finish(state):
        for pieces in groups:
            plane_pieces(state, pieces)
        plane_done(state)

    def line_start(stage, src, slot):
        bank = (2, 0, 1, 0, 1)[stage]
        whole = slice(0, BLK)
        first = {}
        order_z = ((2, top), (nz - 2, low), (2, low), (nz - 2, top), (1, whole), (nz - 1, whole))
        for i, (oz, piece) in enumerate(order_z):
            first[oz, piece.start] = remote(
                src.at[piece, :], slot(r, piece), col_s.at[bank], col_r.at[bank, i], at_line(oz, 0)
            )
            first[oz, piece.start].start()
        over = [remote(src, slot(r), fwd_s.at[bank], fwd_r.at[bank, 0], at_line(0, 1))]
        over[0].start()
        return stage, bank, slot, first, {}, over

    def line_across(state, oz):
        stage, bank, slot, first, second, over = state
        held = slot(nk * off(z, nz - oz, nz) + k)
        over.append(remote(held, held, fwd_s.at[bank], fwd_r.at[bank, 1 if oz in distant else 0], at_line(0, 1)))
        over[-1].start()

    def line_forward(state):
        stage, bank, slot, first, second, over = state
        with jax.named_scope(f"line{stage}a"):
            steps = ((2, top, (2, 1)), (nz - 2, low, (nz - 2, nz - 1)), (2, low, (1,)), (nz - 2, top, (nz - 1,)))
            for oz, piece, onward in steps:
                first[oz, piece.start].wait_recv()
                held = slot(nk * off(z, nz - oz, nz) + k, piece)
                for step in onward:
                    at = 6 + distant.index((oz + step) % nz)
                    remote(held, held, col_s.at[bank], col_r.at[bank, at], at_line(step, 0)).start()

    def line_near(state):
        stage, bank, slot, first, second, over = state
        with jax.named_scope(f"line{stage}n"):
            for oz in (2, nz - 2, 1, nz - 1):
                if oz in (1, nz - 1):
                    first[oz, 0].wait_recv()
                line_across(state, oz)

    close = (0, 2, nz - 2, 1, nz - 1)
    distant = (3, nz - 3, 4)

    def line_far(state):
        stage, bank, slot, first, second, over = state
        with jax.named_scope(f"line{stage}f"):
            for oz in (3, nz - 3, 4):
                all_here(col_r.at[bank, 6 + distant.index(oz)], pieces_of(1))
                line_across(state, oz)

    def line_mid(state):
        with jax.named_scope(f"line{state[0]}m"):
            all_here(fwd_r.at[state[1], 0], pieces_of(len(close)))

    def line_done(state):
        stage, bank, slot, first, second, over = state
        with jax.named_scope(f"line{stage}d"):
            all_here(fwd_r.at[bank, 1], pieces_of(len(distant)))
            all_sent(fwd_s.at[bank], pieces_of(nz))
            all_sent(col_s.at[bank], pieces_of(nz - 1))

    def line_finish(state):
        line_far(state)
        line_mid(state)
        line_done(state)

    def part_of_sum(steps):
        size = nk * BLK
        return [pl.ds(pl.multiple_of(off(z, step, nz) * size, size), size) for step in steps]

    def column_slots(ref):
        def slot(index, part=slice(0, BLK)):
            return ref.at[pl.ds(pl.multiple_of(index * BLK + part.start, half), part.stop - part.start), :]
        return slot

    def row_slots(ref):
        return lambda index, part=slice(0, BLK): ref.at[part, lanes(index)]

    own_block[...] = own_d
    d_col = line_start(0, own_block, column_slots(dcol))

    mall[pl.ds(x, 1)] = m_ref[:, :, lanes(x)][None]
    drow[:, lanes(y, wide)] = dp_ref[...]
    dcol[lanes(r), :] = own_d
    line_forward(d_col)

    for b in range(nx):
        @pl.when(jnp.logical_not(holds & (x == b)))
        @jax.named_scope("diag_r")
        def _(b=b):
            slot = dcm.at[8 * b:8 * b + 8, :]
            remote(slot, slot, dia_s.at[0], dia_r.at[b], dev(x, y, z, k)).wait_recv()

        @pl.when(off_diag | (x != b))
        def _(b=b):
            slot = drt.at[b]
            remote(slot, slot, dia_s.at[0], dia_r.at[nx + b], dev(x, y, z, k)).wait_recv()

    weights = []
    for b in range(nx):
        value = jnp.float32(0.0)
        for t in range(tab_ref.shape[0]):
            value = value + jnp.where(idx_ref[b] == t, tab_ref[t], jnp.float32(0.0))
        weights.append(value)

    row_index = lax.broadcasted_iota(jnp.int32, (nx, BLK), 0)
    row_weights = []
    for h in range(nk):
        value = jnp.zeros((nx, BLK), jnp.float32)
        for b in range(nx // nk):
            value = jnp.where((row_index >= 2 * b) & (row_index < 2 * b + 2), weights[h * (nx // nk) + b], value)
        row_weights.append(value)
    columns = jnp.transpose(dcm[...])
    line_near(d_col)
    far = []
    for i, (step, piece) in enumerate(((1, top), (ny - 1, low))):
        dprow[i].wait_recv()
        far.append(far_block(step, piece, 2 + i))
        far[-1].start()
    with jax.named_scope("a2a"):
        all_here(a2a_r.at[0], mall.at[0:nx - 1])
    total = jnp.zeros((BLK, BLK), jnp.float32)
    spread_row = jnp.zeros((1, BLK), jnp.float32)
    for b in range(nx):
        term = jnp.zeros((BLK, BLK), jnp.float32)
        for p in range(2):
            at_row = columns[:, 8 * b + p:8 * b + p + 1]
            at_col = drt[b, p:p + 1, :]
            term = term + mall[b, p] * (at_row - at_col)
        total = total + (2.0 * weights[b]) * term
        re_d, im_d = drt[b, 0:1, :], drt[b, 1:2, :]
        spread_row = spread_row + weights[b] * (1.0 - re_d * re_d - im_d * im_d)
    gblk[...] = total
    own_p = gp_ref[:, lanes(x)]
    first_line = (r == 0).astype(jnp.float32)
    sums = [total * total, total * own_d, own_d * own_d, own_p * own_p]
    row_sums = [jnp.sum(value, axis=0, keepdims=True) for value in sums] + [spread_row * first_line]
    row_sums.append(jnp.zeros((8 - len(row_sums), BLK), jnp.float32))
    row_sums = jnp.sum(jnp.concatenate(row_sums, axis=0), axis=1, keepdims=True)
    pick = lax.broadcasted_iota(jnp.int32, (8, BLK), 0) == lax.broadcasted_iota(jnp.int32, (8, BLK), 1)
    stile[...] = jnp.sum(jnp.where(pick, row_sums, 0.0), axis=0, keepdims=True)

    def small_plane(stage, src, dst):
        dst[pl.ds(c, 1)] = src[...][None]
        copies = []
        for i, (ox, oy) in enumerate(plane):
            copy = remote(src, dst.at[c], sml_s.at[stage], sml_r.at[stage], at_plane(ox, oy))
            copy.start()
            copies.append(copy)
        return copies

    def small_line(stage, src, dst):
        dst[pl.ds(r, 1)] = src(r)[...][None]
        copies = []
        for i, (oz, ok) in enumerate(others):
            rp = nk * off(z, oz, nz) + off(k, ok, nk)
            copy = remote(src(rp), dst.at[r], sml_s.at[stage], sml_r.at[stage], at_line(oz, ok))
            copy.start()
            copies.append(copy)
        return copies

    def summed(ref):
        value = ref[0]
        for i in range(1, count):
            value = value + ref[i]
        return value

    copies = small_line(0, lambda index: stile, sx)
    grow[:, lanes(c)] = total
    gcol[lanes(r), :] = total
    rows = plane_start(0, gblk, grow)
    cols = line_start(1, gblk, column_slots(gcol))
    with jax.named_scope("small0"):
        all_here(sml_r.at[0], sx.at[0:count - 1])
    all_sent(sml_s.at[0], sx.at[0:count - 1])
    stile[...] = summed(sx)
    copies = small_plane(1, stile, sz)
    line_forward(cols)
    plane_forward(rows)
    line_near(cols)
    line_finish(d_col)
    with jax.named_scope("far"):
        for copy in far:
            copy.wait_recv()
    all_sent(dpr_s.at[0], pieces_of(order // BLK * 3 / 4))
    all_sent(a2a_s.at[0], mall.at[0:nx - 1])
    line_far(cols)
    plane_finish(rows)
    line_mid(cols)
    with jax.named_scope("small1"):
        all_here(sml_r.at[1], sz.at[0:count - 1])
    all_sent(sml_s.at[1], sz.at[0:count - 1])
    sums = jnp.sum(jnp.where(pick, summed(sz), 0.0), axis=1, keepdims=True)
    gg, gd, dd, pp, spread = (jnp.broadcast_to(sums[i:i + 1, :], (1, BLK)) for i in range(5))
    spread = spread / order
    beta = gg / (1.0 + pp)
    norm = jnp.maximum(gg - 2.0 * beta * gd + beta * beta * dd, 0.0)
    scale = STEP_SCALE / jnp.sqrt(1.0 + norm / order)

    chunk = 4 * BLK if order % (4 * BLK) == 0 else BLK
    beta_w = jnp.concatenate([beta] * nk, axis=1)
    scale_w = jnp.concatenate([scale] * nk, axis=1)

    def square(acc, steps):
        for at in part_of_sum(steps):
            left = scale_w * (beta_w * drow[:, at] - grow[:, at])
            right = scale * (beta * dcol[at, :] - gcol[at, :])
            acol[at, :] = right
            acc = acc + dot_split(split(left), split(right))
        return acc

    acc = square(jnp.zeros((BLK, BLK), jnp.float32), close)
    line_done(cols)
    acc = square(acc, distant)
    blk1[...] = acol[lanes(r), :]
    blk2[...] = acc
    row2[:, lanes(c)] = acc
    col2[lanes(r), :] = acc
    rows = plane_start(1, blk2, row2)
    cols = line_start(2, blk2, column_slots(col2))
    for j in range(nx):
        at = pl.ds(pl.multiple_of(y * wide + j * BLK, BLK), BLK)
        piece = grow[:, at]
        grad_ref[:, j * BLK:(j + 1) * BLK] = piece
        dir_ref[:, j * BLK:(j + 1) * BLK] = beta * drow[:, at] - piece

    for b in range(nx):
        for p in range(2):
            i = 2 * b + p
            high, tail = split(jnp.transpose(mall[b, p]))
            mt[i * BLK:(i + 1) * BLK, :] = jnp.concatenate([high, tail, high], axis=1)
    line_forward(cols)
    plane_forward(rows)
    line_near(cols)
    acc3 = plane_sum(
        rows, row2, lambda at: acol[at, :], jnp.zeros((BLK, BLK), jnp.float32), lambda: line_far(cols)
    )
    blk3[...] = acc3
    row3[:, lanes(c)] = acc3
    more = plane_start(4, blk3, row3)
    line_mid(cols)

    def fourth(acc, steps):
        for at in part_of_sum(steps):
            acc = acc + dot_split(split(row2[:, at]), split(col2[at, :]))
        return acc

    acc4 = fourth(jnp.zeros((BLK, BLK), jnp.float32), close)
    line_done(cols)
    acc4 = fourth(acc4, distant)
    blk4[...] = acc4
    row4[:, lanes(c)] = acc4
    col4[lanes(r), :] = acc4
    cols = line_start(3, blk4, column_slots(col4))
    rows = plane_start(2, blk4, row4)
    plane_forward(more)
    for at in range(0, order, chunk):
        acol[at:at + chunk, :] = col2[at:at + chunk, :] * (1.0 / 720.0)
        gcol[at:at + chunk, :] = col2[at:at + chunk, :] * (1.0 / 120.0)
    line_forward(cols)
    line_near(cols)
    plane_forward(rows)
    line_finish(cols)
    plane_finish(more)

    odd = jnp.zeros((BLK, BLK), jnp.float32)
    for at in range(0, order, chunk):
        right = gcol[at:at + chunk, :] + col4[at:at + chunk, :] * (1.0 / 5040.0)
        odd = odd + dot_split(split(row3[:, at:at + chunk]), split(right))
    odd = odd + blk1[...] + blk3[...] * (1.0 / 6.0)
    def even_columns(at):
        return acol[at, :] + col4[at, :] * (1.0 / 40320.0)

    even = plane_sum(rows, row4, even_columns, jnp.zeros((BLK, BLK), jnp.float32))
    even = even + blk2[...] * 0.5 + blk4[...] * (1.0 / 24.0)
    even = even + jnp.where(eye & jnp.logical_not(off_diag), 1.0, 0.0)

    eblk[...] = even + odd
    etr[...] = jnp.transpose(even - odd)
    cols = line_start(4, etr, row_slots(ej))
    rows = plane_start(3, eblk, erow)
    erow[:, lanes(c)] = eblk[...]
    ej[:, lanes(r)] = etr[...]
    plane_forward(rows)
    line_forward(cols)
    line_near(cols)

    def turn(g):
        slots = plane_pieces(rows, groups[g])
        high, tail = split(jnp.concatenate([erow[:, at] for at in slots], axis=1))
        turned[g] = dot(mt[...], jnp.concatenate([high, high, tail], axis=0))

    for g in range(len(groups) - 1):
        turn(g)
    line_far(cols)
    turn(len(groups) - 1)
    plane_done(rows)

    hall = [(ox, oy, ok) for ox in range(nx) for oy in range(ny) for ok in range(nk)]

    def at_hall(ox, oy, ok):
        return dev(off(x, ox, nx), off(y, oy, ny), z, off(k, ok, nk))

    line_mid(cols)
    line_done(cols)
    own = nk * c + k
    copies = []
    for g, pieces in enumerate(groups):
        for i, (ox, oy) in enumerate(pieces):
            back = (nx - ox) % nx, (ny - oy) % ny
            place = nx * off(y, back[1], ny) + off(x, back[0], nx)
            left = ej[:, lanes(place)]
            sums = jnp.concatenate(
                [
                    jnp.sum(left * turned[g, j * BLK:(j + 1) * BLK, i * BLK:(i + 1) * BLK], axis=0, keepdims=True)
                    for j in range(2 * nx)
                ],
                axis=0,
            )
            for h in range(nk):
                part[nk * (4 * g + i) + h] = sums[h * nx:(h + 1) * nx]
        for i, (ox, oy) in enumerate(pieces):
            back = (nx - ox) % nx, (ny - oy) % ny
            for ok in range(nk):
                src = part.at[nk * (4 * g + i) + off(k, ok, nk)]
                if (ox, oy, ok) == (0, 0, 0):
                    pz[pl.ds(own, 1)] = part[pl.ds(nk * (4 * g + i) + k, 1)]
                else:
                    at = hall.index((*back, ok))
                    copies.append(remote(src, pz.at[own], sml_s.at[2], sml_r.at[2], at_hall(*back, ok)))
                    copies[-1].start()
    with jax.named_scope("small2"):
        all_here(sml_r.at[2], pz.at[0:nk * count - 1])
    all_sent(sml_s.at[2], pz.at[0:nk * count - 1])
    value = pz[0]
    for i in range(1, nk * count):
        value = value + pz[i]
    ttile[...] = value
    px[pl.ds(z, 1)] = value[None]
    copies = []
    for oz in range(1, nz):
        copies.append(remote(ttile, px.at[z], sml_s.at[3], sml_r.at[3], at_line(oz, 0)))
        copies[-1].start()
    with jax.named_scope("small3"):
        all_here(sml_r.at[3], px.at[0:nz - 1])
    all_sent(sml_s.at[3], px.at[0:nz - 1])
    value = px[0]
    for i in range(1, nz):
        value = value + px[i]
    qtile[...] = value
    tfin[pl.ds(own, 1)] = value[None]
    copies = []
    for i, (ox, oy, ok) in enumerate(hall[1:]):
        copies.append(remote(qtile, tfin.at[own], sml_s.at[4], sml_r.at[4], at_hall(ox, oy, ok)))
        copies[-1].start()

    @pl.when(holds & (x == px_t))
    def _():
        all_sent(dia_s.at[0], gcol.at[0:8 * (count + len(line) - 2), :])

    @pl.when(holds & (x != px_t))
    def _():
        all_sent(dia_s.at[0], gcol.at[0:8 * (count + len(line) - 1), :])

    with jax.named_scope("small4"):
        all_here(sml_r.at[4], tfin.at[0:nk * count - 1])
    all_sent(sml_s.at[4], tfin.at[0:nk * count - 1])
    trial = jnp.zeros((nx, BLK), jnp.float32)
    for h in range(nk):
        value = jnp.zeros((nx, BLK), jnp.float32)
        for i in range(count):
            value = value + (0.5 - tfin[nk * i + h] * tfin[nk * i + h])
        trial = trial + value * row_weights[h]
    trial = jnp.sum(trial, axis=0, keepdims=True)
    stat_ref[...] = jnp.zeros((8, BLK), jnp.float32)
    stat_ref[0:1, :] = spread
    stat_ref[1:2, :] = jnp.broadcast_to(jnp.sum(trial, axis=1, keepdims=True) / order, (1, BLK))


def hand_out(grad_ref, dir_ref, trial_ref, stat_ref, spread_out, trial_spread_out, grad_out, dir_out, trial_out):
    spread_out[0, 0] = jnp.sum(stat_ref[0:1, 0:1])
    trial_spread_out[0, 0] = jnp.sum(stat_ref[1:2, 0:1])
    grad_out[...] = grad_ref[...]
    dir_out[...] = dir_ref[...]
    halves = trial_out.shape[0] // 2
    for i in range(trial_ref.shape[0] // 2):
        for b in range(trial_out.shape[0]):
            at = 2 * (b % halves)
            trial_out[b, :, i * BLK:(i + 1) * BLK] = trial_ref[2 * i + b // halves, at:at + 2, :]


def shards(dims, m_matrices, bvec_index, weight_table, grad_prev, dir_prev):
    nx, ny, nz, nk = dims
    count = nx * ny
    order = count * BLK
    f32 = jnp.float32
    rows, cols = grad_prev.shape
    vmem = pl.BlockSpec(memory_space=pltpu.VMEM)
    smem = pl.BlockSpec(memory_space=pltpu.SMEM)
    wide = pltpu.VMEM((BLK, order), f32)
    tall = pltpu.VMEM((order, BLK), f32)
    block = pltpu.VMEM((BLK, BLK), f32)
    tile = pltpu.VMEM((8, BLK), f32)
    half_tile = pltpu.VMEM((nx, BLK), f32)
    line = pltpu.VMEM((1, BLK), f32)
    lines = pltpu.VMEM((count, 1, BLK), f32)
    dma = pltpu.SemaphoreType.DMA
    grad, direction, trial, stat = pl.pallas_call(
        functools.partial(kernel, dims),
        out_shape=(
            jax.ShapeDtypeStruct((rows, cols), f32),
            jax.ShapeDtypeStruct((rows, cols), f32),
            jax.ShapeDtypeStruct((nk * count, nx, BLK), f32),
            jax.ShapeDtypeStruct((8, BLK), f32),
        ),
        in_specs=[pl.BlockSpec(memory_space=pltpu.HBM)] * 5,
        out_specs=(vmem, vmem, vmem, vmem),
        scratch_shapes=[
            pltpu.SMEM(bvec_index.shape, jnp.int32), pltpu.SMEM(weight_table.shape, f32),
            pltpu.VMEM(m_matrices.shape[1:], f32), pltpu.VMEM((rows, cols), f32), pltpu.VMEM((rows, cols), f32), dma((5,)),
            pltpu.VMEM((nx, 2, BLK, BLK), f32), block, pltpu.VMEM((nx, 8, BLK), f32), tile,
            block, block, block, block, block, block, block, block, line, lines, lines,
            wide, tall, wide, tall, tall, wide, tall, wide, wide, tall, wide, wide,
            pltpu.VMEM((2 * nx * BLK, 3 * BLK), jnp.bfloat16), pltpu.VMEM((count // 4, 2 * nx * BLK, 4 * BLK), f32),
            pltpu.VMEM((nk * count, nx, BLK), f32), pltpu.VMEM((nk * count, nx, BLK), f32), pltpu.VMEM((nz, nx, BLK), f32),
            half_tile, half_tile,
            dma((1,)), dma((1,)),
            dma((1,)), dma((2 * nx,)),
            dma((1,)), dma((4,)),
            dma((3,)), dma((3, 10)),
            dma((3,)), dma((3, 9)),
            dma((3,)), dma((3, 2)),
            dma((5,)), dma((5,)),
        ],
        compiler_params=pltpu.CompilerParams(
            collective_id=0, has_side_effects=True, vmem_limit_bytes=40 * 1024 * 1024
        ),
    )(*(
        pltpu.with_memory_space_constraint(array, pltpu.HBM)
        for array in (m_matrices.reshape(m_matrices.shape[1:]), dir_prev, grad_prev, bvec_index, weight_table)
    ))
    one = jax.ShapeDtypeStruct((1, 1), f32)
    block_out = jax.ShapeDtypeStruct((rows, cols), f32)
    spread, trial_spread, grad, direction, trial = pl.pallas_call(
        hand_out,
        out_shape=(one, one, block_out, block_out, jax.ShapeDtypeStruct((nx, 2, order), f32)),
        in_specs=[vmem] * 4,
        out_specs=(smem, smem, vmem, vmem, vmem),
        compiler_params=pltpu.CompilerParams(vmem_limit_bytes=8 * 1024 * 1024),
    )(grad, direction, trial, stat)
    return spread.reshape(()), trial_spread.reshape(()), grad, direction, trial


def solution(mesh):
    nx, ny, nk = mesh.shape["bvec"], mesh.shape["col"], 2
    nz = mesh.shape["row"] // nk
    torus = Mesh(mesh.devices.reshape(nx, nz, nk, ny), ("bvec", "zed", "core", "col"))
    return jax.shard_map(
        functools.partial(shards, (nx, ny, nz, nk)),
        mesh=torus,
        in_specs=(P("bvec", None, ROW, "col"), P(), P(), P(ROW, "col"), P(ROW, "col")),
        out_specs=(P(), P(), P(ROW, "col"), P(ROW, "col"), P()),
        check_vma=False,
    )
```

```python
import functools

import jax
import jax.numpy as jnp
from jax import lax
from jax.experimental import pallas as pl
from jax.experimental.pallas import tpu as pltpu
from jax.sharding import Mesh
from jax.sharding import PartitionSpec as P

ROW = ("zed", "core")
STEP_SCALE = 1.75
BLK = 128
MESH = pl.DeviceIdType.MESH


def split(value):
    high = value.astype(jnp.bfloat16)
    low = (value - high.astype(jnp.float32)).astype(jnp.bfloat16)
    return high, low


def dot(left, right):
    return jnp.dot(left, right, preferred_element_type=jnp.float32)


def dot_split(left, right):
    (lh, ll), (rh, rl) = left, right
    size = rh.shape[1]
    both = dot(lh, jnp.concatenate([rh, rl], axis=1))
    return both[:, :size] + (both[:, size:] + dot(ll, rh))


def kernel(
    dims, m_in, dp_in, gp_in, idx_in, tab_in,
    grad_ref, dir_ref, tfin, stat_ref,
    idx_ref, tab_ref, m_ref, gp_ref, dp_ref, in_s,
    mall, dcm, drt, dsrc, gblk, blk1, blk2, blk3, blk4, eblk, etr, own_block, stile, sx, sz,
    drow, dcol, grow, gcol, acol, row2, col2, row3, row4, col4, erow, ej, mt, turned, part, pz, px, qtile, ttile,
    a2a_s, a2a_r, dia_s, dia_r, dpr_s, dpr_r, row_s, row_r, col_s, col_r, fwd_s, fwd_r, sml_s, sml_r,
):
    nx, ny, nz, nk = dims
    count = nx * ny
    order = count * BLK
    wide = nx * BLK
    x, y = lax.axis_index("bvec"), lax.axis_index("col")
    z, k = lax.axis_index("zed"), lax.axis_index("core")
    r = nk * z + k
    c = nx * y + x

    def dev(xx, yy, zz, kk):
        return {"bvec": xx, "zed": zz, "core": kk, "col": yy}

    def off(value, step, size):
        return lax.rem(value + step, size) if step else value

    def lanes(index, size=BLK):
        return pl.ds(pl.multiple_of(index * size, size), size)

    plane = [(ox, oy) for ox in range(nx) for oy in range(ny) if (ox, oy) != (0, 0)]
    line = [(oz, ok) for oz in range(nz) for ok in range(nk)]
    others = line[1:]

    def at_plane(ox, oy):
        return dev(off(x, ox, nx), off(y, oy, ny), z, k)

    def at_line(oz, ok):
        return dev(x, y, off(z, oz, nz), off(k, ok, nk))

    px_t, py_t = lax.rem(r, nx), lax.div(r, nx)
    pz_t, pk_t = lax.div(c, nk), lax.rem(c, nk)
    off_diag = r != c
    holds = y == py_t

    loads = [
        pltpu.make_async_copy(src, dst, in_s.at[i])
        for i, (src, dst) in enumerate(
            ((m_in, m_ref), (dp_in, dp_ref), (gp_in, gp_ref), (idx_in, idx_ref), (tab_in, tab_ref))
        )
    ]
    for copy in loads:
        copy.start()

    barrier = pltpu.get_barrier_semaphore()
    for ox, oy in plane:
        pl.semaphore_signal(barrier, inc=1, device_id=at_plane(ox, oy), device_id_type=MESH)
    for oz, ok in others:
        pl.semaphore_signal(barrier, inc=1, device_id=at_line(oz, ok), device_id_type=MESH)

    for b in range(nx):
        @pl.when((x != b) | off_diag)
        def _(b=b):
            pl.semaphore_signal(barrier, inc=1, device_id=dev(b, y, pz_t, pk_t), device_id_type=MESH)

    for copy in loads:
        copy.wait()

    own_d = dp_ref[:, lanes(x)]
    eye_r = lax.broadcasted_iota(jnp.int32, (BLK, BLK), 0)
    eye_c = lax.broadcasted_iota(jnp.int32, (BLK, BLK), 1)
    eye = eye_r == eye_c
    dsrc[...] = jnp.zeros((8, BLK), jnp.float32)
    for p in range(2):
        dsrc[p:p + 1, :] = jnp.sum(jnp.where(eye, m_ref[p, :, lanes(px_t)], 0.0), axis=0, keepdims=True)
    if nx * 8 < BLK:
        dcm[nx * 8:, :] = jnp.zeros((BLK - nx * 8, BLK), jnp.float32)

    expected = len(plane) + len(others)
    asked = len(line) - (x == px_t).astype(jnp.int32)
    with jax.named_scope("barrier"):
        pl.semaphore_wait(barrier, expected + holds.astype(jnp.int32) * asked)

    def remote(src, dst, send, recv, device):
        return pltpu.make_async_remote_copy(
            src_ref=src, dst_ref=dst, send_sem=send, recv_sem=recv, device_id=device, device_id_type=MESH
        )

    def all_sent(sem, ref):
        remote(ref, ref, sem, sem, dev(x, y, z, k)).wait_send()

    def all_here(sem, ref):
        remote(ref, ref, sem, sem, dev(x, y, z, k)).wait_recv()

    def pieces_of(count_blocks):
        return gcol.at[0:int(count_blocks * BLK), :]

    dia_row = [
        remote(dsrc, dcm.at[pl.ds(pl.multiple_of(8 * x, 8), 8), :], dia_s.at[0], dia_r.at[x], at_plane(ox, oy))
        for i, (ox, oy) in enumerate(plane)
    ]
    dia_col = [
        remote(dsrc, drt.at[x], dia_s.at[0], dia_r.at[nx + x],
               dev(px_t, y, off(z, oz, nz), off(k, ok, nk)))
        for i, (oz, ok) in enumerate(line)
    ]

    @pl.when(holds)
    def _():
        for copy in dia_row:
            copy.start()
        for copy in dia_col[1:]:
            copy.start()
        dcm[pl.ds(pl.multiple_of(8 * x, 8), 8), :] = dsrc[...]

    @pl.when(holds & (x != px_t))
    def _():
        dia_col[0].start()

    @pl.when(jnp.logical_not(off_diag))
    def _():
        drt[pl.ds(x, 1)] = dsrc[...][None]

    a2a = []
    for ox in range(1, nx):
        xp = off(x, ox, nx)
        copy = remote(m_ref.at[:, :, lanes(xp)], mall.at[x], a2a_s.at[0], a2a_r.at[0], dev(xp, y, z, k))
        copy.start()
        a2a.append(copy)

    def wait_all(copies, name="wait"):
        with jax.named_scope(name):
            for copy in copies:
                copy.wait()

    half = BLK // 2
    top, low = slice(0, half), slice(half, BLK)

    def far_block(step, part, index):
        held = drow.at[part, lanes(off(y, ny - step, ny), wide)]
        return remote(held, held, dpr_s.at[0], dpr_r.at[index], at_plane(0, step))

    dprow = []
    for i, oy in enumerate((1, ny - 1)):
        copy = remote(dp_ref, drow.at[:, lanes(y, wide)], dpr_s.at[0], dpr_r.at[i], at_plane(0, oy))
        copy.start()
        dprow.append(copy)

    ring_x = [1, nx - 1, 2]
    ring_y = [1, ny - 1, 2]

    arrivals = [(0, 0), (1, 0), (0, 1), (nx - 1, 0), (0, ny - 1), (2, 0), (0, 2)]
    arrivals += [(ox, oy) for ox in (1, nx - 1) for oy in (1, ny - 1)]
    arrivals += [(ox, oy) for ox, oy in plane if ox and oy and 2 in (ox, oy) and ox != oy] + [(2, 2)]
    groups = [arrivals[i:i + 4] for i in range(0, len(arrivals), 4)]

    def group_sem(bank, ox, oy):
        return row_r.at[bank, 6 + [g for g, pieces in enumerate(groups) if (ox, oy) in pieces][0]]

    def plane_start(stage, src, dst):
        bank = 2 if stage == 4 else stage % 2
        first = []
        for n, (over_x, over_y) in enumerate(((top, low), (low, top))):
            for i in range(3):
                for m, part_of, device in ((0, over_x, at_plane(ring_x[i], 0)), (1, over_y, at_plane(0, ring_y[i]))):
                    step = (0, ring_y[i]) if m else (ring_x[i], 0)
                    sem = group_sem(bank, *step) if n else row_r.at[bank, 2 * i + m]
                    first.append(remote(src.at[part_of, :], dst.at[part_of, lanes(c)], row_s.at[bank], sem, device))
                    first[-1].start()
        return stage, bank, dst, first, []

    def plane_forward(state):
        stage, bank, dst, first, second = state
        with jax.named_scope(f"row{stage}a"):
            for i in range(3):
                first[2 * i].wait_recv()
                held = dst.at[top, lanes(nx * y + off(x, nx - ring_x[i], nx))]
                for j in (2, 0, 1):
                    sem = group_sem(bank, ring_x[i], ring_y[j])
                    second.append(remote(held, held, row_s.at[bank], sem, at_plane(0, ring_y[j])))
                    second[-1].start()
                first[2 * i + 1].wait_recv()
                held = dst.at[low, lanes(nx * off(y, ny - ring_y[i], ny) + x)]
                for j in (2, 0, 1):
                    sem = group_sem(bank, ring_x[j], ring_y[i])
                    second.append(remote(held, held, row_s.at[bank], sem, at_plane(ring_x[j], 0)))
                    second[-1].start()

    def plane_pieces(state, pieces):
        stage, bank, _, _, _ = state
        halves = sum(2 if ox and oy else 1 for ox, oy in pieces if (ox, oy) != (0, 0))
        with jax.named_scope(f"row{stage}w"):
            all_here(row_r.at[bank, 6 + groups.index(pieces)], pieces_of(halves / 2))
        return [lanes(nx * off(y, ny - oy if oy else 0, ny) + off(x, nx - ox if ox else 0, nx)) for ox, oy in pieces]

    def plane_sum(state, left, right, acc, before_last=lambda: None):
        for pieces in groups:
            if pieces is groups[-2]:
                before_last()
            places = plane_pieces(state, pieces)
            rows_l = jnp.concatenate([left[:, at] for at in places], axis=1)
            cols_r = jnp.concatenate([right(at) for at in places], axis=0)
            acc = acc + dot_split(split(rows_l), split(cols_r))
        plane_done(state)
        return acc

    def plane_done(state):
        all_sent(row_s.at[state[1]], pieces_of(count - 1))

    def plane_finish(state):
        for pieces in groups:
            plane_pieces(state, pieces)
        plane_done(state)

    def line_start(stage, src, slot):
        bank = (2, 0, 1, 0, 1)[stage]
        whole = slice(0, BLK)
        first = {}
        order_z = ((2, top), (nz - 2, low), (2, low), (nz - 2, top), (1, whole), (nz - 1, whole))
        for i, (oz, piece) in enumerate(order_z):
            first[oz, piece.start] = remote(
                src.at[piece, :], slot(r, piece), col_s.at[bank], col_r.at[bank, i], at_line(oz, 0)
            )
            first[oz, piece.start].start()
        over = [remote(src, slot(r), fwd_s.at[bank], fwd_r.at[bank, 0], at_line(0, 1))]
        over[0].start()
        return stage, bank, slot, first, {}, over

    def line_across(state, oz):
        stage, bank, slot, first, second, over = state
        held = slot(nk * off(z, nz - oz, nz) + k)
        over.append(remote(held, held, fwd_s.at[bank], fwd_r.at[bank, 1 if oz in distant else 0], at_line(0, 1)))
        over[-1].start()

    def line_forward(state):
        stage, bank, slot, first, second, over = state
        with jax.named_scope(f"line{stage}a"):
            steps = ((2, top, (2, 1)), (nz - 2, low, (nz - 2, nz - 1)), (2, low, (1,)), (nz - 2, top, (nz - 1,)))
            for oz, piece, onward in steps:
                first[oz, piece.start].wait_recv()
                held = slot(nk * off(z, nz - oz, nz) + k, piece)
                for step in onward:
                    at = 6 + distant.index((oz + step) % nz)
                    remote(held, held, col_s.at[bank], col_r.at[bank, at], at_line(step, 0)).start()

    def line_near(state):
        stage, bank, slot, first, second, over = state
        with jax.named_scope(f"line{stage}n"):
            for oz in (2, nz - 2, 1, nz - 1):
                if oz in (1, nz - 1):
                    first[oz, 0].wait_recv()
                line_across(state, oz)

    close = (0, 2, nz - 2, 1, nz - 1)
    distant = (3, nz - 3, 4)

    def line_far(state):
        stage, bank, slot, first, second, over = state
        with jax.named_scope(f"line{stage}f"):
            for oz in (3, nz - 3, 4):
                all_here(col_r.at[bank, 6 + distant.index(oz)], pieces_of(1))
                line_across(state, oz)

    def line_mid(state):
        with jax.named_scope(f"line{state[0]}m"):
            all_here(fwd_r.at[state[1], 0], pieces_of(len(close)))

    def line_done(state):
        stage, bank, slot, first, second, over = state
        with jax.named_scope(f"line{stage}d"):
            all_here(fwd_r.at[bank, 1], pieces_of(len(distant)))
            all_sent(fwd_s.at[bank], pieces_of(nz))
            all_sent(col_s.at[bank], pieces_of(nz - 1))

    def line_finish(state):
        line_far(state)
        line_mid(state)
        line_done(state)

    def part_of_sum(steps):
        size = nk * BLK
        return [pl.ds(pl.multiple_of(off(z, step, nz) * size, size), size) for step in steps]

    def column_slots(ref):
        def slot(index, part=slice(0, BLK)):
            return ref.at[pl.ds(pl.multiple_of(index * BLK + part.start, half), part.stop - part.start), :]
        return slot

    def row_slots(ref):
        return lambda index, part=slice(0, BLK): ref.at[part, lanes(index)]

    own_block[...] = own_d
    d_col = line_start(0, own_block, column_slots(dcol))

    mall[pl.ds(x, 1)] = m_ref[:, :, lanes(x)][None]
    drow[:, lanes(y, wide)] = dp_ref[...]
    dcol[lanes(r), :] = own_d
    line_forward(d_col)

    for b in range(nx):
        @pl.when(jnp.logical_not(holds & (x == b)))
        @jax.named_scope("diag_r")
        def _(b=b):
            slot = dcm.at[8 * b:8 * b + 8, :]
            remote(slot, slot, dia_s.at[0], dia_r.at[b], dev(x, y, z, k)).wait_recv()

        @pl.when(off_diag | (x != b))
        def _(b=b):
            slot = drt.at[b]
            remote(slot, slot, dia_s.at[0], dia_r.at[nx + b], dev(x, y, z, k)).wait_recv()

    weights = []
    for b in range(nx):
        value = jnp.float32(0.0)
        for t in range(tab_ref.shape[0]):
            value = value + jnp.where(idx_ref[b] == t, tab_ref[t], jnp.float32(0.0))
        weights.append(value)

    row_index = lax.broadcasted_iota(jnp.int32, (nx, BLK), 0)
    row_weights = []
    for h in range(nk):
        value = jnp.zeros((nx, BLK), jnp.float32)
        for b in range(nx // nk):
            value = jnp.where((row_index >= 2 * b) & (row_index < 2 * b + 2), weights[h * (nx // nk) + b], value)
        row_weights.append(value)
    columns = jnp.transpose(dcm[...])
    line_near(d_col)
    far = []
    for i, (step, piece) in enumerate(((1, top), (ny - 1, low))):
        dprow[i].wait_recv()
        far.append(far_block(step, piece, 2 + i))
        far[-1].start()
    with jax.named_scope("a2a"):
        all_here(a2a_r.at[0], mall.at[0:nx - 1])
    total = jnp.zeros((BLK, BLK), jnp.float32)
    spread_row = jnp.zeros((1, BLK), jnp.float32)
    for b in range(nx):
        term = jnp.zeros((BLK, BLK), jnp.float32)
        for p in range(2):
            at_row = columns[:, 8 * b + p:8 * b + p + 1]
            at_col = drt[b, p:p + 1, :]
            term = term + mall[b, p] * (at_row - at_col)
        total = total + (2.0 * weights[b]) * term
        re_d, im_d = drt[b, 0:1, :], drt[b, 1:2, :]
        spread_row = spread_row + weights[b] * (1.0 - re_d * re_d - im_d * im_d)
    gblk[...] = total
    own_p = gp_ref[:, lanes(x)]
    first_line = (r == 0).astype(jnp.float32)
    sums = [total * total, total * own_d, own_d * own_d, own_p * own_p]
    row_sums = [jnp.sum(value, axis=0, keepdims=True) for value in sums] + [spread_row * first_line]
    row_sums.append(jnp.zeros((8 - len(row_sums), BLK), jnp.float32))
    row_sums = jnp.sum(jnp.concatenate(row_sums, axis=0), axis=1, keepdims=True)
    pick = lax.broadcasted_iota(jnp.int32, (8, BLK), 0) == lax.broadcasted_iota(jnp.int32, (8, BLK), 1)
    stile[...] = jnp.sum(jnp.where(pick, row_sums, 0.0), axis=0, keepdims=True)

    def small_plane(stage, src, dst):
        dst[pl.ds(c, 1)] = src[...][None]
        copies = []
        for i, (ox, oy) in enumerate(plane):
            copy = remote(src, dst.at[c], sml_s.at[stage], sml_r.at[stage], at_plane(ox, oy))
            copy.start()
            copies.append(copy)
        return copies

    def small_line(stage, src, dst):
        dst[pl.ds(r, 1)] = src(r)[...][None]
        copies = []
        for i, (oz, ok) in enumerate(others):
            rp = nk * off(z, oz, nz) + off(k, ok, nk)
            copy = remote(src(rp), dst.at[r], sml_s.at[stage], sml_r.at[stage], at_line(oz, ok))
            copy.start()
            copies.append(copy)
        return copies

    def summed(ref):
        value = ref[0]
        for i in range(1, count):
            value = value + ref[i]
        return value

    copies = small_line(0, lambda index: stile, sx)
    grow[:, lanes(c)] = total
    gcol[lanes(r), :] = total
    rows = plane_start(0, gblk, grow)
    cols = line_start(1, gblk, column_slots(gcol))
    with jax.named_scope("small0"):
        all_here(sml_r.at[0], sx.at[0:count - 1])
    all_sent(sml_s.at[0], sx.at[0:count - 1])
    stile[...] = summed(sx)
    copies = small_plane(1, stile, sz)
    line_forward(cols)
    plane_forward(rows)
    line_near(cols)
    line_finish(d_col)
    with jax.named_scope("far"):
        for copy in far:
            copy.wait_recv()
    all_sent(dpr_s.at[0], pieces_of(order // BLK * 3 / 4))
    all_sent(a2a_s.at[0], mall.at[0:nx - 1])
    line_far(cols)
    plane_finish(rows)
    line_mid(cols)
    with jax.named_scope("small1"):
        all_here(sml_r.at[1], sz.at[0:count - 1])
    all_sent(sml_s.at[1], sz.at[0:count - 1])
    sums = jnp.sum(jnp.where(pick, summed(sz), 0.0), axis=1, keepdims=True)
    gg, gd, dd, pp, spread = (jnp.broadcast_to(sums[i:i + 1, :], (1, BLK)) for i in range(5))
    spread = spread / order
    beta = gg / (1.0 + pp)
    norm = jnp.maximum(gg - 2.0 * beta * gd + beta * beta * dd, 0.0)
    scale = STEP_SCALE / jnp.sqrt(1.0 + norm / order)

    chunk = 4 * BLK if order % (4 * BLK) == 0 else BLK
    beta_w = jnp.concatenate([beta] * nk, axis=1)
    scale_w = jnp.concatenate([scale] * nk, axis=1)

    def square(acc, steps):
        for at in part_of_sum(steps):
            left = scale_w * (beta_w * drow[:, at] - grow[:, at])
            right = scale * (beta * dcol[at, :] - gcol[at, :])
            acol[at, :] = right
            acc = acc + dot_split(split(left), split(right))
        return acc

    acc = square(jnp.zeros((BLK, BLK), jnp.float32), close)
    line_done(cols)
    acc = square(acc, distant)
    blk1[...] = acol[lanes(r), :]
    blk2[...] = acc
    row2[:, lanes(c)] = acc
    col2[lanes(r), :] = acc
    rows = plane_start(1, blk2, row2)
    cols = line_start(2, blk2, column_slots(col2))
    for j in range(nx):
        at = pl.ds(pl.multiple_of(y * wide + j * BLK, BLK), BLK)
        piece = grow[:, at]
        grad_ref[:, j * BLK:(j + 1) * BLK] = piece
        dir_ref[:, j * BLK:(j + 1) * BLK] = beta * drow[:, at] - piece

    for b in range(nx):
        for p in range(2):
            i = 2 * b + p
            high, tail = split(jnp.transpose(mall[b, p]))
            mt[i * BLK:(i + 1) * BLK, :] = jnp.concatenate([high, tail, high], axis=1)
    line_forward(cols)
    plane_forward(rows)
    line_near(cols)
    acc3 = plane_sum(
        rows, row2, lambda at: acol[at, :], jnp.zeros((BLK, BLK), jnp.float32), lambda: line_far(cols)
    )
    blk3[...] = acc3
    row3[:, lanes(c)] = acc3
    more = plane_start(4, blk3, row3)
    line_mid(cols)

    def fourth(acc, steps):
        for at in part_of_sum(steps):
            acc = acc + dot_split(split(row2[:, at]), split(col2[at, :]))
        return acc

    acc4 = fourth(jnp.zeros((BLK, BLK), jnp.float32), close)
    line_done(cols)
    acc4 = fourth(acc4, distant)
    blk4[...] = acc4
    row4[:, lanes(c)] = acc4
    col4[lanes(r), :] = acc4
    cols = line_start(3, blk4, column_slots(col4))
    rows = plane_start(2, blk4, row4)
    plane_forward(more)
    for at in range(0, order, chunk):
        acol[at:at + chunk, :] = col2[at:at + chunk, :] * (1.0 / 720.0)
        gcol[at:at + chunk, :] = col2[at:at + chunk, :] * (1.0 / 120.0)
    line_forward(cols)
    line_near(cols)
    plane_forward(rows)
    line_far(cols)
    plane_finish(more)
    line_mid(cols)

    def odd_sum(acc, steps):
        for at in part_of_sum(steps):
            right = gcol[at, :] + col4[at, :] * (1.0 / 5040.0)
            acc = acc + dot_split(split(row3[:, at]), split(right))
        return acc

    odd = odd_sum(jnp.zeros((BLK, BLK), jnp.float32), close)
    line_done(cols)
    odd = odd_sum(odd, distant)
    odd = odd + blk1[...] + blk3[...] * (1.0 / 6.0)
    def even_columns(at):
        return acol[at, :] + col4[at, :] * (1.0 / 40320.0)

    even = plane_sum(rows, row4, even_columns, jnp.zeros((BLK, BLK), jnp.float32))
    even = even + blk2[...] * 0.5 + blk4[...] * (1.0 / 24.0)
    even = even + jnp.where(eye & jnp.logical_not(off_diag), 1.0, 0.0)

    eblk[...] = even + odd
    etr[...] = jnp.transpose(even - odd)
    cols = line_start(4, etr, row_slots(ej))
    rows = plane_start(3, eblk, erow)
    erow[:, lanes(c)] = eblk[...]
    ej[:, lanes(r)] = etr[...]
    plane_forward(rows)
    line_forward(cols)
    line_near(cols)

    def turn(g):
        slots = plane_pieces(rows, groups[g])
        high, tail = split(jnp.concatenate([erow[:, at] for at in slots], axis=1))
        turned[g] = dot(mt[...], jnp.concatenate([high, high, tail], axis=0))

    for g in range(len(groups) - 2):
        turn(g)
    line_far(cols)
    for g in range(len(groups) - 2, len(groups)):
        turn(g)
    plane_done(rows)

    hall = [(ox, oy, ok) for ox in range(nx) for oy in range(ny) for ok in range(nk)]
    hall.sort(key=lambda step: min(step[0], nx - step[0]) + min(step[1], ny - step[1]))

    def at_hall(ox, oy, ok):
        return dev(off(x, ox, nx), off(y, oy, ny), z, off(k, ok, nk))

    line_mid(cols)
    line_done(cols)
    own = nk * c + k
    copies = []
    for g, pieces in reversed(list(enumerate(groups))):
        for i, (ox, oy) in enumerate(pieces):
            back = (nx - ox) % nx, (ny - oy) % ny
            place = nx * off(y, back[1], ny) + off(x, back[0], nx)
            left = ej[:, lanes(place)]
            sums = jnp.concatenate(
                [
                    jnp.sum(left * turned[g, j * BLK:(j + 1) * BLK, i * BLK:(i + 1) * BLK], axis=0, keepdims=True)
                    for j in range(2 * nx)
                ],
                axis=0,
            )
            for h in range(nk):
                part[nk * (4 * g + i) + h] = sums[h * nx:(h + 1) * nx]
        for i, (ox, oy) in enumerate(pieces):
            back = (nx - ox) % nx, (ny - oy) % ny
            for ok in range(nk):
                src = part.at[nk * (4 * g + i) + off(k, ok, nk)]
                if (ox, oy, ok) == (0, 0, 0):
                    pz[pl.ds(own, 1)] = part[pl.ds(nk * (4 * g + i) + k, 1)]
                else:
                    at = hall.index((*back, ok))
                    copies.append(remote(src, pz.at[own], sml_s.at[2], sml_r.at[2], at_hall(*back, ok)))
                    copies[-1].start()
    with jax.named_scope("small2"):
        all_here(sml_r.at[2], pz.at[0:nk * count - 1])
    all_sent(sml_s.at[2], pz.at[0:nk * count - 1])
    value = pz[0]
    for i in range(1, nk * count):
        value = value + pz[i]
    ttile[...] = value
    px[pl.ds(z, 1)] = value[None]
    copies = []
    for oz in sorted(range(1, nz), key=lambda oz: -min(oz, nz - oz)):
        copies.append(remote(ttile, px.at[z], sml_s.at[3], sml_r.at[3], at_line(oz, 0)))
        copies[-1].start()
    with jax.named_scope("small3"):
        all_here(sml_r.at[3], px.at[0:nz - 1])
    all_sent(sml_s.at[3], px.at[0:nz - 1])
    value = px[0]
    for i in range(1, nz):
        value = value + px[i]
    qtile[...] = value
    tfin[pl.ds(own, 1)] = value[None]
    copies = []
    for ox, oy, ok in reversed(hall[1:]):
        copies.append(remote(qtile, tfin.at[own], sml_s.at[4], sml_r.at[4], at_hall(ox, oy, ok)))
        copies[-1].start()

    @pl.when(holds & (x == px_t))
    def _():
        all_sent(dia_s.at[0], gcol.at[0:8 * (count + len(line) - 2), :])

    @pl.when(holds & (x != px_t))
    def _():
        all_sent(dia_s.at[0], gcol.at[0:8 * (count + len(line) - 1), :])

    with jax.named_scope("small4"):
        all_here(sml_r.at[4], tfin.at[0:nk * count - 1])
    all_sent(sml_s.at[4], tfin.at[0:nk * count - 1])
    trial = jnp.zeros((nx, BLK), jnp.float32)
    for h in range(nk):
        value = jnp.zeros((nx, BLK), jnp.float32)
        for i in range(count):
            value = value + (0.5 - tfin[nk * i + h] * tfin[nk * i + h])
        trial = trial + value * row_weights[h]
    trial = jnp.sum(trial, axis=0, keepdims=True)
    stat_ref[...] = jnp.zeros((8, BLK), jnp.float32)
    stat_ref[0:1, :] = spread
    stat_ref[1:2, :] = jnp.broadcast_to(jnp.sum(trial, axis=1, keepdims=True) / order, (1, BLK))


def hand_out(grad_ref, dir_ref, trial_ref, stat_ref, spread_out, trial_spread_out, grad_out, dir_out, trial_out):
    spread_out[0, 0] = jnp.sum(stat_ref[0:1, 0:1])
    trial_spread_out[0, 0] = jnp.sum(stat_ref[1:2, 0:1])
    grad_out[...] = grad_ref[...]
    dir_out[...] = dir_ref[...]
    halves = trial_out.shape[0] // 2
    for i in range(trial_ref.shape[0] // 2):
        for b in range(trial_out.shape[0]):
            at = 2 * (b % halves)
            trial_out[b, :, i * BLK:(i + 1) * BLK] = trial_ref[2 * i + b // halves, at:at + 2, :]


def shards(dims, m_matrices, bvec_index, weight_table, grad_prev, dir_prev):
    nx, ny, nz, nk = dims
    count = nx * ny
    order = count * BLK
    f32 = jnp.float32
    rows, cols = grad_prev.shape
    vmem = pl.BlockSpec(memory_space=pltpu.VMEM)
    smem = pl.BlockSpec(memory_space=pltpu.SMEM)
    wide = pltpu.VMEM((BLK, order), f32)
    tall = pltpu.VMEM((order, BLK), f32)
    block = pltpu.VMEM((BLK, BLK), f32)
    tile = pltpu.VMEM((8, BLK), f32)
    half_tile = pltpu.VMEM((nx, BLK), f32)
    line = pltpu.VMEM((1, BLK), f32)
    lines = pltpu.VMEM((count, 1, BLK), f32)
    dma = pltpu.SemaphoreType.DMA
    grad, direction, trial, stat = pl.pallas_call(
        functools.partial(kernel, dims),
        out_shape=(
            jax.ShapeDtypeStruct((rows, cols), f32),
            jax.ShapeDtypeStruct((rows, cols), f32),
            jax.ShapeDtypeStruct((nk * count, nx, BLK), f32),
            jax.ShapeDtypeStruct((8, BLK), f32),
        ),
        in_specs=[pl.BlockSpec(memory_space=pltpu.HBM)] * 5,
        out_specs=(vmem, vmem, vmem, vmem),
        scratch_shapes=[
            pltpu.SMEM(bvec_index.shape, jnp.int32), pltpu.SMEM(weight_table.shape, f32),
            pltpu.VMEM(m_matrices.shape[1:], f32), pltpu.VMEM((rows, cols), f32), pltpu.VMEM((rows, cols), f32), dma((5,)),
            pltpu.VMEM((nx, 2, BLK, BLK), f32), block, pltpu.VMEM((nx, 8, BLK), f32), tile,
            block, block, block, block, block, block, block, block, line, lines, lines,
            wide, tall, wide, tall, tall, wide, tall, wide, wide, tall, wide, wide,
            pltpu.VMEM((2 * nx * BLK, 3 * BLK), jnp.bfloat16), pltpu.VMEM((count // 4, 2 * nx * BLK, 4 * BLK), f32),
            pltpu.VMEM((nk * count, nx, BLK), f32), pltpu.VMEM((nk * count, nx, BLK), f32), pltpu.VMEM((nz, nx, BLK), f32),
            half_tile, half_tile,
            dma((1,)), dma((1,)),
            dma((1,)), dma((2 * nx,)),
            dma((1,)), dma((4,)),
            dma((3,)), dma((3, 10)),
            dma((3,)), dma((3, 9)),
            dma((3,)), dma((3, 2)),
            dma((5,)), dma((5,)),
        ],
        compiler_params=pltpu.CompilerParams(
            collective_id=0, has_side_effects=True, vmem_limit_bytes=40 * 1024 * 1024
        ),
    )(*(
        pltpu.with_memory_space_constraint(array, pltpu.HBM)
        for array in (m_matrices.reshape(m_matrices.shape[1:]), dir_prev, grad_prev, bvec_index, weight_table)
    ))
    one = jax.ShapeDtypeStruct((1, 1), f32)
    block_out = jax.ShapeDtypeStruct((rows, cols), f32)
    spread, trial_spread, grad, direction, trial = pl.pallas_call(
        hand_out,
        out_shape=(one, one, block_out, block_out, jax.ShapeDtypeStruct((nx, 2, order), f32)),
        in_specs=[vmem] * 4,
        out_specs=(smem, smem, vmem, vmem, vmem),
        compiler_params=pltpu.CompilerParams(vmem_limit_bytes=8 * 1024 * 1024),
    )(grad, direction, trial, stat)
    return spread.reshape(()), trial_spread.reshape(()), grad, direction, trial


def solution(mesh):
    nx, ny, nk = mesh.shape["bvec"], mesh.shape["col"], 2
    nz = mesh.shape["row"] // nk
    torus = Mesh(mesh.devices.reshape(nx, nz, nk, ny), ("bvec", "zed", "core", "col"))
    return jax.shard_map(
        functools.partial(shards, (nx, ny, nz, nk)),
        mesh=torus,
        in_specs=(P("bvec", None, ROW, "col"), P(), P(), P(ROW, "col"), P(ROW, "col")),
        out_specs=(P(), P(), P(ROW, "col"), P(ROW, "col"), P()),
        check_vma=False,
    )
```

```python
import functools

import jax
import jax.numpy as jnp
from jax import lax
from jax.experimental import pallas as pl
from jax.experimental.pallas import tpu as pltpu
from jax.sharding import Mesh
from jax.sharding import PartitionSpec as P

ROW = ("zed", "core")
STEP_SCALE = 1.75
BLK = 128
MESH = pl.DeviceIdType.MESH


def split(value):
    high = value.astype(jnp.bfloat16)
    low = (value - high.astype(jnp.float32)).astype(jnp.bfloat16)
    return high, low


def dot(left, right):
    return jnp.dot(left, right, preferred_element_type=jnp.float32)


def dot_split(left, right):
    (lh, ll), (rh, rl) = left, right
    size = rh.shape[1]
    both = dot(lh, jnp.concatenate([rh, rl], axis=1))
    return both[:, :size] + (both[:, size:] + dot(ll, rh))


def kernel(
    dims, m_in, dp_in, gp_in, idx_in, tab_in,
    grad_ref, dir_ref, tfin, stat_ref,
    idx_ref, tab_ref, m_ref, gp_ref, dp_ref, in_s,
    mall, dcm, drt, dsrc, gblk, blk1, blk2, blk3, blk4, eblk, etr, own_block, stile, sx, sz,
    drow, dcol, grow, gcol, acol, row2, col2, row3, row4, col4, erow, ej, mt, turned, part, pz, px, qtile, ttile,
    a2a_s, a2a_r, dia_s, dia_r, dpr_s, dpr_r, row_s, row_r, col_s, col_r, fwd_s, fwd_r, sml_s, sml_r,
):
    nx, ny, nz, nk = dims
    count = nx * ny
    order = count * BLK
    wide = nx * BLK
    x, y = lax.axis_index("bvec"), lax.axis_index("col")
    z, k = lax.axis_index("zed"), lax.axis_index("core")
    r = nk * z + k
    c = nx * y + x

    def dev(xx, yy, zz, kk):
        return {"bvec": xx, "zed": zz, "core": kk, "col": yy}

    def off(value, step, size):
        return lax.rem(value + step, size) if step else value

    def lanes(index, size=BLK):
        return pl.ds(pl.multiple_of(index * size, size), size)

    plane = [(ox, oy) for ox in range(nx) for oy in range(ny) if (ox, oy) != (0, 0)]
    line = [(oz, ok) for oz in range(nz) for ok in range(nk)]
    others = line[1:]

    def at_plane(ox, oy):
        return dev(off(x, ox, nx), off(y, oy, ny), z, k)

    def at_line(oz, ok):
        return dev(x, y, off(z, oz, nz), off(k, ok, nk))

    px_t, py_t = lax.rem(r, nx), lax.div(r, nx)
    pz_t, pk_t = lax.div(c, nk), lax.rem(c, nk)
    off_diag = r != c
    holds = y == py_t

    loads = [
        pltpu.make_async_copy(src, dst, in_s.at[i])
        for i, (src, dst) in enumerate(
            ((m_in, m_ref), (dp_in, dp_ref), (gp_in, gp_ref), (idx_in, idx_ref), (tab_in, tab_ref))
        )
    ]
    for copy in loads:
        copy.start()

    barrier = pltpu.get_barrier_semaphore()
    for ox, oy in plane:
        pl.semaphore_signal(barrier, inc=1, device_id=at_plane(ox, oy), device_id_type=MESH)
    for oz, ok in others:
        pl.semaphore_signal(barrier, inc=1, device_id=at_line(oz, ok), device_id_type=MESH)

    for b in range(nx):
        @pl.when((x != b) | off_diag)
        def _(b=b):
            pl.semaphore_signal(barrier, inc=1, device_id=dev(b, y, pz_t, pk_t), device_id_type=MESH)

    for copy in loads:
        copy.wait()

    own_d = dp_ref[:, lanes(x)]
    eye_r = lax.broadcasted_iota(jnp.int32, (BLK, BLK), 0)
    eye_c = lax.broadcasted_iota(jnp.int32, (BLK, BLK), 1)
    eye = eye_r == eye_c
    dsrc[...] = jnp.zeros((8, BLK), jnp.float32)
    for p in range(2):
        dsrc[p:p + 1, :] = jnp.sum(jnp.where(eye, m_ref[p, :, lanes(px_t)], 0.0), axis=0, keepdims=True)
    if nx * 8 < BLK:
        dcm[nx * 8:, :] = jnp.zeros((BLK - nx * 8, BLK), jnp.float32)

    expected = len(plane) + len(others)
    asked = len(line) - (x == px_t).astype(jnp.int32)
    with jax.named_scope("barrier"):
        pl.semaphore_wait(barrier, expected + holds.astype(jnp.int32) * asked)

    def remote(src, dst, send, recv, device):
        return pltpu.make_async_remote_copy(
            src_ref=src, dst_ref=dst, send_sem=send, recv_sem=recv, device_id=device, device_id_type=MESH
        )

    def all_sent(sem, ref):
        remote(ref, ref, sem, sem, dev(x, y, z, k)).wait_send()

    def all_here(sem, ref):
        remote(ref, ref, sem, sem, dev(x, y, z, k)).wait_recv()

    def pieces_of(count_blocks):
        return gcol.at[0:int(count_blocks * BLK), :]

    dia_row = [
        remote(dsrc, dcm.at[pl.ds(pl.multiple_of(8 * x, 8), 8), :], dia_s.at[0], dia_r.at[x], at_plane(ox, oy))
        for i, (ox, oy) in enumerate(plane)
    ]
    dia_col = [
        remote(dsrc, drt.at[x], dia_s.at[0], dia_r.at[nx + x],
               dev(px_t, y, off(z, oz, nz), off(k, ok, nk)))
        for i, (oz, ok) in enumerate(line)
    ]

    @pl.when(holds)
    def _():
        for copy in dia_row:
            copy.start()
        for copy in dia_col[1:]:
            copy.start()
        dcm[pl.ds(pl.multiple_of(8 * x, 8), 8), :] = dsrc[...]

    @pl.when(holds & (x != px_t))
    def _():
        dia_col[0].start()

    @pl.when(jnp.logical_not(off_diag))
    def _():
        drt[pl.ds(x, 1)] = dsrc[...][None]

    a2a = []
    for ox in range(1, nx):
        xp = off(x, ox, nx)
        copy = remote(m_ref.at[:, :, lanes(xp)], mall.at[x], a2a_s.at[0], a2a_r.at[0], dev(xp, y, z, k))
        copy.start()
        a2a.append(copy)

    def wait_all(copies, name="wait"):
        with jax.named_scope(name):
            for copy in copies:
                copy.wait()

    half = BLK // 2
    top, low = slice(0, half), slice(half, BLK)

    def far_block(step, part, index):
        held = drow.at[part, lanes(off(y, ny - step, ny), wide)]
        return remote(held, held, dpr_s.at[0], dpr_r.at[index], at_plane(0, step))

    dprow = []
    for i, oy in enumerate((1, ny - 1)):
        copy = remote(dp_ref, drow.at[:, lanes(y, wide)], dpr_s.at[0], dpr_r.at[i], at_plane(0, oy))
        copy.start()
        dprow.append(copy)

    ring_x = [1, nx - 1, 2]
    ring_y = [1, ny - 1, 2]

    arrivals = [(0, 0), (1, 0), (0, 1), (nx - 1, 0), (0, ny - 1), (2, 0), (0, 2)]
    arrivals += [(ox, oy) for ox in (1, nx - 1) for oy in (1, ny - 1)]
    arrivals += [(ox, oy) for ox, oy in plane if ox and oy and 2 in (ox, oy) and ox != oy] + [(2, 2)]
    groups = [arrivals[i:i + 4] for i in range(0, len(arrivals), 4)]

    def group_sem(bank, ox, oy):
        return row_r.at[bank, 6 + [g for g, pieces in enumerate(groups) if (ox, oy) in pieces][0]]

    def plane_start(stage, src, dst):
        bank = 2 if stage == 4 else stage % 2
        first = []
        for n, (over_x, over_y) in enumerate(((top, low), (low, top))):
            for i in range(3):
                for m, part_of, device in ((0, over_x, at_plane(ring_x[i], 0)), (1, over_y, at_plane(0, ring_y[i]))):
                    step = (0, ring_y[i]) if m else (ring_x[i], 0)
                    sem = group_sem(bank, *step) if n else row_r.at[bank, 2 * i + m]
                    first.append(remote(src.at[part_of, :], dst.at[part_of, lanes(c)], row_s.at[bank], sem, device))
                    first[-1].start()
        return stage, bank, dst, first, []

    def plane_forward(state):
        stage, bank, dst, first, second = state
        with jax.named_scope(f"row{stage}a"):
            for i in range(3):
                first[2 * i].wait_recv()
                held = dst.at[top, lanes(nx * y + off(x, nx - ring_x[i], nx))]
                for j in (2, 0, 1):
                    sem = group_sem(bank, ring_x[i], ring_y[j])
                    second.append(remote(held, held, row_s.at[bank], sem, at_plane(0, ring_y[j])))
                    second[-1].start()
                first[2 * i + 1].wait_recv()
                held = dst.at[low, lanes(nx * off(y, ny - ring_y[i], ny) + x)]
                for j in (2, 0, 1):
                    sem = group_sem(bank, ring_x[j], ring_y[i])
                    second.append(remote(held, held, row_s.at[bank], sem, at_plane(ring_x[j], 0)))
                    second[-1].start()

    def plane_pieces(state, pieces):
        stage, bank, _, _, _ = state
        halves = sum(2 if ox and oy else 1 for ox, oy in pieces if (ox, oy) != (0, 0))
        with jax.named_scope(f"row{stage}w"):
            all_here(row_r.at[bank, 6 + groups.index(pieces)], pieces_of(halves / 2))
        return [lanes(nx * off(y, ny - oy if oy else 0, ny) + off(x, nx - ox if ox else 0, nx)) for ox, oy in pieces]

    def plane_sum(state, left, right, acc, before_last=lambda: None):
        for pieces in groups:
            if pieces is groups[-2]:
                before_last()
            places = plane_pieces(state, pieces)
            rows_l = jnp.concatenate([left[:, at] for at in places], axis=1)
            cols_r = jnp.concatenate([right(at) for at in places], axis=0)
            acc = acc + dot_split(split(rows_l), split(cols_r))
        plane_done(state)
        return acc

    def plane_done(state):
        all_sent(row_s.at[state[1]], pieces_of(count - 1))

    def plane_finish(state):
        for pieces in groups:
            plane_pieces(state, pieces)
        plane_done(state)

    def line_start(stage, src, slot):
        bank = (2, 0, 1, 0, 1)[stage]
        whole = slice(0, BLK)
        first = {}
        order_z = ((2, top), (nz - 2, low), (2, low), (nz - 2, top), (1, whole), (nz - 1, whole))
        for i, (oz, piece) in enumerate(order_z):
            first[oz, piece.start] = remote(
                src.at[piece, :], slot(r, piece), col_s.at[bank], col_r.at[bank, i], at_line(oz, 0)
            )
            first[oz, piece.start].start()
        over = [remote(src, slot(r), fwd_s.at[bank], fwd_r.at[bank, 0], at_line(0, 1))]
        over[0].start()
        return stage, bank, slot, first, {}, over

    def line_across(state, oz):
        stage, bank, slot, first, second, over = state
        held = slot(nk * off(z, nz - oz, nz) + k)
        over.append(remote(held, held, fwd_s.at[bank], fwd_r.at[bank, 1 if oz in distant else 0], at_line(0, 1)))
        over[-1].start()

    def line_forward(state):
        stage, bank, slot, first, second, over = state
        with jax.named_scope(f"line{stage}a"):
            steps = ((2, top, (2, 1)), (nz - 2, low, (nz - 2, nz - 1)), (2, low, (1,)), (nz - 2, top, (nz - 1,)))
            for oz, piece, onward in steps:
                first[oz, piece.start].wait_recv()
                held = slot(nk * off(z, nz - oz, nz) + k, piece)
                for step in onward:
                    at = 6 + distant.index((oz + step) % nz)
                    remote(held, held, col_s.at[bank], col_r.at[bank, at], at_line(step, 0)).start()

    def line_near(state):
        stage, bank, slot, first, second, over = state
        with jax.named_scope(f"line{stage}n"):
            for oz in (2, nz - 2, 1, nz - 1):
                if oz in (1, nz - 1):
                    first[oz, 0].wait_recv()
                line_across(state, oz)

    close = (0, 2, nz - 2, 1, nz - 1)
    distant = (3, nz - 3, 4)

    def line_far(state):
        stage, bank, slot, first, second, over = state
        with jax.named_scope(f"line{stage}f"):
            for oz in (3, nz - 3, 4):
                all_here(col_r.at[bank, 6 + distant.index(oz)], pieces_of(1))
                line_across(state, oz)

    def line_mid(state):
        with jax.named_scope(f"line{state[0]}m"):
            all_here(fwd_r.at[state[1], 0], pieces_of(len(close)))

    def line_done(state):
        stage, bank, slot, first, second, over = state
        with jax.named_scope(f"line{stage}d"):
            all_here(fwd_r.at[bank, 1], pieces_of(len(distant)))
            all_sent(fwd_s.at[bank], pieces_of(nz))
            all_sent(col_s.at[bank], pieces_of(nz - 1))

    def line_finish(state):
        line_far(state)
        line_mid(state)
        line_done(state)

    def part_of_sum(steps):
        size = nk * BLK
        return [pl.ds(pl.multiple_of(off(z, step, nz) * size, size), size) for step in steps]

    def column_slots(ref):
        def slot(index, part=slice(0, BLK)):
            return ref.at[pl.ds(pl.multiple_of(index * BLK + part.start, half), part.stop - part.start), :]
        return slot

    def row_slots(ref):
        return lambda index, part=slice(0, BLK): ref.at[part, lanes(index)]

    own_block[...] = own_d
    d_col = line_start(0, own_block, column_slots(dcol))

    mall[pl.ds(x, 1)] = m_ref[:, :, lanes(x)][None]
    drow[:, lanes(y, wide)] = dp_ref[...]
    dcol[lanes(r), :] = own_d
    line_forward(d_col)

    for b in range(nx):
        @pl.when(jnp.logical_not(holds & (x == b)))
        @jax.named_scope("diag_r")
        def _(b=b):
            slot = dcm.at[8 * b:8 * b + 8, :]
            remote(slot, slot, dia_s.at[0], dia_r.at[b], dev(x, y, z, k)).wait_recv()

        @pl.when(off_diag | (x != b))
        def _(b=b):
            slot = drt.at[b]
            remote(slot, slot, dia_s.at[0], dia_r.at[nx + b], dev(x, y, z, k)).wait_recv()

    weights = []
    for b in range(nx):
        value = jnp.float32(0.0)
        for t in range(tab_ref.shape[0]):
            value = value + jnp.where(idx_ref[b] == t, tab_ref[t], jnp.float32(0.0))
        weights.append(value)

    row_index = lax.broadcasted_iota(jnp.int32, (nx, BLK), 0)
    row_weights = []
    for h in range(nk):
        value = jnp.zeros((nx, BLK), jnp.float32)
        for b in range(nx // nk):
            value = jnp.where((row_index >= 2 * b) & (row_index < 2 * b + 2), weights[h * (nx // nk) + b], value)
        row_weights.append(value)
    columns = jnp.transpose(dcm[...])
    line_near(d_col)
    far = []
    for i, (step, piece) in enumerate(((1, top), (ny - 1, low))):
        dprow[i].wait_recv()
        far.append(far_block(step, piece, 2 + i))
        far[-1].start()
    with jax.named_scope("a2a"):
        all_here(a2a_r.at[0], mall.at[0:nx - 1])
    total = jnp.zeros((BLK, BLK), jnp.float32)
    spread_row = jnp.zeros((1, BLK), jnp.float32)
    for b in range(nx):
        term = jnp.zeros((BLK, BLK), jnp.float32)
        for p in range(2):
            at_row = columns[:, 8 * b + p:8 * b + p + 1]
            at_col = drt[b, p:p + 1, :]
            term = term + mall[b, p] * (at_row - at_col)
        total = total + (2.0 * weights[b]) * term
        re_d, im_d = drt[b, 0:1, :], drt[b, 1:2, :]
        spread_row = spread_row + weights[b] * (1.0 - re_d * re_d - im_d * im_d)
    gblk[...] = total
    own_p = gp_ref[:, lanes(x)]
    first_line = (r == 0).astype(jnp.float32)
    sums = [total * total, total * own_d, own_d * own_d, own_p * own_p]
    row_sums = [jnp.sum(value, axis=0, keepdims=True) for value in sums] + [spread_row * first_line]
    row_sums.append(jnp.zeros((8 - len(row_sums), BLK), jnp.float32))
    row_sums = jnp.sum(jnp.concatenate(row_sums, axis=0), axis=1, keepdims=True)
    pick = lax.broadcasted_iota(jnp.int32, (8, BLK), 0) == lax.broadcasted_iota(jnp.int32, (8, BLK), 1)
    stile[...] = jnp.sum(jnp.where(pick, row_sums, 0.0), axis=0, keepdims=True)

    def small_plane(stage, src, dst):
        dst[pl.ds(c, 1)] = src[...][None]
        copies = []
        for i, (ox, oy) in enumerate(plane):
            copy = remote(src, dst.at[c], sml_s.at[stage], sml_r.at[stage], at_plane(ox, oy))
            copy.start()
            copies.append(copy)
        return copies

    def small_line(stage, src, dst):
        dst[pl.ds(r, 1)] = src(r)[...][None]
        copies = []
        for i, (oz, ok) in enumerate(others):
            rp = nk * off(z, oz, nz) + off(k, ok, nk)
            copy = remote(src(rp), dst.at[r], sml_s.at[stage], sml_r.at[stage], at_line(oz, ok))
            copy.start()
            copies.append(copy)
        return copies

    def summed(ref):
        value = ref[0]
        for i in range(1, count):
            value = value + ref[i]
        return value

    copies = small_line(0, lambda index: stile, sx)
    cols = line_start(1, gblk, column_slots(gcol))
    rows = plane_start(0, gblk, grow)
    grow[:, lanes(c)] = total
    gcol[lanes(r), :] = total
    with jax.named_scope("small0"):
        all_here(sml_r.at[0], sx.at[0:count - 1])
    all_sent(sml_s.at[0], sx.at[0:count - 1])
    stile[...] = summed(sx)
    copies = small_plane(1, stile, sz)
    line_forward(cols)
    plane_forward(rows)
    line_near(cols)
    line_finish(d_col)
    with jax.named_scope("far"):
        for copy in far:
            copy.wait_recv()
    all_sent(dpr_s.at[0], pieces_of(order // BLK * 3 / 4))
    all_sent(a2a_s.at[0], mall.at[0:nx - 1])
    line_far(cols)
    plane_finish(rows)
    line_mid(cols)
    with jax.named_scope("small1"):
        all_here(sml_r.at[1], sz.at[0:count - 1])
    all_sent(sml_s.at[1], sz.at[0:count - 1])
    sums = jnp.sum(jnp.where(pick, summed(sz), 0.0), axis=1, keepdims=True)
    gg, gd, dd, pp, spread = (jnp.broadcast_to(sums[i:i + 1, :], (1, BLK)) for i in range(5))
    spread = spread / order
    beta = gg / (1.0 + pp)
    norm = jnp.maximum(gg - 2.0 * beta * gd + beta * beta * dd, 0.0)
    scale = STEP_SCALE / jnp.sqrt(1.0 + norm / order)

    chunk = 4 * BLK if order % (4 * BLK) == 0 else BLK
    beta_w = jnp.concatenate([beta] * nk, axis=1)

    def square(acc, steps):
        for at in part_of_sum(steps):
            left = beta_w * drow[:, at] - grow[:, at]
            right = beta * dcol[at, :] - gcol[at, :]
            acol[at, :] = right
            acc = acc + dot_split(split(left), split(right))
        return acc

    acc = square(jnp.zeros((BLK, BLK), jnp.float32), close)
    line_done(cols)
    acc = square(acc, distant)
    acc = acc * scale * scale
    blk1[...] = scale * acol[lanes(r), :]
    blk2[...] = acc
    cols = line_start(2, blk2, column_slots(col2))
    rows = plane_start(1, blk2, row2)
    row2[:, lanes(c)] = acc
    col2[lanes(r), :] = acc
    for j in range(nx):
        at = pl.ds(pl.multiple_of(y * wide + j * BLK, BLK), BLK)
        piece = grow[:, at]
        grad_ref[:, j * BLK:(j + 1) * BLK] = piece
        dir_ref[:, j * BLK:(j + 1) * BLK] = beta * drow[:, at] - piece

    for b in range(nx):
        for p in range(2):
            i = 2 * b + p
            high, tail = split(jnp.transpose(mall[b, p]))
            mt[i * BLK:(i + 1) * BLK, :] = jnp.concatenate([high, tail, high], axis=1)
    line_forward(cols)
    plane_forward(rows)
    line_near(cols)
    acc3 = plane_sum(
        rows, row2, lambda at: acol[at, :], jnp.zeros((BLK, BLK), jnp.float32), lambda: line_far(cols)
    )
    acc3 = acc3 * scale
    blk3[...] = acc3
    row3[:, lanes(c)] = acc3
    more = plane_start(4, blk3, row3)
    line_mid(cols)

    def fourth(acc, steps):
        for at in part_of_sum(steps):
            acc = acc + dot_split(split(row2[:, at]), split(col2[at, :]))
        return acc

    acc4 = fourth(jnp.zeros((BLK, BLK), jnp.float32), close)
    line_done(cols)
    acc4 = fourth(acc4, distant)
    blk4[...] = acc4
    cols = line_start(3, blk4, column_slots(col4))
    rows = plane_start(2, blk4, row4)
    row4[:, lanes(c)] = acc4
    col4[lanes(r), :] = acc4
    plane_forward(more)
    for at in range(0, order, chunk):
        acol[at:at + chunk, :] = col2[at:at + chunk, :] * (1.0 / 720.0)
        gcol[at:at + chunk, :] = col2[at:at + chunk, :] * (1.0 / 120.0)
    line_forward(cols)
    plane_forward(rows)
    line_near(cols)
    line_far(cols)
    plane_finish(more)
    line_mid(cols)

    def odd_sum(acc, steps):
        for at in part_of_sum(steps):
            right = gcol[at, :] + col4[at, :] * (1.0 / 5040.0)
            acc = acc + dot_split(split(row3[:, at]), split(right))
        return acc

    odd = odd_sum(jnp.zeros((BLK, BLK), jnp.float32), close)
    line_done(cols)
    odd = odd_sum(odd, distant)
    odd = odd + blk1[...] + blk3[...] * (1.0 / 6.0)
    def even_columns(at):
        return acol[at, :] + col4[at, :] * (1.0 / 40320.0)

    even = plane_sum(rows, row4, even_columns, jnp.zeros((BLK, BLK), jnp.float32))
    even = even + blk2[...] * 0.5 + blk4[...] * (1.0 / 24.0)
    even = even + jnp.where(eye & jnp.logical_not(off_diag), 1.0, 0.0)

    eblk[...] = even + odd
    etr[...] = jnp.transpose(even - odd)
    cols = line_start(4, etr, row_slots(ej))
    rows = plane_start(3, eblk, erow)
    erow[:, lanes(c)] = eblk[...]
    ej[:, lanes(r)] = etr[...]
    plane_forward(rows)
    line_forward(cols)
    line_near(cols)

    def turn(g):
        slots = plane_pieces(rows, groups[g])
        high, tail = split(jnp.concatenate([erow[:, at] for at in slots], axis=1))
        turned[g] = dot(mt[...], jnp.concatenate([high, high, tail], axis=0))

    for g in range(len(groups) - 2):
        turn(g)
    line_far(cols)
    for g in range(len(groups) - 2, len(groups)):
        turn(g)
    plane_done(rows)

    hall = [(ox, oy, ok) for ox in range(nx) for oy in range(ny) for ok in range(nk)]
    hall.sort(key=lambda step: min(step[0], nx - step[0]) + min(step[1], ny - step[1]))

    def at_hall(ox, oy, ok):
        return dev(off(x, ox, nx), off(y, oy, ny), z, off(k, ok, nk))

    line_mid(cols)
    line_done(cols)
    own = nk * c + k
    copies = []
    for g, pieces in reversed(list(enumerate(groups))):
        for i, (ox, oy) in enumerate(pieces):
            back = (nx - ox) % nx, (ny - oy) % ny
            place = nx * off(y, back[1], ny) + off(x, back[0], nx)
            left = ej[:, lanes(place)]
            sums = jnp.concatenate(
                [
                    jnp.sum(left * turned[g, j * BLK:(j + 1) * BLK, i * BLK:(i + 1) * BLK], axis=0, keepdims=True)
                    for j in range(2 * nx)
                ],
                axis=0,
            )
            for h in range(nk):
                part[nk * (4 * g + i) + h] = sums[h * nx:(h + 1) * nx]
        for i, (ox, oy) in enumerate(pieces):
            back = (nx - ox) % nx, (ny - oy) % ny
            for ok in range(nk):
                src = part.at[nk * (4 * g + i) + off(k, ok, nk)]
                if (ox, oy, ok) == (0, 0, 0):
                    pz[pl.ds(own, 1)] = part[pl.ds(nk * (4 * g + i) + k, 1)]
                else:
                    at = hall.index((*back, ok))
                    copies.append(remote(src, pz.at[own], sml_s.at[2], sml_r.at[2], at_hall(*back, ok)))
                    copies[-1].start()
    with jax.named_scope("small2"):
        all_here(sml_r.at[2], pz.at[0:nk * count - 1])
    all_sent(sml_s.at[2], pz.at[0:nk * count - 1])
    value = pz[0]
    for i in range(1, nk * count):
        value = value + pz[i]
    ttile[...] = value
    px[pl.ds(z, 1)] = value[None]
    copies = []
    for oz in sorted(range(1, nz), key=lambda oz: -min(oz, nz - oz)):
        copies.append(remote(ttile, px.at[z], sml_s.at[3], sml_r.at[3], at_line(oz, 0)))
        copies[-1].start()
    with jax.named_scope("small3"):
        all_here(sml_r.at[3], px.at[0:nz - 1])
    all_sent(sml_s.at[3], px.at[0:nz - 1])
    value = px[0]
    for i in range(1, nz):
        value = value + px[i]
    qtile[...] = value
    tfin[pl.ds(own, 1)] = value[None]
    copies = []
    for ox, oy, ok in reversed(hall[1:]):
        copies.append(remote(qtile, tfin.at[own], sml_s.at[4], sml_r.at[4], at_hall(ox, oy, ok)))
        copies[-1].start()

    @pl.when(holds & (x == px_t))
    def _():
        all_sent(dia_s.at[0], gcol.at[0:8 * (count + len(line) - 2), :])

    @pl.when(holds & (x != px_t))
    def _():
        all_sent(dia_s.at[0], gcol.at[0:8 * (count + len(line) - 1), :])

    with jax.named_scope("small4"):
        all_here(sml_r.at[4], tfin.at[0:nk * count - 1])
    all_sent(sml_s.at[4], tfin.at[0:nk * count - 1])
    trial = jnp.zeros((nx, BLK), jnp.float32)
    for h in range(nk):
        value = jnp.zeros((nx, BLK), jnp.float32)
        for i in range(count):
            value = value + (0.5 - tfin[nk * i + h] * tfin[nk * i + h])
        trial = trial + value * row_weights[h]
    trial = jnp.sum(trial, axis=0, keepdims=True)
    stat_ref[...] = jnp.zeros((8, BLK), jnp.float32)
    stat_ref[0:1, :] = spread
    stat_ref[1:2, :] = jnp.broadcast_to(jnp.sum(trial, axis=1, keepdims=True) / order, (1, BLK))


def hand_out(grad_ref, dir_ref, trial_ref, stat_ref, spread_out, trial_spread_out, grad_out, dir_out, trial_out):
    spread_out[0, 0] = jnp.sum(stat_ref[0:1, 0:1])
    trial_spread_out[0, 0] = jnp.sum(stat_ref[1:2, 0:1])
    grad_out[...] = grad_ref[...]
    dir_out[...] = dir_ref[...]
    halves = trial_out.shape[0] // 2
    for i in range(trial_ref.shape[0] // 2):
        for b in range(trial_out.shape[0]):
            at = 2 * (b % halves)
            trial_out[b, :, i * BLK:(i + 1) * BLK] = trial_ref[2 * i + b // halves, at:at + 2, :]


def shards(dims, m_matrices, bvec_index, weight_table, grad_prev, dir_prev):
    nx, ny, nz, nk = dims
    count = nx * ny
    order = count * BLK
    f32 = jnp.float32
    rows, cols = grad_prev.shape
    vmem = pl.BlockSpec(memory_space=pltpu.VMEM)
    smem = pl.BlockSpec(memory_space=pltpu.SMEM)
    wide = pltpu.VMEM((BLK, order), f32)
    tall = pltpu.VMEM((order, BLK), f32)
    block = pltpu.VMEM((BLK, BLK), f32)
    tile = pltpu.VMEM((8, BLK), f32)
    half_tile = pltpu.VMEM((nx, BLK), f32)
    line = pltpu.VMEM((1, BLK), f32)
    lines = pltpu.VMEM((count, 1, BLK), f32)
    dma = pltpu.SemaphoreType.DMA
    grad, direction, trial, stat = pl.pallas_call(
        functools.partial(kernel, dims),
        out_shape=(
            jax.ShapeDtypeStruct((rows, cols), f32),
            jax.ShapeDtypeStruct((rows, cols), f32),
            jax.ShapeDtypeStruct((nk * count, nx, BLK), f32),
            jax.ShapeDtypeStruct((8, BLK), f32),
        ),
        in_specs=[pl.BlockSpec(memory_space=pltpu.HBM)] * 5,
        out_specs=(vmem, vmem, vmem, vmem),
        scratch_shapes=[
            pltpu.SMEM(bvec_index.shape, jnp.int32), pltpu.SMEM(weight_table.shape, f32),
            pltpu.VMEM(m_matrices.shape[1:], f32), pltpu.VMEM((rows, cols), f32), pltpu.VMEM((rows, cols), f32), dma((5,)),
            pltpu.VMEM((nx, 2, BLK, BLK), f32), block, pltpu.VMEM((nx, 8, BLK), f32), tile,
            block, block, block, block, block, block, block, block, line, lines, lines,
            wide, tall, wide, tall, tall, wide, tall, wide, wide, tall, wide, wide,
            pltpu.VMEM((2 * nx * BLK, 3 * BLK), jnp.bfloat16), pltpu.VMEM((count // 4, 2 * nx * BLK, 4 * BLK), f32),
            pltpu.VMEM((nk * count, nx, BLK), f32), pltpu.VMEM((nk * count, nx, BLK), f32), pltpu.VMEM((nz, nx, BLK), f32),
            half_tile, half_tile,
            dma((1,)), dma((1,)),
            dma((1,)), dma((2 * nx,)),
            dma((1,)), dma((4,)),
            dma((3,)), dma((3, 10)),
            dma((3,)), dma((3, 9)),
            dma((3,)), dma((3, 2)),
            dma((5,)), dma((5,)),
        ],
        compiler_params=pltpu.CompilerParams(
            collective_id=0, has_side_effects=True, vmem_limit_bytes=40 * 1024 * 1024
        ),
    )(*(
        pltpu.with_memory_space_constraint(array, pltpu.HBM)
        for array in (m_matrices.reshape(m_matrices.shape[1:]), dir_prev, grad_prev, bvec_index, weight_table)
    ))
    one = jax.ShapeDtypeStruct((1, 1), f32)
    block_out = jax.ShapeDtypeStruct((rows, cols), f32)
    spread, trial_spread, grad, direction, trial = pl.pallas_call(
        hand_out,
        out_shape=(one, one, block_out, block_out, jax.ShapeDtypeStruct((nx, 2, order), f32)),
        in_specs=[vmem] * 4,
        out_specs=(smem, smem, vmem, vmem, vmem),
        compiler_params=pltpu.CompilerParams(vmem_limit_bytes=8 * 1024 * 1024),
    )(grad, direction, trial, stat)
    return spread.reshape(()), trial_spread.reshape(()), grad, direction, trial


def solution(mesh):
    nx, ny, nk = mesh.shape["bvec"], mesh.shape["col"], 2
    nz = mesh.shape["row"] // nk
    torus = Mesh(mesh.devices.reshape(nx, nz, nk, ny), ("bvec", "zed", "core", "col"))
    return jax.shard_map(
        functools.partial(shards, (nx, ny, nz, nk)),
        mesh=torus,
        in_specs=(P("bvec", None, ROW, "col"), P(), P(), P(ROW, "col"), P(ROW, "col")),
        out_specs=(P(), P(), P(ROW, "col"), P(ROW, "col"), P()),
        check_vma=False,
    )
```
